32 devices in a mesh: hp: 4 (over x, y), cp: 8 (over z, core).
Axes of the slice: x: 2, y: 2, z: 4, core: 2. Of those that a mesh axis runs over, the one named last changes fastest.
Arguments:
- q: bfloat16 [6144, 16, 64], P('cp', 'hp'), parts along dimension 1
- k: bfloat16 [6144, 16, 64], P('cp', 'hp'), parts along dimension 1
- v: bfloat16 [6144, 16, 64], P('cp', 'hp'), parts along dimension 1
- u_bias: float32 [16, 64], P('hp'), parts along dimension 0
- v_bias: float32 [16, 64], P('hp'), parts along dimension 0
- rel_table: bfloat16 [6144, 1024], P('cp')
- w_rel: bfloat16 [1024, 16, 64], P(None, 'hp'), parts along dimension 1
- d_out: bfloat16 [6144, 16, 64], P('cp', 'hp'), parts along dimension 1
Outputs:
- output 1: bfloat16 [6144, 16, 64], P('cp', 'hp'), parts along dimension 1
- output 2: bfloat16 [6144, 16, 64], P('cp', 'hp'), parts along dimension 1
- output 3: bfloat16 [6144, 16, 64], P('cp', 'hp'), parts along dimension 1
- output 4: bfloat16 [6144, 16, 64], P('cp', 'hp'), parts along dimension 1
- output 5: float32 [16, 64], P('hp'), parts along dimension 0
- output 6: float32 [16, 64], P('hp'), parts along dimension 0
- output 7: float32 [1024, 16, 64], P(None, 'hp'), parts along dimension 1
There are 4 independent parts. The reference program is written for one: setup_inputs(seed, part) draws one part's arguments, and reference() takes and returns one part's arrays. A program takes and returns all parts, laid end to end along the dimension named above; an argument that names none is the same for every part.
All inputs are finite; a program needn't handle non-finite values.
Results may differ from the reference program's by a relative error of at most 0.0151205.
Values are sent between devices in bfloat16 or wider.
A program may use at most 1 GiB of HBM per device.

```python
import math
import jax
import jax.numpy as jnp
from jax import lax

SEQ_LEN = 6144
HEADS_PART = 4
HEAD_DIM = 64
MODEL_DIM = 1024
ROW_BLOCK = math.gcd(SEQ_LEN, 256)
INV_SQRT = HEAD_DIM ** -0.5


def setup_inputs(seed: int = 0, part: int = 0) -> dict:
    part_key = jax.random.fold_in(jax.random.key(seed), part)
    keys_part = jax.random.split(part_key, 7)
    table_keys = jax.random.split(jax.random.key(seed + 17), 2)
    seq_shape = (SEQ_LEN, HEADS_PART, HEAD_DIM)
    head_shape = (HEADS_PART, HEAD_DIM)
    q = jax.random.normal(keys_part[0], seq_shape, jnp.float32)
    k = 2.0 * jax.random.normal(keys_part[1], seq_shape, jnp.float32)
    v = jax.random.normal(keys_part[2], seq_shape, jnp.float32)
    u_bias = 0.5 * jax.random.normal(keys_part[3], head_shape, jnp.float32)
    v_bias = jax.random.normal(keys_part[4], head_shape, jnp.float32)
    w_rel = jax.random.normal(keys_part[5], (MODEL_DIM, HEADS_PART, HEAD_DIM), jnp.float32) * MODEL_DIM ** -0.5
    d_out = jax.random.normal(keys_part[6], seq_shape, jnp.float32)
    freq_cols = 10000.0 ** (-jax.random.uniform(table_keys[0], (MODEL_DIM,), jnp.float32))
    phases = 2.0 * math.pi * jax.random.uniform(table_keys[1], (MODEL_DIM,), jnp.float32)
    offsets = jnp.arange(SEQ_LEN, dtype=jnp.float32)
    rel_table = jnp.sin(offsets[:, None] * freq_cols[None, :] + phases[None, :])
    return {
        'q': q.astype(jnp.bfloat16),
        'k': k.astype(jnp.bfloat16),
        'v': v.astype(jnp.bfloat16),
        'u_bias': u_bias,
        'v_bias': v_bias,
        'rel_table': rel_table.astype(jnp.bfloat16),
        'w_rel': w_rel.astype(jnp.bfloat16),
        'd_out': d_out.astype(jnp.bfloat16),
    }


def attention(q_u, q_v, k, v, rel):
    key_pos = jnp.arange(SEQ_LEN)

    def one_head(head_args):
        qu_h, qv_h, k_h, v_h, rel_h = head_args

        def row_block(start):
            qu_rows = lax.dynamic_slice_in_dim(qu_h, start, ROW_BLOCK)
            qv_rows = lax.dynamic_slice_in_dim(qv_h, start, ROW_BLOCK)
            query_pos = start + jnp.arange(ROW_BLOCK)
            offset_ij = query_pos[:, None] - key_pos[None, :]
            content = jnp.dot(qu_rows, k_h.T)
            by_offset = jnp.dot(qv_rows, rel_h.T)
            position = jnp.take_along_axis(by_offset, jnp.clip(offset_ij, 0, SEQ_LEN - 1), axis=1)
            score_ij = jnp.where(offset_ij >= 0, (content + position) * INV_SQRT, -jnp.inf)
            return jnp.dot(jax.nn.softmax(score_ij, axis=-1), v_h)

        starts = jnp.arange(0, SEQ_LEN, ROW_BLOCK)
        return lax.map(jax.checkpoint(row_block), starts).reshape(SEQ_LEN, HEAD_DIM)

    per_head = lax.map(jax.checkpoint(one_head), tuple(stacked.transpose(1, 0, 2) for stacked in (q_u, q_v, k, v, rel)))
    return per_head.transpose(1, 0, 2)


def reference(q, k, v, u_bias, v_bias, rel_table, w_rel, d_out):
    rel = jnp.dot(rel_table, w_rel.reshape(MODEL_DIM, HEADS_PART * HEAD_DIM), preferred_element_type=jnp.float32)
    rel = rel.astype(jnp.bfloat16).reshape(SEQ_LEN, HEADS_PART, HEAD_DIM)
    q_wide = q.astype(jnp.float32)
    q_u = (q_wide + u_bias).astype(jnp.bfloat16).astype(jnp.float32)
    q_v = (q_wide + v_bias).astype(jnp.bfloat16).astype(jnp.float32)
    out_full, pullback = jax.vjp(attention, q_u, q_v, k.astype(jnp.float32), v.astype(jnp.float32), rel.astype(jnp.float32))
    g_qu, g_qv, g_k, g_v, g_rel = pullback(d_out.astype(jnp.float32))
    d_rel = g_rel.astype(jnp.bfloat16).reshape(SEQ_LEN, HEADS_PART * HEAD_DIM)
    d_w_rel = jnp.dot(rel_table.T, d_rel, preferred_element_type=jnp.float32).reshape(MODEL_DIM, HEADS_PART, HEAD_DIM)
    return (
        out_full.astype(jnp.bfloat16),
        (g_qu + g_qv).astype(jnp.bfloat16),
        g_k.astype(jnp.bfloat16),
        g_v.astype(jnp.bfloat16),
        g_qu.sum(axis=0),
        g_qv.sum(axis=0),
        d_w_rel,
    )
```

```python
import functools
import math
import jax
import jax.numpy as jnp
from jax import lax
from jax.experimental import pallas as pl
from jax.experimental.pallas import tpu as pltpu
from jax.sharding import PartitionSpec as P

F32, BF16 = jnp.float32, jnp.bfloat16
LOG2E = math.log2(math.e)
BQ = 256
BK = 512
NC = BK // 128
PAD = 512
MESH_ID = pl.DeviceIdType.MESH


def dot_nn(a, b):
    return lax.dot_general(a, b, (((1,), (0,)), ((), ())), preferred_element_type=F32)


def dot_nt(a, b):
    return lax.dot_general(a, b, (((1,), (1,)), ((), ())), preferred_element_type=F32)


def aligned(x, m):
    return pl.multiple_of(x, m)


def anti_eye(n):
    rows = lax.broadcasted_iota(jnp.int32, (n, n), 0)
    cols = lax.broadcasted_iota(jnp.int32, (n, n), 1)
    return (rows + cols == n - 1).astype(F32).astype(BF16)


def flip_lanes(x, eye):
    n, w = x.shape[1], eye.shape[0]
    parts = [dot_nn(x[:, s:s + w], eye).astype(BF16) for s in range(0, n, w)]
    return jnp.concatenate(parts[::-1], axis=1)


def reverse_rows(x):
    ix = 7 - lax.broadcasted_iota(jnp.int32, (8, x.shape[1]), 0)
    n = x.shape[0] // 8
    return jnp.concatenate([jnp.take_along_axis(x[(n - 1 - g) * 8:(n - g) * 8], ix, axis=0) for g in range(n)], 0)


def owner_core(rb):
    return lax.rem(rb + rb // 2, 2)


def barrier_all(n):
    me, hp = lax.axis_index('cp'), lax.axis_index('hp')
    bar = pltpu.get_barrier_semaphore()
    for o in range(1, n):
        pl.semaphore_signal(bar, 1, device_id=(hp, lax.rem(me + o, n)), device_id_type=MESH_ID)
    pl.semaphore_wait(bar, n - 1)


def gather_kernel(n, q_in, k_in, v_in, do_in, table, w_rel, q_out, do_out, k_out, v_out, r_out,
                  rel_buf, send_d, send_f, send_q, recv_b, recv_q, loc_b, loc_q):
    me, hp = lax.axis_index('cp'), lax.axis_index('hp')
    chip, core = me // 2, lax.rem(me, 2)
    heads, _, blk = q_in.shape
    per_blk = blk // BQ
    nslot = q_out.shape[1] // BQ
    srcs = (k_in, v_in, rel_buf)
    fulls = (k_out, v_out, r_out)
    barrier_all(n)

    def col(t, b):
        b = (n - 1 - b) if t == 2 else b
        return pl.ds(aligned(b * blk, blk), blk)

    def direct(t, i):
        h = lax.rem(chip + i, heads)
        return pltpu.make_async_remote_copy(
            srcs[t].at[h], fulls[t].at[:, col(t, me)], send_d.at[t, i], recv_b.at[t, me],
            device_id=(hp, 2 * h + core), device_id_type=MESH_ID)

    def forward(t, i):
        b = 2 * lax.rem(chip + i, heads) + core
        src = srcs[t].at[chip] if i == 0 else fulls[t].at[:, col(t, b)]
        return pltpu.make_async_remote_copy(
            src, fulls[t].at[:, col(t, b)], send_f.at[t, i], recv_b.at[t, b],
            device_id=(hp, 2 * chip + 1 - core), device_id_type=MESH_ID)

    def wait_block(t, b):
        pltpu.make_async_remote_copy(
            srcs[t].at[0], fulls[t].at[:, col(t, b)], send_f.at[t, 0], recv_b.at[t, b],
            device_id=(hp, me), device_id_type=MESH_ID).wait_recv()

    def own(t):
        return pltpu.make_async_copy(srcs[t].at[chip], fulls[t].at[:, col(t, me)], loc_b.at[t])

    def rows(t, h, j):
        rb = me * per_blk + j
        src = (q_in, do_in)[t].at[h, :, pl.ds(j * BQ, BQ)]
        dst = (q_out, do_out)[t].at[:, pl.ds(aligned(rb // 2 * BQ, BQ), BQ)]
        return rb, src, dst

    def send_rows(t, i, j, wait):
        h = lax.rem(chip + i, heads)
        rb, src, dst = rows(t, h, j)
        to = 2 * h + owner_core(rb)

        @pl.when(to != me)
        def _():
            c = pltpu.make_async_remote_copy(src, dst, send_q.at[t, i, j], recv_q.at[t, rb // 2],
                                             device_id=(hp, to), device_id_type=MESH_ID)
            c.wait_send() if wait else c.start()

        @pl.when(to == me)
        def _():
            c = pltpu.make_async_copy(src, dst, loc_q.at[t, j])
            c.wait() if wait else c.start()

    for t in (0, 1):
        for i in range(1, heads):
            direct(t, i).start()
        forward(t, 0).start()
        own(t).start()
    rel = dot_nt(w_rel[...], table[...]).astype(BF16)
    rel = flip_lanes(rel, anti_eye(256))
    for h in range(heads):
        rel_buf[h] = rel[h * 64:(h + 1) * 64]
    r_out_pad = r_out.at[:, pl.ds(n * blk, PAD)]
    r_out_pad[...] = jnp.zeros(r_out_pad.shape, BF16)
    for i in range(1, heads):
        direct(2, i).start()
    forward(2, 0).start()
    own(2).start()
    for t in (0, 1):
        for i in range(heads):
            for j in range(per_blk):
                send_rows(t, i, j, False)
    for t in range(3):
        for i in range(1, heads):
            wait_block(t, 2 * lax.rem(chip + i, heads) + core)
            forward(t, i).start()
    for t in range(3):
        own(t).wait()
        for i in range(heads):
            wait_block(t, 2 * i + 1 - core)
            forward(t, i).wait_send()
            if i:
                direct(t, i).wait_send()
    for t in (0, 1):
        for k in range(nslot):
            rb = 2 * k + lax.rem(k + core, 2)

            @pl.when(rb // per_blk != me)
            def _():
                dst = (q_out, do_out)[t].at[:, pl.ds(k * BQ, BQ)]
                pltpu.make_async_remote_copy(
                    (q_in, do_in)[t].at[0, :, pl.ds(0, BQ)], dst, send_q.at[t, 0, 0], recv_q.at[t, k],
                    device_id=(hp, me), device_id_type=MESH_ID).wait_recv()
        for i in range(heads):
            for j in range(per_blk):
                send_rows(t, i, j, True)


def attention_kernel(qT, doT, kT, vT, relF, ub, vb, oT, dqT, dkT, dvT, drF, du, dv, s_scr, r_scr, q_scr):
    me = lax.axis_index('cp')
    chip, core = me // 2, lax.rem(me, 2)
    dim, seq = kT.shape
    nslot = seq // BQ // 2
    scale = dim ** -0.5
    for ref in (dkT, dvT, drF, du, dv):
        ref[...] = jnp.zeros_like(ref)
    eye = anti_eye(BQ)

    def bias_col(ref):
        pick = lax.broadcasted_iota(jnp.int32, ref.shape, 0) == chip
        row = jnp.sum(jnp.where(pick, ref[...], 0.0), axis=0, keepdims=True)
        return jnp.broadcast_to(row, (128, dim)).T[:, :1]

    u_col, v_col = bias_col(ub), bias_col(vb)

    def row_block(k, _):
        rb = 2 * k + lax.rem(k + core, 2)
        tiles = (rb + 2) // 2
        i0 = rb * BQ
        qs = pl.ds(aligned(k * BQ, BQ), BQ)
        q = qT[:, qs].astype(F32)
        quT, qvT = (q + u_col).astype(BF16), (q + v_col).astype(BF16)
        qv = qvT.astype(F32).T.astype(BF16)
        quTr, qvTr, doTr = (flip_lanes(x, eye) for x in (quT, qvT, doT[:, qs]))
        qur, dor = quTr.astype(F32).T.astype(BF16), doTr.astype(F32).T.astype(BF16)
        q_scr[0], q_scr[1], q_scr[2] = qv, qur, dor
        base = seq - i0
        lane = lax.broadcasted_iota(jnp.int32, (128, 128), 1)
        row = lax.broadcasted_iota(jnp.int32, (128, 128), 0)
        past = lane > row

        def skew(t):
            return pltpu.roll(t, 1, 1, stride=1, stride_axis=0)

        t0 = dot_nn(qv, relF[:, pl.ds(aligned(base - 256, 128), 256)])
        r_scr[:, :128], r_scr[:, 128:] = skew(t0[:, :128]), skew(t0[:, 128:])

        def scores(t, mx, last):
            j0 = aligned(t * BK, BK)
            by_offset = dot_nn(q_scr[0], relF[:, pl.ds(aligned(base + j0, 128), BK)])
            content = dot_nn(q_scr[1], kT[:, pl.ds(j0, BK)])
            rolled = [r_scr[:, :128], r_scr[:, 128:]]
            rolled += [skew(by_offset[:, m * 128:(m + 1) * 128]) for m in range(NC)]
            for m in range(NC):
                top = jnp.where(past, rolled[m + 2][:128], rolled[m + 1][:128])
                bot = jnp.where(past, rolled[m + 1][128:], rolled[m][128:])
                s = content[:, m * 128:(m + 1) * 128] + reverse_rows(jnp.concatenate([top, bot], 0))
                s = s * (scale * LOG2E)
                if last:
                    ip = i0 + BQ - 1 - lax.broadcasted_iota(jnp.int32, (BQ, 128), 0)
                    jp = j0 + m * 128 + lax.broadcasted_iota(jnp.int32, (BQ, 128), 1)
                    s = jnp.where(jp > ip, -jnp.inf, s)
                s_scr[t, :, m * 128:(m + 1) * 128] = s
                mx = jnp.maximum(mx, s)
            r_scr[:, :128], r_scr[:, 128:] = rolled[NC], rolled[NC + 1]
            return mx

        mx = jnp.full((BQ, 128), -jnp.inf, F32)
        mx = lax.fori_loop(0, tiles - 1, lambda t, mx: scores(t, mx, False), mx)
        mx = jnp.max(scores(tiles - 1, mx, True), axis=1, keepdims=True)

        def weigh(t, carry):
            total, out = carry
            parts = []
            for m in range(NC):
                p = jnp.exp2(s_scr[t, :, m * 128:(m + 1) * 128] - mx)
                s_scr[t, :, m * 128:(m + 1) * 128] = p
                total = total + p
                parts.append(p.astype(BF16))
            out = out + dot_nt(jnp.concatenate(parts, 1), vT[:, pl.ds(aligned(t * BK, BK), BK)])
            return total, out

        total, out = lax.fori_loop(0, tiles, weigh, (jnp.zeros((BQ, 128), F32), jnp.zeros((BQ, dim), F32)))
        inv = 1.0 / jnp.sum(total, axis=1, keepdims=True)
        out = out * inv
        delta = jnp.sum(q_scr[2].astype(F32) * out, axis=1, keepdims=True)
        oT[:, qs] = flip_lanes(out.T.astype(BF16), eye)

        before = lane < row
        none = jnp.zeros((BQ, 128), BF16)

        def unskew(held, m):
            top = jnp.where(before, held[m + 1][:128], held[m + 2][:128])
            bot = jnp.where(before, held[m][128:], held[m + 1][128:])
            return jnp.concatenate([top, bot], 0)

        def offset_grads(by_offset, us, gv):
            drF[:, us] += dot_nn(qvTr, by_offset)
            return gv + dot_nt(by_offset, relF[:, us])

        def grads(t, carry):
            gu, gv, held_a, held_b = carry
            j0 = aligned(t * BK, BK)
            js = pl.ds(j0, BK)
            dp = dot_nn(q_scr[2], vT[:, js])
            ps, dss, held = [], [], [held_a, held_b]
            for m in range(NC):
                p = s_scr[t, :, m * 128:(m + 1) * 128] * inv
                ds = (p * ((dp[:, m * 128:(m + 1) * 128] - delta) * scale)).astype(BF16)
                ps.append(p.astype(BF16))
                dss.append(ds)
                held.append(pltpu.roll(ds, 0, 1, stride=1, stride_axis=0))
            p_all, ds_all = jnp.concatenate(ps, 1), jnp.concatenate(dss, 1)
            dvT[:, js] += dot_nn(doTr, p_all)
            dkT[:, js] += dot_nn(quTr, ds_all)
            gu = gu + dot_nt(ds_all, kT[:, js])
            by_offset = jnp.concatenate([unskew(held, m) for m in range(NC)], 1)
            gv = offset_grads(by_offset, pl.ds(aligned(base + j0 - 256, 128), BK), gv)
            return gu, gv, held[NC], held[NC + 1]

        zero = jnp.zeros((BQ, dim), F32)
        gu, gv, held_a, held_b = lax.fori_loop(0, tiles, grads, (zero, zero, none, none))
        held = [held_a, held_b, none, none]
        rest = jnp.concatenate([unskew(held, 0), unskew(held, 1)], 1)
        gv = offset_grads(rest, pl.ds(aligned(base + tiles * BK - 256, 128), 256), gv)
        dqT[:, qs] = flip_lanes((gu + gv).T.astype(BF16), eye)
        du[...] += jnp.sum(gu.reshape(BQ // 8, 8, dim), axis=0)
        dv[...] += jnp.sum(gv.reshape(BQ // 8, 8, dim), axis=0)
        return 0

    lax.fori_loop(0, nslot, row_block, 0)


def scatter_kernel(n, oT, dqT, dkT, dvT, drF, du, dv, table, o_out, dq_out, dk_out, dv_out, bias_out, dw_out,
                   pair_buf, send_buf, dr_buf, bias_buf, half_in, half_sum, part_in, w_acc,
                   send_p, recv_p, send_q, recv_q, loc_q, send_s, recv_s, send_b, recv_b, send_w, recv_w):
    me, hp = lax.axis_index('cp'), lax.axis_index('hp')
    chip, core = me // 2, lax.rem(me, 2)
    mate = 2 * chip + 1 - core
    heads, dim, blk = o_out.shape
    per_blk = blk // BQ
    nslot = oT.shape[1] // BQ
    parts = (dkT, dvT, drF)
    sinks = (dk_out, dv_out, dr_buf)

    def remote(src, dst, ss, rs, to):
        return pltpu.make_async_remote_copy(src, dst, ss, rs, device_id=(hp, to), device_id_type=MESH_ID)

    def col(t, b):
        b = (n - 1 - b) if t == 2 else b
        return pl.ds(aligned(b * blk, blk), blk)

    bias_buf[me, 0] = jnp.sum(du[...], axis=0, keepdims=True) + jnp.zeros((8, dim), F32)
    bias_buf[me, 1] = jnp.sum(dv[...], axis=0, keepdims=True) + jnp.zeros((8, dim), F32)
    barrier_all(n)

    def pair(t, i):
        return remote(parts[t].at[:, col(t, 2 * i + 1 - core)], pair_buf.at[t, i], send_p.at[t, i], recv_p.at[t, i], mate)

    for t in (2, 0, 1):
        for i in range(heads):
            pair(t, i).start()

    def rows(t, k, wait):
        rb = 2 * k + lax.rem(k + core, 2)
        to = rb // per_blk
        src = (oT, dqT)[t].at[:, pl.ds(k * BQ, BQ)]
        dst = (o_out, dq_out)[t].at[chip, :, pl.ds(aligned(lax.rem(rb, per_blk) * BQ, BQ), BQ)]

        @pl.when(to != me)
        def _():
            c = remote(src, dst, send_q.at[t, k], recv_q.at[t, chip, lax.rem(rb, per_blk)], to)
            c.wait_send() if wait else c.start()

        @pl.when(to == me)
        def _():
            c = pltpu.make_async_copy(src, dst, loc_q.at[t, lax.rem(rb, per_blk)])
            c.wait() if wait else c.start()

    def bias(o):
        return remote(bias_buf.at[me], bias_buf.at[me], send_b.at[o], recv_b.at[me], lax.rem(me + o, n))

    for o in range(1, n):
        bias(o).start()

    def sink(t, i):
        b = lax.rem(chip + i, heads)
        return remote(send_buf.at[t, b], sinks[t].at[chip], send_s.at[t, i], recv_s.at[t, chip], 2 * b + core)

    def combine(t):
        for i in (1, 2, 3, 0):
            b = lax.rem(chip + i, heads)
            remote(parts[t].at[:, col(t, 2 * b + core)], pair_buf.at[t, b], send_p.at[t, 0], recv_p.at[t, b], mate).wait_recv()
            both = (parts[t][:, col(t, 2 * b + core)] + pair_buf[t, b]).astype(BF16)
            if i:
                send_buf[t, b] = both
                sink(t, i).start()
            else:
                sinks[t][chip] = both

    combine(2)
    for k in range(nslot):
        rows(0, k, False)
    for k in range(nslot):
        rows(1, k, False)
    combine(0)
    combine(1)
    for i in range(1, heads):
        h = lax.rem(chip + i, heads)
        remote(send_buf.at[2, 0], dr_buf.at[h], send_s.at[2, 0], recv_s.at[2, h], me).wait_recv()
    eye = anti_eye(256)
    for h in range(heads):
        w_acc[h * dim:(h + 1) * dim] = dot_nn(flip_lanes(dr_buf[h], eye), table[...])
    half = heads * dim // 2
    piece = half // heads

    def swap():
        return remote(w_acc.at[pl.ds(aligned((1 - core) * half, half), half)], half_in, send_w.at[0], recv_w.at[0], mate)

    swap().start()
    swap().wait()
    half_sum[...] = w_acc[pl.ds(aligned(core * half, half), half)] + half_in[...]

    def spread(i):
        z = lax.rem(chip + i, heads)
        return remote(half_sum.at[pl.ds(aligned(z * piece, piece), piece)], part_in.at[i], send_w.at[i], recv_w.at[i], 2 * z + core)

    for i in range(1, heads):
        spread(i).start()
    for i in range(1, heads):
        spread(i).wait()
    mine = half_sum[pl.ds(aligned(chip * piece, piece), piece)]
    for i in range(1, heads):
        mine = mine + part_in[i]
    half_in[pl.ds(0, piece)] = mine

    def place(c, z):
        return dw_out.at[pl.ds(aligned(c * half + z * piece, piece), piece)]

    def collect(i):
        z = lax.rem(chip + i, heads)
        return remote(half_in.at[pl.ds(0, piece)], place(core, chip), send_w.at[4 + i], recv_w.at[4 + chip], 2 * z + core)

    def hand_over(i):
        z = lax.rem(chip + i, heads)
        src = half_in.at[pl.ds(0, piece)] if i == 0 else place(core, z)
        return remote(src, place(core, z), send_w.at[8 + i], recv_w.at[8 + z], mate)

    for i in range(1, heads):
        collect(i).start()
    hand_over(0).start()
    place(core, chip)[...] = mine
    for i in range(1, heads):
        z = lax.rem(chip + i, heads)
        remote(half_in.at[pl.ds(0, piece)], place(core, z), send_w.at[0], recv_w.at[4 + z], me).wait_recv()
        hand_over(i).start()
    for o in range(1, n):
        b = lax.rem(me + o, n)
        remote(bias_buf.at[b], bias_buf.at[b], send_b.at[0], recv_b.at[b], me).wait_recv()
    for h in range(heads):
        bias_out[h] = bias_buf[2 * h] + bias_buf[2 * h + 1]
    for i in range(heads):
        remote(half_in.at[pl.ds(0, piece)], place(1 - core, i), send_w.at[0], recv_w.at[8 + i], me).wait_recv()
        hand_over(i).wait_send()
        if i:
            collect(i).wait_send()
    for o in range(1, n):
        bias(o).wait_send()
    for t in range(3):
        for i in range(heads):
            pair(t, i).wait_send()
            if i:
                h = lax.rem(chip + i, heads)
                sink(t, i).wait_send()
                if t < 2:
                    remote(send_buf.at[t, 0], sinks[t].at[h], send_s.at[t, 0], recv_s.at[t, h], me).wait_recv()
    for t in (0, 1):
        for k in range(nslot):
            rows(t, k, True)
        for h in range(heads):
            for j in range(per_blk):
                rb = me * per_blk + j

                @pl.when(2 * h + owner_core(rb) != me)
                def _():
                    remote((oT, dqT)[t].at[:, pl.ds(0, BQ)], (o_out, dq_out)[t].at[h, :, pl.ds(j * BQ, BQ)],
                           send_q.at[t, 0], recv_q.at[t, h, j], me).wait_recv()


def solution(mesh):
    n = mesh.shape['cp']
    seq_spec, head_spec, weight_spec = P('cp', 'hp', None), P('hp', None), P(None, 'hp', None)
    vmem = pl.BlockSpec(memory_space=pltpu.VMEM)
    hbm = pl.BlockSpec(memory_space=pl.ANY)
    dma, sds = pltpu.SemaphoreType.DMA, jax.ShapeDtypeStruct

    def local_fn(q, k, v, u_bias, v_bias, rel_table, w_rel, d_out):
        blk, heads, dim = q.shape
        seq = n * blk
        rows = seq // 2
        nslot = rows // BQ
        per_blk = blk // BQ
        qT, kT, vT, doT = (x.transpose(1, 2, 0) for x in (q, k, v, d_out))
        wT = w_rel.transpose(1, 2, 0).reshape(heads * dim, -1)
        model = wT.shape[1]
        q_h, do_h, k_h, v_h, r_h = pl.pallas_call(
            functools.partial(gather_kernel, n),
            out_shape=[sds((dim, rows), BF16), sds((dim, rows), BF16), sds((dim, seq), BF16), sds((dim, seq), BF16),
                       sds((dim, seq + PAD), BF16)],
            in_specs=[vmem] * 6, out_specs=[vmem] * 5,
            scratch_shapes=[pltpu.VMEM((heads, dim, blk), BF16), dma((3, heads)), dma((3, heads)), dma((2, heads, per_blk)),
                            dma((3, n)), dma((2, nslot)), dma((3,)), dma((2, per_blk))],
            compiler_params=pltpu.CompilerParams(collective_id=0, has_side_effects=True),
            name='gather_heads',
        )(qT, kT, vT, doT, rel_table, wT)
        oT, dqT, dkT, dvT, drF, du, dv = pl.pallas_call(
            attention_kernel,
            out_shape=[sds((dim, rows), BF16), sds((dim, rows), BF16), sds((dim, seq), F32), sds((dim, seq), F32),
                       sds((dim, seq + PAD), F32), sds((8, dim), F32), sds((8, dim), F32)],
            in_specs=[vmem] * 7, out_specs=[vmem] * 7,
            scratch_shapes=[pltpu.VMEM((seq // BK, BQ, BK), F32), pltpu.VMEM((BQ, 256), F32), pltpu.VMEM((3, BQ, dim), BF16)],
            compiler_params=pltpu.CompilerParams(vmem_limit_bytes=56 << 20),
            name='attention',
        )(q_h, do_h, k_h, v_h, r_h, u_bias, v_bias)
        o, dq, dk, dvv, bias, dw = pl.pallas_call(
            functools.partial(scatter_kernel, n),
            out_shape=[sds((heads, dim, blk), BF16)] * 4 + [sds((heads, 2, 8, dim), F32), sds((heads * dim, model), F32)],
            in_specs=[vmem] * 8, out_specs=[vmem] * 6,
            scratch_shapes=[pltpu.VMEM((3, heads, dim, blk), F32), pltpu.VMEM((3, heads, dim, blk), BF16),
                            pltpu.VMEM((heads, dim, blk), BF16), pltpu.VMEM((n, 2, 8, dim), F32),
                            pltpu.VMEM((heads * dim // 2, model), F32), pltpu.VMEM((heads * dim // 2, model), F32),
                            pltpu.VMEM((heads, heads * dim // 8, model), F32), pltpu.VMEM((heads * dim, model), F32),
                            dma((3, heads)), dma((3, heads)), dma((2, nslot)), dma((2, heads, per_blk)), dma((2, per_blk)),
                            dma((3, heads)), dma((3, heads)), dma((n,)), dma((n,)), dma((12,)), dma((12,))],
            compiler_params=pltpu.CompilerParams(collective_id=1, has_side_effects=True, vmem_limit_bytes=56 << 20),
            name='scatter_rows',
        )(oT, dqT, dkT, dvT, drF, du, dv, rel_table)
        back = lambda x: x.transpose(2, 0, 1)
        return (back(o), back(dq), back(dk), back(dvv), bias[:, 0, 0], bias[:, 1, 0],
                back(dw.reshape(heads, dim, model)))

    return jax.shard_map(
        local_fn, mesh=mesh,
        in_specs=(seq_spec, seq_spec, seq_spec, head_spec, head_spec, P('cp', None), weight_spec, seq_spec),
        out_specs=(seq_spec, seq_spec, seq_spec, seq_spec, head_spec, head_spec, weight_spec),
        check_vma=False,
    )
```

```python
import functools
import math
import jax
import jax.numpy as jnp
from jax import lax
from jax.experimental import pallas as pl
from jax.experimental.pallas import tpu as pltpu
from jax.sharding import PartitionSpec as P

F32, BF16 = jnp.float32, jnp.bfloat16
LOG2E = math.log2(math.e)
BQ = 256
BK = 512
NC = BK // 128
PAD = 512
KX = 80
GROUP = 3
UNROLL = 3
MESH_ID = pl.DeviceIdType.MESH


def dot_nn(a, b):
    return lax.dot_general(a, b, (((1,), (0,)), ((), ())), preferred_element_type=F32)


def dot_nt(a, b):
    return lax.dot_general(a, b, (((1,), (1,)), ((), ())), preferred_element_type=F32)


def aligned(x, m):
    return pl.multiple_of(x, m)


def anti_eye(n):
    rows = lax.broadcasted_iota(jnp.int32, (n, n), 0)
    cols = lax.broadcasted_iota(jnp.int32, (n, n), 1)
    return (rows + cols == n - 1).astype(F32).astype(BF16)


def flip_lanes(x, eye):
    n, w = x.shape[1], eye.shape[0]
    parts = [dot_nn(x[:, s:s + w], eye).astype(BF16) for s in range(0, n, w)]
    return jnp.concatenate(parts[::-1], axis=1)


def reverse_rows(x):
    ix = 7 - lax.broadcasted_iota(jnp.int32, (8, x.shape[1]), 0)
    n = x.shape[0] // 8
    return jnp.concatenate([jnp.take_along_axis(x[(n - 1 - g) * 8:(n - g) * 8], ix, axis=0) for g in range(n)], 0)


def owner_core(rb):
    return lax.rem(rb + rb // 2, 2)


def remote_copy(src, dst, send_sem, recv_sem, to):
    return pltpu.make_async_remote_copy(src, dst, send_sem, recv_sem, device_id=(lax.axis_index('hp'), to),
                                        device_id_type=MESH_ID)


def barrier_all(n):
    me, hp = lax.axis_index('cp'), lax.axis_index('hp')
    bar = pltpu.get_barrier_semaphore()
    for o in range(1, n):
        pl.semaphore_signal(bar, 1, device_id=(hp, lax.rem(me + o, n)), device_id_type=MESH_ID)
    pl.semaphore_wait(bar, n - 1)


def rel_kernel(table, w_rel, out):
    rel = dot_nt(w_rel[...], table[...]).astype(BF16)
    rel = flip_lanes(rel, anti_eye(256))
    heads, dim, _ = out.shape
    for h in range(heads):
        out[h] = rel[h * dim:(h + 1) * dim]


def attention_kernel(n, q_in, k_in, v_in, do_in, r_in, ub, vb,
                     o_out, dq_out, dk_out, dv_out, dr_out, du, dv,
                     qT, doT, kT, vT, relX, oT, dqT, dkT, dvT, drF,
                     s_all, q_off, q_row, do_row, q_col, qo_col, do_col, mx, total, o_acc, gu, gv, r_scr, h_scr,
                     pair_buf, send_buf,
                     send_d, send_f, send_q, recv_b, recv_q, loc_b, loc_q,
                     send_o, recv_o, loc_o, send_p, recv_p, send_s, recv_s, loc_s):
    me = lax.axis_index('cp')
    chip, core = me // 2, lax.rem(me, 2)
    mate = 2 * chip + 1 - core
    heads, dim, blk = q_in.shape
    seq = n * blk
    per_blk = blk // BQ
    groups = n // 2
    nslot = qT.shape[1] // BQ
    scale = dim ** -0.5
    barrier_all(n)

    srcs, fulls = (r_in, k_in, v_in), (relX, kT, vT)

    def col(t, b, flipped):
        b = (n - 1 - b) if t == flipped else b
        return pl.ds(aligned(b * blk, blk), blk)

    def full_at(t, b):
        return fulls[t].at[pl.ds(0, dim), col(t, b, 0)]

    def direct(t, i):
        h = lax.rem(chip + i, heads)
        return remote_copy(srcs[t].at[h], full_at(t, me), send_d.at[t, i], recv_b.at[t, me], 2 * h + core)

    def own(t):
        return pltpu.make_async_copy(srcs[t].at[chip], full_at(t, me), loc_b.at[t])

    def to_mate(t):
        return remote_copy(srcs[t].at[chip], full_at(t, me), send_f.at[t, chip], recv_b.at[t, me], mate)

    def forward(t, g):
        b = 2 * g + core
        return remote_copy(full_at(t, b), full_at(t, b), send_f.at[t, g], recv_b.at[t, b], mate)

    def landed(t, b):
        remote_copy(srcs[t].at[0], full_at(t, b), send_f.at[t, 0], recv_b.at[t, b], me).wait_recv()

    def pass_on(t, g):
        @pl.when(g != chip)
        def _():
            landed(t, 2 * g + core)
            forward(t, g).start()

        @pl.when(g == chip)
        def _():
            own(t).wait()

    def from_mate(t, g):
        landed(t, 2 * g + 1 - core)

    def row_copy(t, i, j, wait):
        h = lax.rem(chip + i, heads)
        rb = me * per_blk + j
        src = (q_in, do_in)[t].at[h, :, pl.ds(j * BQ, BQ)]
        dst = (qT, doT)[t].at[:, pl.ds(aligned(rb // 2 * BQ, BQ), BQ)]
        to = 2 * h + owner_core(rb)

        @pl.when(to != me)
        def _():
            c = remote_copy(src, dst, send_q.at[t, i, j], recv_q.at[t, rb // 2], to)
            c.wait_send() if wait else c.start()

        @pl.when(to == me)
        def _():
            c = pltpu.make_async_copy(src, dst, loc_q.at[t, j])
            c.wait() if wait else c.start()

    def row_block(k):
        return 2 * k + lax.rem(k + core, 2)

    def row_landed(t, k):
        src = (q_in, do_in)[t].at[0, :, pl.ds(0, BQ)]
        dst = (qT, doT)[t].at[:, pl.ds(aligned(k * BQ, BQ), BQ)]
        rb = row_block(k)

        @pl.when(rb // per_blk != me)
        def _():
            remote_copy(src, dst, send_q.at[t, 0, 0], recv_q.at[t, k], me).wait_recv()

        @pl.when(rb // per_blk == me)
        def _():
            pltpu.make_async_copy(src, dst, loc_q.at[t, lax.rem(rb, per_blk)]).wait()

    order = (1, 3, 2)
    for t in (0, 1):
        to_mate(t).start()
        own(t).start()
    for i in order:
        direct(0, i).start()
        direct(1, i).start()
        for j in range(per_blk):
            row_copy(0, i, j, False)
    for j in range(per_blk):
        row_copy(0, 0, j, False)
    to_mate(2).start()
    own(2).start()
    for i in order:
        direct(2, i).start()
    for i in order + (0,):
        for j in range(per_blk):
            row_copy(1, i, j, False)

    for ref in (dkT, dvT, drF, du, dv, total, o_acc, h_scr):
        ref[...] = jnp.zeros_like(ref)
    mx[...] = jnp.full(mx.shape, -jnp.inf, F32)
    relX[pl.ds(0, dim), pl.ds(seq, PAD)] = jnp.zeros((dim, PAD), BF16)
    first = lax.broadcasted_iota(jnp.int32, (KX - dim, PAD), 0) == 0
    relX[pl.ds(dim, KX - dim), pl.ds(0, seq)] = jnp.zeros((KX - dim, seq), BF16)
    relX[pl.ds(dim, KX - dim), pl.ds(seq, PAD)] = jnp.where(first, -jnp.inf, 0.0).astype(BF16)
    ones_col = (lax.broadcasted_iota(jnp.int32, (BQ, KX - dim), 1) == 0).astype(F32).astype(BF16)
    eye = anti_eye(BQ)
    lane = lax.broadcasted_iota(jnp.int32, (128, 128), 1)
    row = lax.broadcasted_iota(jnp.int32, (128, 128), 0)
    past, before = lane > row, lane < row

    def bias_col(ref):
        pick = lax.broadcasted_iota(jnp.int32, ref.shape, 0) == chip
        r = jnp.sum(jnp.where(pick, ref[...], 0.0), axis=0, keepdims=True)
        return jnp.broadcast_to(r, (128, dim)).T[:, :1]

    u_col, v_col = bias_col(ub), bias_col(vb)

    def skew(t):
        return pltpu.roll(t, 1, 1, stride=1, stride_axis=0)

    def slot_cols(k):
        return pl.ds(aligned(k * BQ, BQ), BQ)

    def transposed(x):
        return x.astype(F32).T.astype(BF16)

    def prepare(k, i):
        q = qT[:, slot_cols(k)].astype(F32)
        quT, qvT = (q + u_col).astype(BF16), (q + v_col).astype(BF16)
        q_off[k] = jnp.concatenate([transposed(qvT), ones_col], 1)
        q_col[k] = flip_lanes(quT, eye)
        q_row[k] = transposed(q_col[k])
        qo_col[k] = flip_lanes(qvT, eye)
        base = seq - row_block(k) * BQ
        t0 = dot_nn(q_off[k], relX[:, pl.ds(aligned(base - 256, 128), 256)])
        r_scr[i, :, :128], r_scr[i, :, 128:] = skew(t0[:, :128]), skew(t0[:, 128:])

    def scores(tile, k, t):
        j0 = aligned(t * BK, BK)
        base = seq - row_block(k) * BQ
        by_offset = dot_nn(q_off[k], relX[:, pl.ds(aligned(base + j0, 128), BK)])
        content = dot_nn(q_row[k], kT[:, pl.ds(j0, BK)])
        ri = jnp.where(t == 0, lax.rem(k, GROUP), GROUP)
        rolled = [r_scr[ri, :, :128], r_scr[ri, :, 128:]]
        rolled += [skew(by_offset[:, m * 128:(m + 1) * 128]) for m in range(NC)]
        top_s = mx[k]
        for m in range(NC):
            top = jnp.where(past, rolled[m + 2][:128], rolled[m + 1][:128])
            bot = jnp.where(past, rolled[m + 1][128:], rolled[m][128:])
            s = content[:, m * 128:(m + 1) * 128] + reverse_rows(jnp.concatenate([top, bot], 0))
            s = s * (scale * LOG2E)
            s_all[tile, :, m * 128:(m + 1) * 128] = s
            top_s = jnp.maximum(top_s, s)
        mx[k] = top_s
        r_scr[GROUP, :, :128], r_scr[GROUP, :, 128:] = rolled[NC], rolled[NC + 1]

    def weigh(tile, k, t):
        top_s, tot = mx[k], total[k]
        parts = []
        for m in range(NC):
            p = jnp.exp2(s_all[tile, :, m * 128:(m + 1) * 128] - top_s)
            s_all[tile, :, m * 128:(m + 1) * 128] = p
            tot = tot + p
            parts.append(p.astype(BF16))
        total[k] = tot
        o_acc[k] += dot_nt(jnp.concatenate(parts, 1), vT[:, pl.ds(aligned(t * BK, BK), BK)])

    def finish_rows(k):
        do_col[k] = flip_lanes(doT[:, slot_cols(k)], eye)
        do_row[k] = transposed(do_col[k])
        inv = 1.0 / jnp.sum(total[k], axis=1, keepdims=True)
        out = o_acc[k] * inv
        delta = jnp.sum(do_row[k].astype(F32) * out, axis=1, keepdims=True)
        total[k] = jnp.broadcast_to(inv, (BQ, 128))
        mx[k] = jnp.broadcast_to(delta, (BQ, 128))
        oT[:, slot_cols(k)] = flip_lanes(out.T.astype(BF16), eye)

    def grads(tile, k, t):
        j0 = aligned(t * BK, BK)
        base = seq - row_block(k) * BQ
        js, us = pl.ds(j0, BK), pl.ds(aligned(base + j0 - 256, 128), BK)
        i = lax.rem(k, GROUP)
        dp = dot_nn(do_row[k], vT[:, js])
        inv, delta = total[k], mx[k]
        hi = jnp.where(t == 0, 0, 1)
        ps, dss, held = [], [], [h_scr[hi, :, :128], h_scr[hi, :, 128:]]
        for m in range(NC):
            p = s_all[tile, :, m * 128:(m + 1) * 128] * inv
            ds = (p * ((dp[:, m * 128:(m + 1) * 128] - delta) * scale)).astype(BF16)
            ps.append(p.astype(BF16))
            dss.append(ds)
            held.append(pltpu.roll(ds, 0, 1, stride=1, stride_axis=0))
        h_scr[1, :, :128], h_scr[1, :, 128:] = held[NC], held[NC + 1]
        by_offset = []
        for m in range(NC):
            top = jnp.where(before, held[m + 1][:128], held[m + 2][:128])
            bot = jnp.where(before, held[m][128:], held[m + 1][128:])
            by_offset.append(jnp.concatenate([top, bot], 0))
        p_all, ds_all, by_offset = (jnp.concatenate(x, 1) for x in (ps, dss, by_offset))
        dvT[:, js] += dot_nn(do_col[k], p_all)
        dkT[:, js] += dot_nn(q_col[k], ds_all)
        drF[:, us] += dot_nn(qo_col[k], by_offset)
        gu[i] += dot_nt(ds_all, kT[:, js])
        gv[i] += dot_nt(by_offset, relX[:dim, us])

    def over_tiles(step, g):
        k0 = GROUP * g
        tile0 = k0 * (k0 + 1) // 2

        def some(i, kt):
            k, t = kt
            for u in range(UNROLL):
                step(tile0 + UNROLL * i + u, k, t)
                last = t == k
                k, t = jnp.where(last, k + 1, k), jnp.where(last, 0, t + 1)
            return k, t

        lax.fori_loop(0, (GROUP * GROUP * g + GROUP * (GROUP + 1) // 2) // UNROLL, some, (k0, 0))

    def each(fn):
        lax.fori_loop(0, groups, lambda g, c: (fn(g), c)[1], 0)

    def forward_scores(g):
        for t in (0, 1):
            pass_on(t, g)
        for t in (0, 1):
            from_mate(t, g)
        for i in range(GROUP):
            row_landed(0, GROUP * g + i)
        for i in range(GROUP):
            prepare(GROUP * g + i, i)
        over_tiles(scores, g)

    each(forward_scores)
    each(lambda g: pass_on(2, g))

    def row_max(g):
        for i in range(GROUP):
            k = GROUP * g + i
            mx[k] = jnp.broadcast_to(jnp.max(mx[k], axis=1, keepdims=True), (BQ, 128))

    each(row_max)

    def weigh_group(g):
        from_mate(2, g)
        over_tiles(weigh, g)

    each(weigh_group)

    def out_rows(t, k, wait):
        rb = row_block(k)
        to, j = rb // per_blk, lax.rem(rb, per_blk)
        src = (oT, dqT)[t].at[:, slot_cols(k)]
        dst = (o_out, dq_out)[t].at[chip, :, pl.ds(aligned(j * BQ, BQ), BQ)]

        @pl.when(to != me)
        def _():
            c = remote_copy(src, dst, send_o.at[t, k], recv_o.at[t, chip, j], to)
            c.wait_send() if wait else c.start()

        @pl.when(to == me)
        def _():
            c = pltpu.make_async_copy(src, dst, loc_o.at[t, j])
            c.wait() if wait else c.start()

    def finish_group(g):
        for i in range(GROUP):
            row_landed(1, GROUP * g + i)
        for i in range(GROUP):
            finish_rows(GROUP * g + i)
        for i in range(GROUP):
            out_rows(0, GROUP * g + i, False)

    each(finish_group)

    parts, sinks = (drF, dkT, dvT), (dr_out, dk_out, dv_out)

    def pair(t, g):
        return remote_copy(parts[t].at[:, col(t, 2 * g + 1 - core, 0)], pair_buf.at[t, g], send_p.at[t, g], recv_p.at[t, g], mate)

    def sink(t, g):
        return remote_copy(send_buf.at[t, g], sinks[t].at[chip], send_s.at[t, g], recv_s.at[t, chip], 2 * g + core)

    def keep(t, g):
        return pltpu.make_async_copy(send_buf.at[t, g], sinks[t].at[chip], loc_s.at[t])

    def combine(g):
        for t in range(3):
            mine = col(t, 2 * g + core, 0)
            remote_copy(parts[t].at[:, mine], pair_buf.at[t, g], send_p.at[t, g], recv_p.at[t, g], mate).wait_recv()
            send_buf[t, g] = (parts[t][:, mine] + pair_buf[t, g]).astype(BF16)
        for t in range(3):
            @pl.when(g != chip)
            def _():
                sink(t, g).start()

            @pl.when(g == chip)
            def _():
                keep(t, g).start()

    def backward_group(step):
        g = groups - 1 - step
        gu[...] = jnp.zeros_like(gu)
        gv[...] = jnp.zeros_like(gv)
        over_tiles(grads, g)
        for t in range(3):
            pair(t, g).start()
        for i in range(GROUP):
            dqT[:, slot_cols(GROUP * g + i)] = flip_lanes((gu[i] + gv[i]).T.astype(BF16), eye)
            du[...] += jnp.sum(gu[i].reshape(BQ // 8, 8, dim), axis=0)
            dv[...] += jnp.sum(gv[i].reshape(BQ // 8, 8, dim), axis=0)
        for i in range(GROUP):
            out_rows(1, GROUP * g + i, False)
        combine(g)

    each(backward_group)

    for t in range(3):
        for i in range(heads):
            h = lax.rem(chip + i, heads)
            pair(t, i).wait_send()
            if i:
                direct(t, i).wait_send()
                sink(t, h).wait_send()
                remote_copy(send_buf.at[t, 0], sinks[t].at[h], send_s.at[t, 0], recv_s.at[t, h], me).wait_recv()
                forward(t, h).wait_send()
            else:
                to_mate(t).wait_send()
                keep(t, chip).wait()
    for t in (0, 1):
        for i in range(heads):
            for j in range(per_blk):
                to = 2 * lax.rem(chip + i, heads) + owner_core(me * per_blk + j)

                @pl.when(to != me)
                def _():
                    remote_copy((q_in, do_in)[t].at[0, :, pl.ds(0, BQ)], (qT, doT)[t].at[:, pl.ds(0, BQ)],
                                send_q.at[t, i, j], recv_q.at[t, 0], to).wait_send()
        for k in range(nslot):
            out_rows(t, k, True)
        for h in range(heads):
            for j in range(per_blk):
                @pl.when(2 * h + owner_core(me * per_blk + j) != me)
                def _():
                    remote_copy((oT, dqT)[t].at[:, pl.ds(0, BQ)], (o_out, dq_out)[t].at[h, :, pl.ds(j * BQ, BQ)],
                                send_o.at[t, 0], recv_o.at[t, h, j], me).wait_recv()


def table_grad_kernel(n, dr, du, dv, table, bias_out, dw_out, bias_buf, half_in, half_sum, part_in, w_acc,
                      send_b, recv_b, send_w, recv_w):
    me = lax.axis_index('cp')
    chip, core = me // 2, lax.rem(me, 2)
    mate = 2 * chip + 1 - core
    heads, dim, _ = dr.shape
    bias_buf[me, 0] = jnp.sum(du[...], axis=0, keepdims=True) + jnp.zeros((8, dim), F32)
    bias_buf[me, 1] = jnp.sum(dv[...], axis=0, keepdims=True) + jnp.zeros((8, dim), F32)
    eye = anti_eye(256)
    for h in range(heads):
        w_acc[h * dim:(h + 1) * dim] = dot_nn(flip_lanes(dr[h], eye), table[...])
    barrier_all(n)

    def bias(o):
        return remote_copy(bias_buf.at[me], bias_buf.at[me], send_b.at[o], recv_b.at[me], lax.rem(me + o, n))

    half = heads * dim // 2
    piece = half // heads

    def swap():
        return remote_copy(w_acc.at[pl.ds(aligned((1 - core) * half, half), half)], half_in, send_w.at[0], recv_w.at[0], mate)

    swap().start()
    for o in range(1, n):
        bias(o).start()
    swap().wait()
    half_sum[...] = w_acc[pl.ds(aligned(core * half, half), half)] + half_in[...]

    def spread(i):
        z = lax.rem(chip + i, heads)
        return remote_copy(half_sum.at[pl.ds(aligned(z * piece, piece), piece)], part_in.at[i], send_w.at[i], recv_w.at[i], 2 * z + core)

    for i in range(1, heads):
        spread(i).start()
    for i in range(1, heads):
        spread(i).wait()
    mine = half_sum[pl.ds(aligned(chip * piece, piece), piece)]
    for i in range(1, heads):
        mine = mine + part_in[i]
    half_in[pl.ds(0, piece)] = mine
    whole = half_in.at[pl.ds(0, piece)]

    def place(c, z):
        return dw_out.at[pl.ds(aligned(c * half + z * piece, piece), piece)]

    def collect(i):
        z = lax.rem(chip + i, heads)
        return remote_copy(whole, place(core, chip), send_w.at[4 + i], recv_w.at[4 + chip], 2 * z + core)

    def hand_over(i):
        z = lax.rem(chip + i, heads)
        return remote_copy(whole if i == 0 else place(core, z), place(core, z), send_w.at[8 + i], recv_w.at[8 + z], mate)

    for i in range(1, heads):
        collect(i).start()
    hand_over(0).start()
    place(core, chip)[...] = mine
    for i in range(1, heads):
        z = lax.rem(chip + i, heads)
        remote_copy(whole, place(core, z), send_w.at[0], recv_w.at[4 + z], me).wait_recv()
        hand_over(i).start()
    for o in range(1, n):
        b = lax.rem(me + o, n)
        remote_copy(bias_buf.at[b], bias_buf.at[b], send_b.at[0], recv_b.at[b], me).wait_recv()
    for h in range(heads):
        bias_out[h] = bias_buf[2 * h] + bias_buf[2 * h + 1]
    for i in range(heads):
        remote_copy(whole, place(1 - core, i), send_w.at[0], recv_w.at[8 + i], me).wait_recv()
        hand_over(i).wait_send()
        if i:
            collect(i).wait_send()
    for o in range(1, n):
        bias(o).wait_send()


def solution(mesh):
    n = mesh.shape['cp']
    seq_spec, head_spec, weight_spec = P('cp', 'hp', None), P('hp', None), P(None, 'hp', None)
    vmem = pl.BlockSpec(memory_space=pltpu.VMEM)
    hbm = pl.BlockSpec(memory_space=pl.ANY)
    dma, sds, buf = pltpu.SemaphoreType.DMA, jax.ShapeDtypeStruct, pltpu.VMEM

    def local_fn(q, k, v, u_bias, v_bias, rel_table, w_rel, d_out):
        blk, heads, dim = q.shape
        seq = n * blk
        rows = seq // 2
        nslot = rows // BQ
        per_blk = blk // BQ
        tiles = nslot * (nslot + 1) // 2
        qT, kT, vT, doT = (x.transpose(1, 2, 0) for x in (q, k, v, d_out))
        wT = w_rel.transpose(1, 2, 0).reshape(heads * dim, -1)
        model = wT.shape[1]
        relT = pl.pallas_call(rel_kernel, out_shape=sds((heads, dim, blk), BF16), in_specs=[vmem] * 2, out_specs=vmem,
                              name='rel_project')(rel_table, wT)
        o, dq, dk, dvv, dr, du, dv = pl.pallas_call(
            functools.partial(attention_kernel, n),
            out_shape=[sds((heads, dim, blk), BF16)] * 5 + [sds((8, dim), F32)] * 2,
            in_specs=[hbm] * 5 + [vmem] * 2, out_specs=[hbm] * 5 + [vmem] * 2,
            scratch_shapes=[
                buf((dim, rows), BF16), buf((dim, rows), BF16), buf((dim, seq), BF16), buf((dim, seq), BF16), buf((KX, seq + PAD), BF16),
                buf((dim, rows), BF16), buf((dim, rows), BF16), buf((dim, seq), F32), buf((dim, seq), F32), buf((dim, seq + PAD), F32),
                buf((tiles, BQ, BK), F32), buf((nslot, BQ, KX), BF16), buf((nslot, BQ, dim), BF16), buf((nslot, BQ, dim), BF16),
                buf((nslot, dim, BQ), BF16), buf((nslot, dim, BQ), BF16), buf((nslot, dim, BQ), BF16),
                buf((nslot, BQ, 128), F32), buf((nslot, BQ, 128), F32), buf((nslot, BQ, dim), F32),
                buf((GROUP, BQ, dim), F32), buf((GROUP, BQ, dim), F32), buf((GROUP + 1, BQ, 256), F32), buf((2, BQ, 256), BF16),
                buf((3, heads, dim, blk), F32), buf((3, heads, dim, blk), BF16),
                dma((3, heads)), dma((3, heads)), dma((2, heads, per_blk)), dma((3, n)), dma((2, nslot)), dma((3,)), dma((2, per_blk)),
                dma((2, nslot)), dma((2, heads, per_blk)), dma((2, per_blk)), dma((3, heads)), dma((3, heads)),
                dma((3, heads)), dma((3, heads)), dma((3,))],
            compiler_params=pltpu.CompilerParams(collective_id=0, has_side_effects=True, vmem_limit_bytes=67043328),
            name='attention',
        )(qT, kT, vT, doT, relT, u_bias, v_bias)
        half = heads * dim // 2
        bias, dw = pl.pallas_call(
            functools.partial(table_grad_kernel, n),
            out_shape=[sds((heads, 2, 8, dim), F32), sds((heads * dim, model), F32)],
            in_specs=[vmem] * 4, out_specs=[vmem] * 2,
            scratch_shapes=[buf((n, 2, 8, dim), F32), buf((half, model), F32), buf((half, model), F32),
                            buf((heads, half // heads, model), F32), buf((heads * dim, model), F32),
                            dma((n,)), dma((n,)), dma((12,)), dma((12,))],
            compiler_params=pltpu.CompilerParams(collective_id=1, has_side_effects=True),
            name='table_grad',
        )(dr, du, dv, rel_table)
        back = lambda x: x.transpose(2, 0, 1)
        return (back(o), back(dq), back(dk), back(dvv), bias[:, 0, 0], bias[:, 1, 0],
                back(dw.reshape(heads, dim, model)))

    return jax.shard_map(
        local_fn, mesh=mesh,
        in_specs=(seq_spec, seq_spec, seq_spec, head_spec, head_spec, P('cp', None), weight_spec, seq_spec),
        out_specs=(seq_spec, seq_spec, seq_spec, seq_spec, head_spec, head_spec, weight_spec),
        check_vma=False,
    )
```

```python
import functools
import math
import jax
import jax.numpy as jnp
from jax import lax
from jax.experimental import pallas as pl
from jax.experimental.pallas import tpu as pltpu
from jax.sharding import PartitionSpec as P

F32, BF16 = jnp.float32, jnp.bfloat16
LOG2E = math.log2(math.e)
BQ = 256
BK = 512
NC = BK // 128
PAD = 512
KX = 80
GROUP = 3
UNROLL = 3
MESH_ID = pl.DeviceIdType.MESH


def dot_nn(a, b):
    return lax.dot_general(a, b, (((1,), (0,)), ((), ())), preferred_element_type=F32)


def dot_nt(a, b):
    return lax.dot_general(a, b, (((1,), (1,)), ((), ())), preferred_element_type=F32)


def aligned(x, m):
    return pl.multiple_of(x, m)


def anti_eye(n):
    rows = lax.broadcasted_iota(jnp.int32, (n, n), 0)
    cols = lax.broadcasted_iota(jnp.int32, (n, n), 1)
    return (rows + cols == n - 1).astype(F32).astype(BF16)


def flip_lanes(x, eye):
    n, w = x.shape[1], eye.shape[0]
    parts = [dot_nn(x[:, s:s + w], eye).astype(BF16) for s in range(0, n, w)]
    return jnp.concatenate(parts[::-1], axis=1)


def reverse_rows(x):
    ix = 7 - lax.broadcasted_iota(jnp.int32, (8, x.shape[1]), 0)
    n = x.shape[0] // 8
    return jnp.concatenate([jnp.take_along_axis(x[(n - 1 - g) * 8:(n - g) * 8], ix, axis=0) for g in range(n)], 0)


def owner_core(rb):
    return lax.rem(rb + rb // 2, 2)


def remote_copy(src, dst, send_sem, recv_sem, to):
    return pltpu.make_async_remote_copy(src, dst, send_sem, recv_sem, device_id=(lax.axis_index('hp'), to),
                                        device_id_type=MESH_ID)


def barrier_all(n):
    me, hp = lax.axis_index('cp'), lax.axis_index('hp')
    bar = pltpu.get_barrier_semaphore()
    for o in range(1, n):
        pl.semaphore_signal(bar, 1, device_id=(hp, lax.rem(me + o, n)), device_id_type=MESH_ID)
    pl.semaphore_wait(bar, n - 1)


def hand_off_kernel(o, dq, dk, dv, dw, bias, o_out, dq_out, dk_out, dv_out, dw_out, u_out, v_out):
    for src, dst in ((o, o_out), (dq, dq_out), (dk, dk_out), (dv, dv_out), (dw, dw_out)):
        dst[...] = src[...]
    u_out[...], v_out[...] = bias[0], bias[1]


def attention_kernel(n, q_in, k_in, v_in, do_in, table_in, w_rel, ub, vb,
                     o_out, dq_out, dk_out, dv_out, dw_out, bias_out,
                     qT, doT, kT, vT, relX, oT, dqT, dkT, dvT, drF,
                     s_all, q_off, q_row, do_row, q_col, qo_col, do_col, mx, total, acc, gv, r_scr,
                     pair_buf, send_buf, dr_buf, table, bias_buf,
                     send_d, send_f, send_q, recv_b, recv_q, loc_b, loc_q,
                     send_o, recv_o, loc_o, send_p, recv_p, send_s, recv_s, loc_s,
                     loc_t, send_w, recv_w, loc_w, send_b, recv_b2):
    me = lax.axis_index('cp')
    chip, core = me // 2, lax.rem(me, 2)
    mate = 2 * chip + 1 - core
    heads, dim, blk = q_in.shape
    seq = n * blk
    per_blk = blk // BQ
    groups = n // 2
    nslot = qT.shape[1] // BQ
    scale = dim ** -0.5
    pltpu.make_async_copy(table_in, table, loc_t).start()
    barrier_all(n)

    rel_buf = dr_buf
    srcs, fulls = (rel_buf, k_in, v_in), (relX, kT, vT)

    def col(t, b, flipped):
        b = (n - 1 - b) if t == flipped else b
        return pl.ds(aligned(b * blk, blk), blk)

    def full_at(t, b):
        return fulls[t].at[pl.ds(0, dim), col(t, b, 0)]

    def direct(t, i):
        h = lax.rem(chip + i, heads)
        return remote_copy(srcs[t].at[h], full_at(t, me), send_d.at[t, i], recv_b.at[t, me], 2 * h + core)

    def own(t):
        return pltpu.make_async_copy(srcs[t].at[chip], full_at(t, me), loc_b.at[t])

    def to_mate(t):
        return remote_copy(srcs[t].at[chip], full_at(t, me), send_f.at[t, chip], recv_b.at[t, me], mate)

    def forward(t, g):
        b = 2 * g + core
        return remote_copy(full_at(t, b), full_at(t, b), send_f.at[t, g], recv_b.at[t, b], mate)

    def landed(t, b):
        remote_copy(srcs[t].at[0], full_at(t, b), send_f.at[t, 0], recv_b.at[t, b], me).wait_recv()

    def pass_on(t, g):
        @pl.when(g != chip)
        def _():
            landed(t, 2 * g + core)
            forward(t, g).start()

        pl.when(g == chip)(own(t).wait)

    def from_mate(t, g):
        landed(t, 2 * g + 1 - core)

    def row_copy(t, i, j, wait):
        h = lax.rem(chip + i, heads)
        rb = me * per_blk + j
        src = (q_in, do_in)[t].at[h, :, pl.ds(j * BQ, BQ)]
        dst = (qT, doT)[t].at[:, pl.ds(aligned(rb // 2 * BQ, BQ), BQ)]
        to = 2 * h + owner_core(rb)

        @pl.when(to != me)
        def _():
            c = remote_copy(src, dst, send_q.at[t, i, j], recv_q.at[t, rb // 2], to)
            c.wait_send() if wait else c.start()

        @pl.when(to == me)
        def _():
            c = pltpu.make_async_copy(src, dst, loc_q.at[t, j])
            c.wait() if wait else c.start()

    def row_block(k):
        return 2 * k + lax.rem(k + core, 2)

    def row_landed(t, k):
        src = (q_in, do_in)[t].at[0, :, pl.ds(0, BQ)]
        dst = (qT, doT)[t].at[:, pl.ds(aligned(k * BQ, BQ), BQ)]
        rb = row_block(k)

        @pl.when(rb // per_blk != me)
        def _():
            remote_copy(src, dst, send_q.at[t, 0, 0], recv_q.at[t, k], me).wait_recv()

        @pl.when(rb // per_blk == me)
        def _():
            pltpu.make_async_copy(src, dst, loc_q.at[t, lax.rem(rb, per_blk)]).wait()

    order = (1, 3, 2)
    eye = anti_eye(BQ)
    pltpu.make_async_copy(table_in, table, loc_t).wait()
    rel = flip_lanes(dot_nt(w_rel[...], table[...]).astype(BF16), eye)
    for h in range(heads):
        rel_buf[h] = rel[h * dim:(h + 1) * dim]
    to_mate(1).start()
    own(1).start()
    for i in order:
        direct(1, i).start()
        direct(0, i).start()
        for j in range(per_blk):
            row_copy(0, i, j, False)
    for j in range(per_blk):
        row_copy(0, 0, j, False)
    to_mate(0).start()
    own(0).start()

    def send_values():
        to_mate(2).start()
        own(2).start()
        for i in order:
            direct(2, i).start()

    def send_cotangent():
        for i in range(1, heads):
            direct(0, i).wait_send()
        to_mate(0).wait_send()
        for i in order + (0,):
            for j in range(per_blk):
                row_copy(1, i, j, False)

    for ref in (dkT, dvT, drF, total, acc, gv):
        ref[...] = jnp.zeros_like(ref)
    mx[...] = jnp.full(mx.shape, -jnp.inf, F32)
    relX[pl.ds(0, dim), pl.ds(seq, PAD)] = jnp.zeros((dim, PAD), BF16)
    first = lax.broadcasted_iota(jnp.int32, (KX - dim, PAD), 0) == 0
    relX[pl.ds(dim, KX - dim), pl.ds(0, seq)] = jnp.zeros((KX - dim, seq), BF16)
    relX[pl.ds(dim, KX - dim), pl.ds(seq, PAD)] = jnp.where(first, -jnp.inf, 0.0).astype(BF16)
    ones_col = (lax.broadcasted_iota(jnp.int32, (BQ, KX - dim), 1) == 0).astype(F32).astype(BF16)
    lane = lax.broadcasted_iota(jnp.int32, (128, 128), 1)
    row = lax.broadcasted_iota(jnp.int32, (128, 128), 0)
    past, before = lane > row, lane < row

    def bias_col(ref):
        pick = lax.broadcasted_iota(jnp.int32, ref.shape, 0) == chip
        r = jnp.sum(jnp.where(pick, ref[...], 0.0), axis=0, keepdims=True)
        return jnp.broadcast_to(r, (128, dim)).T[:, :1]

    u_col, v_col = bias_col(ub), bias_col(vb)

    def skew(t):
        return pltpu.roll(t, 1, 1, stride=1, stride_axis=0)

    def slot_cols(k):
        return pl.ds(aligned(k * BQ, BQ), BQ)

    def transposed(x):
        return x.astype(F32).T.astype(BF16)

    def prepare(k, i):
        q = qT[:, slot_cols(k)].astype(F32)
        quT, qvT = (q + u_col).astype(BF16), (q + v_col).astype(BF16)
        q_off[k] = jnp.concatenate([transposed(qvT), ones_col], 1)
        q_col[k] = flip_lanes(quT, eye)
        q_row[k] = transposed(q_col[k])
        qo_col[k] = flip_lanes(qvT, eye)
        base = seq - row_block(k) * BQ
        t0 = dot_nn(q_off[k], relX[:, pl.ds(aligned(base - 256, 128), 256)])
        r_scr[i, :, :128], r_scr[i, :, 128:] = skew(t0[:, :128]), skew(t0[:, 128:])

    def scores(tile, k, t):
        j0 = aligned(t * BK, BK)
        base = seq - row_block(k) * BQ
        by_offset = dot_nn(q_off[k], relX[:, pl.ds(aligned(base + j0, 128), BK)])
        content = dot_nn(q_row[k], kT[:, pl.ds(j0, BK)])
        ri = jnp.where(t == 0, lax.rem(k, GROUP), GROUP)
        rolled = [r_scr[ri, :, :128], r_scr[ri, :, 128:]]
        rolled += [skew(by_offset[:, m * 128:(m + 1) * 128]) for m in range(NC)]
        top_s = mx[k]
        for m in range(NC):
            top = jnp.where(past, rolled[m + 2][:128], rolled[m + 1][:128])
            bot = jnp.where(past, rolled[m + 1][128:], rolled[m][128:])
            s = content[:, m * 128:(m + 1) * 128] + reverse_rows(jnp.concatenate([top, bot], 0))
            s = s * (scale * LOG2E)
            s_all[tile, :, m * 128:(m + 1) * 128] = s
            top_s = jnp.maximum(top_s, s)
        mx[k] = top_s
        r_scr[GROUP, :, :128], r_scr[GROUP, :, 128:] = rolled[NC], rolled[NC + 1]

    def weigh(tile, k, t):
        top_s, tot = mx[k], total[k]
        parts = []
        for m in range(NC):
            p = jnp.exp2(s_all[tile, :, m * 128:(m + 1) * 128] - top_s)
            s_all[tile, :, m * 128:(m + 1) * 128] = p
            tot = tot + p
            parts.append(p.astype(BF16))
        total[k] = tot
        acc[k] += dot_nt(jnp.concatenate(parts, 1), vT[:, pl.ds(aligned(t * BK, BK), BK)])

    def finish_rows(k):
        do_col[k] = flip_lanes(doT[:, slot_cols(k)], eye)
        do_row[k] = transposed(do_col[k])
        inv = 1.0 / jnp.sum(total[k], axis=1, keepdims=True)
        out = acc[k] * inv
        delta = jnp.sum(do_row[k].astype(F32) * out, axis=1, keepdims=True)
        total[k] = jnp.broadcast_to(inv, (BQ, 128))
        mx[k] = jnp.broadcast_to(delta, (BQ, 128))
        oT[:, slot_cols(k)] = flip_lanes(out.T.astype(BF16), eye)
        acc[k] = jnp.zeros((BQ, dim), F32)

    def grads(tile, k, t):
        j0 = aligned(t * BK, BK)
        base = seq - row_block(k) * BQ
        js, us = pl.ds(j0, BK), pl.ds(aligned(base + j0 - 256, 128), BK)
        dp = dot_nn(do_row[k], vT[:, js])
        inv, delta = total[k], mx[k]
        prev = jnp.maximum(tile - 1, 0)
        ps, dss = [], []
        held = [jnp.where(t > 0, s_all[prev, :, m * 128:(m + 1) * 128], 0.0).astype(BF16) for m in range(2)]
        for m in range(NC):
            p = s_all[tile, :, m * 128:(m + 1) * 128] * inv
            ds = (p * ((dp[:, m * 128:(m + 1) * 128] - delta) * scale)).astype(BF16)
            ps.append(p.astype(BF16))
            dss.append(ds)
            held.append(pltpu.roll(ds, 0, 1, stride=1, stride_axis=0))
        for m in range(2):
            s_all[tile, :, m * 128:(m + 1) * 128] = held[NC + m].astype(F32)
        by_offset = []
        for m in range(NC):
            top = jnp.where(before, held[m + 1][:128], held[m + 2][:128])
            bot = jnp.where(before, held[m][128:], held[m + 1][128:])
            by_offset.append(jnp.concatenate([top, bot], 0))
        p_all, ds_all, by_offset = (jnp.concatenate(x, 1) for x in (ps, dss, by_offset))
        dvT[:, js] += dot_nn(do_col[k], p_all)
        dkT[:, js] += dot_nn(q_col[k], ds_all)
        drF[:, us] += dot_nn(qo_col[k], by_offset)
        acc[k] += dot_nt(ds_all, kT[:, js])
        gv[k] += dot_nt(by_offset, relX[:dim, us])

    def walk(step, count, k, t_low, t_cap):
        def some(i, kt):
            k, t = kt
            for u in range(UNROLL):
                step(k * (k + 1) // 2 + t, k, t)
                last = t == jnp.minimum(k, t_cap)
                k, t = jnp.where(last, k + 1, k), jnp.where(last, t_low, t + 1)
            return k, t

        lax.fori_loop(0, count // UNROLL, some, (k, t_low))

    def group_tiles(g):
        return GROUP * GROUP * g + GROUP * (GROUP + 1) // 2

    def over_tiles(step, g):
        walk(step, group_tiles(g), GROUP * g, 0, nslot)

    def each(fn):
        lax.fori_loop(0, groups, lambda g, c: (fn(g), c)[1], 0)

    def forward_scores(g):
        for t in (0, 1):
            pass_on(t, g)
        for t in (0, 1):
            from_mate(t, g)
        for i in range(GROUP):
            row_landed(0, GROUP * g + i)
        for i in range(GROUP):
            prepare(GROUP * g + i, i)
        lower = chip < groups // 2
        pl.when(g == jnp.where(lower, 3, 1))(send_values)
        pl.when((g == 2) & ~lower)(send_cotangent)
        over_tiles(scores, g)

    each(forward_scores)
    pl.when(chip < groups // 2)(send_cotangent)
    each(lambda g: pass_on(2, g))

    def row_max(g):
        for i in range(GROUP):
            k = GROUP * g + i
            mx[k] = jnp.broadcast_to(jnp.max(mx[k], axis=1, keepdims=True), (BQ, 128))

    each(row_max)

    def weigh_group(g):
        from_mate(2, g)
        over_tiles(weigh, g)

    each(weigh_group)

    def out_rows(t, k, wait):
        rb = row_block(k)
        to, j = rb // per_blk, lax.rem(rb, per_blk)
        src = (oT, dqT)[t].at[:, slot_cols(k)]
        dst = (o_out, dq_out)[t].at[chip, :, pl.ds(aligned(j * BQ, BQ), BQ)]

        @pl.when(to != me)
        def _():
            c = remote_copy(src, dst, send_o.at[t, k], recv_o.at[t, chip, j], to)
            c.wait_send() if wait else c.start()

        @pl.when(to == me)
        def _():
            c = pltpu.make_async_copy(src, dst, loc_o.at[t, j])
            c.wait() if wait else c.start()

    def finish_group(g):
        for i in range(GROUP):
            row_landed(1, GROUP * g + i)
        for i in range(GROUP):
            finish_rows(GROUP * g + i)
        for i in range(GROUP):
            out_rows(0, GROUP * g + i, False)

    each(finish_group)

    parts, sinks = (drF, dkT, dvT), (dr_buf, dk_out, dv_out)

    def pair(t, g, s):
        return remote_copy(parts[t].at[:, col(t, 2 * g + 1 - core, 0)], pair_buf.at[t, s], send_p.at[t, s], recv_p.at[t, s], mate)

    def sink(t, g, s):
        return remote_copy(send_buf.at[t, s], sinks[t].at[chip], send_s.at[t, s], recv_s.at[t, chip], 2 * g + core)

    def keep(t, s):
        return pltpu.make_async_copy(send_buf.at[t, s], sinks[t].at[chip], loc_s.at[t])

    def out_groups(step):
        g = groups - 1 - step
        return g, jnp.where(chip < groups // 2, g, step)

    def combine(step, s):
        gd, gk = out_groups(step)
        for t, g in ((0, gd), (1, gk), (2, gk)):
            mine = col(t, 2 * g + core, 0)
            remote_copy(parts[t].at[:, mine], pair_buf.at[t, s], send_p.at[t, s], recv_p.at[t, s], mate).wait_recv()
            send_buf[t, s] = (parts[t][:, mine] + pair_buf[t, s]).astype(BF16)
        for t, g in ((0, gd), (1, gk), (2, gk)):
            @pl.when(g != chip)
            def _():
                sink(t, g, s).start()

            @pl.when(g == chip)
            def _():
                keep(t, s).start()

    w_acc, w_in, w_half, w_part, w_mine = (9, 0), (10, 0), (10, 1), (11, 0), (11, 1)

    def place(kt, c=0):
        return kt[0] * (kt[0] + 1) // 2 + kt[1] + c

    half = heads * dim // 2
    piece = half // heads

    def swap(c):
        return remote_copy(s_all.at[place(w_acc, c), pl.ds(aligned((1 - core) * half, half), half)],
                           s_all.at[place(w_in), pl.ds(c * half, half)], send_w.at[0, c], recv_w.at[0, c], mate)

    def spread(i, c):
        z = lax.rem(chip + i, heads)
        return remote_copy(s_all.at[place(w_half), pl.ds(aligned(c * half + z * piece, piece), piece)],
                           s_all.at[place(w_part), pl.ds((2 * i + c) * piece, piece)], send_w.at[i, c], recv_w.at[i, c], 2 * z + core)

    def table_grad():
        for h in range(heads):
            @pl.when(h != chip)
            def _():
                remote_copy(send_buf.at[0, 0], dr_buf.at[h], send_s.at[0, 0], recv_s.at[0, h], me).wait_recv()

            @pl.when(h == chip)
            def _():
                keep(0, 0).wait()
        dr = jnp.concatenate([flip_lanes(dr_buf[h], eye) for h in range(heads)], 0)
        for c in range(2):
            s_all[place(w_acc, c)] = dot_nn(dr, table[:, c * BK:(c + 1) * BK])
        for c in range(2):
            swap(c).start()
        for c in range(2):
            swap(c).wait()
            s_all[place(w_half), c * half:(c + 1) * half] = (
                s_all[place(w_acc, c), pl.ds(aligned(core * half, half), half)] + s_all[place(w_in), c * half:(c + 1) * half])
        for i in range(1, heads):
            for c in range(2):
                spread(i, c).start()

    def backward_step(step):
        gd, gk = out_groups(step)
        left = chip < groups // 2
        s = lax.rem(step, 2)
        walk(grads, group_tiles(gd), GROUP * gk, jnp.where(left, 0, GROUP * step), jnp.where(left, nslot, GROUP * step + GROUP - 1))

        @pl.when(step > 1)
        def _():
            pd, pk = out_groups(step - 2)
            for t, g, p in ((0, gd, pd), (1, gk, pk), (2, gk, pk)):
                pair(t, p, s).wait_send()

                @pl.when(p != chip)
                def _():
                    sink(t, p, s).wait_send()

                @pl.when((p == chip) & (t > 0))
                def _():
                    keep(t, s).wait()

        for t, g in ((0, gd), (1, gk), (2, gk)):
            pair(t, g, s).start()
        for i in range(GROUP):
            k = GROUP * gk + i
            dqT[:, slot_cols(k)] = flip_lanes((acc[k] + gv[k]).T.astype(BF16), eye)
        combine(step, s)
        for i in range(GROUP):
            out_rows(1, GROUP * gk + i, False)

        pl.when((step > 0) & (chip == groups - step))(table_grad)

    each(backward_step)
    for t, ref in ((0, acc), (1, gv)):
        rows_sum = jnp.sum(ref[...].reshape(nslot * BQ // 8, 8, dim), axis=0)
        bias_buf[me, t] = jnp.sum(rows_sum, axis=0, keepdims=True) + jnp.zeros((8, dim), F32)

    def bias(o):
        return remote_copy(bias_buf.at[me], bias_buf.at[me], send_b.at[o], recv_b2.at[me], lax.rem(me + o, n))

    for o in range(1, n):
        bias(o).start()
    pl.when(chip == 0)(table_grad)
    for i in range(1, heads):
        for c in range(2):
            spread(i, c).wait()
    mine = place(w_mine)
    for c in range(2):
        got = s_all[place(w_half), pl.ds(aligned(c * half + chip * piece, piece), piece)]
        for i in range(1, heads):
            got = got + s_all[place(w_part), (2 * i + c) * piece:(2 * i + c + 1) * piece]
        s_all[mine, c * piece:(c + 1) * piece] = got

    def home(co, z, c):
        return dw_out.at[pl.ds(aligned(co * half + z * piece, piece), piece), pl.ds(c * BK, BK)]

    def my_piece(c):
        return s_all.at[mine, pl.ds(c * piece, piece)]

    def collect(i, c):
        z = lax.rem(chip + i, heads)
        return remote_copy(my_piece(c), home(core, chip, c), send_w.at[4 + i, c], recv_w.at[4 + chip, c], 2 * z + core)

    def hand_over(i, c):
        z = lax.rem(chip + i, heads)
        return remote_copy(my_piece(c) if i == 0 else home(core, z, c), home(core, z, c), send_w.at[8 + i, c], recv_w.at[8 + z, c], mate)

    def stay(c):
        return pltpu.make_async_copy(my_piece(c), home(core, chip, c), loc_w.at[c])

    for c in range(2):
        for i in range(1, heads):
            collect(i, c).start()
        hand_over(0, c).start()
        stay(c).start()
    for i in range(1, heads):
        z = lax.rem(chip + i, heads)
        for c in range(2):
            remote_copy(my_piece(c), home(core, z, c), send_w.at[0, c], recv_w.at[4 + z, c], me).wait_recv()
            hand_over(i, c).start()
    for o in range(1, n):
        b = lax.rem(me + o, n)
        remote_copy(bias_buf.at[b], bias_buf.at[b], send_b.at[0], recv_b2.at[b], me).wait_recv()
    for t in range(2):
        bias_out[t] = jnp.concatenate([bias_buf[2 * h, t, :1] + bias_buf[2 * h + 1, t, :1] for h in range(heads)], 0)

    for c in range(2):
        stay(c).wait()
        for i in range(heads):
            remote_copy(my_piece(c), home(1 - core, i, c), send_w.at[0, c], recv_w.at[8 + i, c], me).wait_recv()
            hand_over(i, c).wait_send()
            if i:
                collect(i, c).wait_send()
    for o in range(1, n):
        bias(o).wait_send()
    for t in range(3):
        for step in (groups - 2, groups - 1):
            gd, gk = out_groups(step)
            g = gk if t else gd
            pair(t, g, step % 2).wait_send()

            @pl.when(g != chip)
            def _():
                sink(t, g, step % 2).wait_send()

            if t:
                @pl.when(g == chip)
                def _():
                    keep(t, step % 2).wait()
        if t:
            to_mate(t).wait_send()
        for i in range(1, heads):
            h = lax.rem(chip + i, heads)
            forward(t, h).wait_send()
            if t:
                direct(t, i).wait_send()
                remote_copy(send_buf.at[t, 0], sinks[t].at[h], send_s.at[t, 0], recv_s.at[t, h], me).wait_recv()
    for t in (0, 1):
        for i in range(heads):
            for j in range(per_blk):
                to = 2 * lax.rem(chip + i, heads) + owner_core(me * per_blk + j)

                @pl.when(to != me)
                def _():
                    remote_copy((q_in, do_in)[t].at[0, :, pl.ds(0, BQ)], (qT, doT)[t].at[:, pl.ds(0, BQ)],
                                send_q.at[t, i, j], recv_q.at[t, 0], to).wait_send()
        for k in range(nslot):
            out_rows(t, k, True)
        for h in range(heads):
            for j in range(per_blk):
                @pl.when(2 * h + owner_core(me * per_blk + j) != me)
                def _():
                    remote_copy((oT, dqT)[t].at[:, pl.ds(0, BQ)], (o_out, dq_out)[t].at[h, :, pl.ds(j * BQ, BQ)],
                                send_o.at[t, 0], recv_o.at[t, h, j], me).wait_recv()


def solution(mesh):
    n = mesh.shape['cp']
    seq_spec, head_spec, weight_spec = P('cp', 'hp', None), P('hp', None), P(None, 'hp', None)
    vmem = pl.BlockSpec(memory_space=pltpu.VMEM)
    hbm = pl.BlockSpec(memory_space=pl.ANY)
    dma, sds, buf = pltpu.SemaphoreType.DMA, jax.ShapeDtypeStruct, pltpu.VMEM

    def local_fn(q, k, v, u_bias, v_bias, rel_table, w_rel, d_out):
        blk, heads, dim = q.shape
        seq = n * blk
        rows = seq // 2
        nslot = rows // BQ
        per_blk = blk // BQ
        tiles = nslot * (nslot + 1) // 2
        qT, kT, vT, doT = (x.transpose(1, 2, 0) for x in (q, k, v, d_out))
        wT = w_rel.transpose(1, 2, 0).reshape(heads * dim, -1)
        model = wT.shape[1]
        o, dq, dk, dvv, dw, bias = pl.pallas_call(
            functools.partial(attention_kernel, n),
            out_shape=[sds((heads, dim, blk), BF16)] * 4 + [sds((heads * dim, model), F32), sds((2, heads, dim), F32)],
            in_specs=[hbm] * 5 + [vmem] * 3, out_specs=[hbm] * 5 + [vmem],
            scratch_shapes=[
                buf((dim, rows), BF16), buf((dim, rows), BF16), buf((dim, seq), BF16), buf((dim, seq), BF16), buf((KX, seq + PAD), BF16),
                buf((dim, rows), BF16), buf((dim, rows), BF16), buf((dim, seq), F32), buf((dim, seq), F32), buf((dim, seq + PAD), F32),
                buf((tiles, BQ, BK), F32), buf((nslot, BQ, KX), BF16), buf((nslot, BQ, dim), BF16), buf((nslot, BQ, dim), BF16),
                buf((nslot, dim, BQ), BF16), buf((nslot, dim, BQ), BF16), buf((nslot, dim, BQ), BF16),
                buf((nslot, BQ, 128), F32), buf((nslot, BQ, 128), F32), buf((nslot, BQ, dim), F32), buf((nslot, BQ, dim), F32),
                buf((GROUP + 1, BQ, 256), F32),
                buf((3, 2, dim, blk), F32), buf((3, 2, dim, blk), BF16), buf((heads, dim, blk), BF16), buf((blk, model), BF16),
                buf((n, 2, 8, dim), F32),
                dma((3, heads)), dma((3, heads)), dma((2, heads, per_blk)), dma((3, n)), dma((2, nslot)), dma((3,)), dma((2, per_blk)),
                dma((2, nslot)), dma((2, heads, per_blk)), dma((2, per_blk)), dma((3, 2)), dma((3, 2)),
                dma((3, 2)), dma((3, heads)), dma((3,)),
                dma, dma((12, 2)), dma((12, 2)), dma((2,)), dma((n,)), dma((n,))],
            compiler_params=pltpu.CompilerParams(collective_id=0, has_side_effects=True, vmem_limit_bytes=67043328),
            name='attention',
        )(qT, kT, vT, doT, rel_table, wT, u_bias, v_bias)
        steps = 2
        part = pl.BlockSpec((heads // steps, dim, blk), lambda i: (i, 0, 0))
        wide = pl.BlockSpec((heads * dim // steps, model), lambda i: (i, 0))
        whole = lambda *shape: pl.BlockSpec(shape, lambda i: (0,) * len(shape))
        o, dq, dk, dvv, dw, du, dv = pl.pallas_call(
            hand_off_kernel, grid=(steps,),
            out_shape=[sds((heads, dim, blk), BF16)] * 4 + [sds((heads * dim, model), F32)] + [sds((heads, dim), F32)] * 2,
            in_specs=[part] * 4 + [wide, whole(2, heads, dim)],
            out_specs=[part] * 4 + [wide, whole(heads, dim), whole(heads, dim)],
            name='hand_off',
        )(o, dq, dk, dvv, dw, bias)
        back = lambda x: x.transpose(2, 0, 1)
        return back(o), back(dq), back(dk), back(dvv), du, dv, back(dw.reshape(heads, dim, model))

    return jax.shard_map(
        local_fn, mesh=mesh,
        in_specs=(seq_spec, seq_spec, seq_spec, head_spec, head_spec, P('cp', None), weight_spec, seq_spec),
        out_specs=(seq_spec, seq_spec, seq_spec, seq_spec, head_spec, head_spec, weight_spec),
        check_vma=False,
    )
```

```python
import functools
import math
import jax
import jax.numpy as jnp
from jax import lax
from jax.experimental import pallas as pl
from jax.experimental.pallas import tpu as pltpu
from jax.sharding import PartitionSpec as P

F32, BF16 = jnp.float32, jnp.bfloat16
LOG2E = math.log2(math.e)
BQ = 256
BK = 512
NC = BK // 128
PAD = 512
KX = 80
GROUP = 3
UNROLL = 3
VALUES_AT = 6
MESH_ID = pl.DeviceIdType.MESH


def dot_nn(a, b):
    return lax.dot_general(a, b, (((1,), (0,)), ((), ())), preferred_element_type=F32)


def dot_nt(a, b):
    return lax.dot_general(a, b, (((1,), (1,)), ((), ())), preferred_element_type=F32)


def aligned(x, m):
    return pl.multiple_of(x, m)


def anti_eye(n):
    rows = lax.broadcasted_iota(jnp.int32, (n, n), 0)
    cols = lax.broadcasted_iota(jnp.int32, (n, n), 1)
    return (rows + cols == n - 1).astype(F32).astype(BF16)


def flip_lanes(x, eye):
    n, w = x.shape[1], eye.shape[0]
    parts = [dot_nn(x[:, s:s + w], eye).astype(BF16) for s in range(0, n, w)]
    return jnp.concatenate(parts[::-1], axis=1)


def reverse_rows(x):
    ix = 7 - lax.broadcasted_iota(jnp.int32, (8, x.shape[1]), 0)
    n = x.shape[0] // 8
    return jnp.concatenate([jnp.take_along_axis(x[(n - 1 - g) * 8:(n - g) * 8], ix, axis=0) for g in range(n)], 0)


def owner_core(rb):
    return lax.rem(rb + rb // 2, 2)


def remote_copy(src, dst, send_sem, recv_sem, to):
    return pltpu.make_async_remote_copy(src, dst, send_sem, recv_sem, device_id=(lax.axis_index('hp'), to),
                                        device_id_type=MESH_ID)


def barrier_all(n):
    me, hp = lax.axis_index('cp'), lax.axis_index('hp')
    bar = pltpu.get_barrier_semaphore()
    for o in range(1, n):
        pl.semaphore_signal(bar, 1, device_id=(hp, lax.rem(me + o, n)), device_id_type=MESH_ID)
    pl.semaphore_wait(bar, n - 1)


def hand_off_kernel(o, dq, dk, dv, dw, bias, o_out, dq_out, dk_out, dv_out, dw_out, u_out, v_out):
    for src, dst in ((o, o_out), (dq, dq_out), (dk, dk_out), (dv, dv_out), (dw, dw_out)):
        dst[...] = src[...]
    u_out[...], v_out[...] = bias[0], bias[1]


def attention_kernel(n, q_in, k_in, v_in, do_in, table_in, w_rel, ub, vb,
                     o_out, dq_out, dk_out, dv_out, dw_out, bias_out,
                     qT, doT, kT, vT, relX, oT, dqT, dkT, dvT, drF,
                     s_all, q_off, q_row, do_row, q_col, qo_col, do_col, mx, total, acc, r_scr,
                     pair_buf, dr_send, send_buf, dr_buf, table, bias_buf,
                     send_d, send_f, send_q, recv_b, recv_q, loc_b, loc_q,
                     send_o, recv_o, loc_o, send_p, recv_p, send_s, recv_s, loc_s,
                     loc_t, send_w, recv_w, loc_w, send_b, recv_b2):
    me = lax.axis_index('cp')
    chip, core = me // 2, lax.rem(me, 2)
    mate = 2 * chip + 1 - core
    heads, dim, blk = q_in.shape
    seq = n * blk
    per_blk = blk // BQ
    groups = n // 2
    nslot = qT.shape[1] // BQ
    scale = dim ** -0.5
    pltpu.make_async_copy(table_in, table, loc_t).start()
    barrier_all(n)

    rel_buf = dr_buf
    srcs, fulls = (rel_buf, k_in, v_in), (relX, kT, vT)

    def col(t, b, flipped):
        b = (n - 1 - b) if t == flipped else b
        return pl.ds(aligned(b * blk, blk), blk)

    def full_at(t, b):
        return fulls[t].at[pl.ds(0, dim), col(t, b, 0)]

    def direct(t, h):
        return remote_copy(srcs[t].at[h], full_at(t, me), send_d.at[t, h], recv_b.at[t, me], 2 * h + core)

    def own(t):
        return pltpu.make_async_copy(srcs[t].at[chip], full_at(t, me), loc_b.at[t])

    def to_mate(t):
        return remote_copy(srcs[t].at[chip], full_at(t, me), send_f.at[t, chip], recv_b.at[t, me], mate)

    def forward(t, g):
        b = 2 * g + core
        return remote_copy(full_at(t, b), full_at(t, b), send_f.at[t, g], recv_b.at[t, b], mate)

    def landed(t, b):
        remote_copy(srcs[t].at[0], full_at(t, b), send_f.at[t, 0], recv_b.at[t, b], me).wait_recv()

    def pass_on(t, g):
        @pl.when(g != chip)
        def _():
            landed(t, 2 * g + core)
            forward(t, g).start()

        pl.when(g == chip)(own(t).wait)

    def from_mate(t, g):
        landed(t, 2 * g + 1 - core)

    def row_copy(t, h, j, wait):
        rb = me * per_blk + j
        src = (q_in, do_in)[t].at[h, :, pl.ds(j * BQ, BQ)]
        dst = (qT, doT)[t].at[:, pl.ds(aligned(rb // 2 * BQ, BQ), BQ)]
        to = 2 * h + owner_core(rb)

        @pl.when(to != me)
        def _():
            c = remote_copy(src, dst, send_q.at[t, h, j], recv_q.at[t, rb // 2], to)
            c.wait_send() if wait else c.start()

        @pl.when(to == me)
        def _():
            c = pltpu.make_async_copy(src, dst, loc_q.at[t, j])
            c.wait() if wait else c.start()

    def row_block(k):
        return 2 * k + lax.rem(k + core, 2)

    def row_landed(t, k):
        src = (q_in, do_in)[t].at[0, :, pl.ds(0, BQ)]
        dst = (qT, doT)[t].at[:, pl.ds(aligned(k * BQ, BQ), BQ)]
        rb = row_block(k)

        @pl.when(rb // per_blk != me)
        def _():
            remote_copy(src, dst, send_q.at[t, 0, 0], recv_q.at[t, k], me).wait_recv()

        @pl.when(rb // per_blk == me)
        def _():
            pltpu.make_async_copy(src, dst, loc_q.at[t, lax.rem(rb, per_blk)]).wait()

    lower = chip < groups // 2
    side = chip + 1 - 2 * lax.rem(chip, 2)
    near, far = jnp.where(lower, groups // 2, groups // 2 - 1), jnp.where(lower, groups - 1, 0)
    across = near, far

    def send_rows(t, h):
        for j in range(per_blk):
            row_copy(t, h, j, False)

    def send_scores_input(h):
        direct(1, h).start()
        send_rows(0, h)

    to_mate(1).start()
    own(1).start()
    send_scores_input(side)
    send_rows(0, chip)
    eye = anti_eye(BQ)
    pltpu.make_async_copy(table_in, table, loc_t).wait()
    rel = flip_lanes(dot_nt(w_rel[...], table[...]).astype(BF16), eye)
    for h in range(heads):
        rel_buf[h] = rel[h * dim:(h + 1) * dim]
    to_mate(0).start()
    own(0).start()
    for h in (side, *across):
        direct(0, h).start()
    for h in across:
        send_scores_input(h)

    def send_values():
        to_mate(2).start()
        own(2).start()
        for h in (side, *across):
            direct(2, h).start()

    def send_cotangent():
        for h in (side, *across):
            direct(0, h).wait_send()
        to_mate(0).wait_send()
        for h in (side, *across, chip):
            send_rows(1, h)

    for ref in (dkT, dvT, drF, total, acc):
        ref[...] = jnp.zeros_like(ref)
    mx[...] = jnp.full(mx.shape, -jnp.inf, F32)
    relX[pl.ds(0, dim), pl.ds(seq, PAD)] = jnp.zeros((dim, PAD), BF16)
    first = lax.broadcasted_iota(jnp.int32, (KX - dim, PAD), 0) == 0
    relX[pl.ds(dim, KX - dim), pl.ds(0, seq)] = jnp.zeros((KX - dim, seq), BF16)
    relX[pl.ds(dim, KX - dim), pl.ds(seq, PAD)] = jnp.where(first, -jnp.inf, 0.0).astype(BF16)
    ones_col = (lax.broadcasted_iota(jnp.int32, (BQ, KX - dim), 1) == 0).astype(F32).astype(BF16)
    lane = lax.broadcasted_iota(jnp.int32, (128, 128), 1)
    row = lax.broadcasted_iota(jnp.int32, (128, 128), 0)
    past, before = lane > row, lane < row

    def bias_col(ref):
        pick = lax.broadcasted_iota(jnp.int32, ref.shape, 0) == chip
        r = jnp.sum(jnp.where(pick, ref[...], 0.0), axis=0, keepdims=True)
        return jnp.broadcast_to(r, (128, dim)).T[:, :1]

    u_col, v_col = bias_col(ub), bias_col(vb)

    def skew(t):
        return pltpu.roll(t, 1, 1, stride=1, stride_axis=0)

    def slot_cols(k):
        return pl.ds(aligned(k * BQ, BQ), BQ)

    def transposed(x):
        return x.astype(F32).T.astype(BF16)

    def prepare(k):
        q = qT[:, slot_cols(k)].astype(F32)
        quT, qvT = (q + u_col).astype(BF16), (q + v_col).astype(BF16)
        q_off[k, :, :KX] = jnp.concatenate([transposed(qvT), ones_col], 1)
        q_col[k] = flip_lanes(quT, eye)
        q_row[k, :, :dim] = transposed(q_col[k])
        qo_col[k] = flip_lanes(qvT, eye)

    def prepare_skew(k, i, t):
        start = seq - row_block(k) * BQ + t * BK - 256
        t0 = dot_nn(q_off[k, :, :KX], relX[:, pl.ds(aligned(start, 128), 256)])
        r_scr[i, :, :128], r_scr[i, :, 128:] = skew(t0[:, :128]), skew(t0[:, 128:])

    def scores(tile, k, t):
        j0 = aligned(t * BK, BK)
        base = seq - row_block(k) * BQ
        by_offset = dot_nn(q_off[k, :, :KX], relX[:, pl.ds(aligned(base + j0, 128), BK)])
        content = dot_nn(q_row[k, :, :dim], kT[:, pl.ds(j0, BK)])
        ri = jnp.where(lax.rem(t, GROUP) == 0, lax.rem(k, GROUP), GROUP)
        rolled = [r_scr[ri, :, :128], r_scr[ri, :, 128:]]
        rolled += [skew(by_offset[:, m * 128:(m + 1) * 128]) for m in range(NC)]
        top_s = mx[k]
        for m in range(NC):
            top = jnp.where(past, rolled[m + 2][:128], rolled[m + 1][:128])
            bot = jnp.where(past, rolled[m + 1][128:], rolled[m][128:])
            s = content[:, m * 128:(m + 1) * 128] + reverse_rows(jnp.concatenate([top, bot], 0))
            s = s * (scale * LOG2E)
            s_all[tile, :, m * 128:(m + 1) * 128] = s
            top_s = jnp.maximum(top_s, s)
        mx[k] = top_s
        r_scr[GROUP, :, :128], r_scr[GROUP, :, 128:] = rolled[NC], rolled[NC + 1]

    def weigh(tile, k, t):
        top_s, tot = mx[k], total[k]
        parts = []
        for m in range(NC):
            p = jnp.exp2(s_all[tile, :, m * 128:(m + 1) * 128] - top_s)
            s_all[tile, :, m * 128:(m + 1) * 128] = p
            tot = tot + p
            parts.append(p.astype(BF16))
        total[k] = tot
        acc[k, :, :dim] += dot_nt(jnp.concatenate(parts, 1), vT[:, pl.ds(aligned(t * BK, BK), BK)])

    def finish_rows(k):
        do_col[k] = flip_lanes(doT[:, slot_cols(k)], eye)
        do_row[k] = transposed(do_col[k])
        inv = 1.0 / jnp.sum(total[k], axis=1, keepdims=True)
        out = acc[k, :, :dim] * inv
        delta = jnp.sum(do_row[k].astype(F32) * out, axis=1, keepdims=True)
        total[k] = jnp.broadcast_to(inv, (BQ, 128))
        mx[k] = jnp.broadcast_to(delta, (BQ, 128))
        oT[:, slot_cols(k)] = flip_lanes(out.T.astype(BF16), eye)
        acc[k] = jnp.zeros((BQ, 2 * dim), F32)

    def score_grads(k, t):
        return dot_nn(do_row[k], vT[:, pl.ds(aligned(t * BK, BK), BK)])

    def split_grads(tile, k, t, dp):
        inv, delta = total[k], mx[k]
        carry = (q_off, q_row)
        ps, dss = [], []
        held = [jnp.where(t > 0, c[k], jnp.zeros((BQ, 128), BF16)) for c in carry]
        for m in range(NC):
            p = s_all[tile, :, m * 128:(m + 1) * 128] * inv
            ds = (p * ((dp[:, m * 128:(m + 1) * 128] - delta) * scale)).astype(BF16)
            ps.append(p.astype(BF16))
            dss.append(ds)
            held.append(pltpu.roll(ds, 0, 1, stride=1, stride_axis=0))
        for m in range(2):
            carry[m][k] = held[NC + m]
        by_offset = []
        for m in range(NC):
            top = jnp.where(before, held[m + 1][:128], held[m + 2][:128])
            bot = jnp.where(before, held[m][128:], held[m + 1][128:])
            by_offset.append(jnp.concatenate([top, bot], 0))
        return tuple(jnp.concatenate(x, 1) for x in (ps, dss, by_offset))

    def add_grads(k, t, p_all, ds_all, by_offset):
        j0 = aligned(t * BK, BK)
        base = seq - row_block(k) * BQ
        js, us = pl.ds(j0, BK), pl.ds(aligned(base + j0 - 256, 128), BK)
        dvT[:, js] += dot_nn(do_col[k], p_all)
        dkT[:, js] += dot_nn(q_col[k], ds_all)
        drF[:, us] += dot_nn(qo_col[k], by_offset)
        none = jnp.zeros((dim, BK), BF16)
        keys = jnp.concatenate([jnp.concatenate([kT[:, js], none], 0), jnp.concatenate([none, relX[:dim, us]], 0)], 1)
        acc[k] += dot_nt(jnp.concatenate([ds_all, by_offset], 1), keys)

    def walk(steps, count, k, t_low, t_cap):
        def some(i, kt):
            k, t = kt
            at = []
            for u in range(UNROLL):
                at.append((k, t))
                last = t == jnp.minimum(k, t_cap)
                k, t = jnp.where(last, k + 1, k), jnp.where(last, t_low, t + 1)
            steps(at)
            return k, t

        lax.fori_loop(0, count // UNROLL, some, (k, t_low))

    def tile_of(k, t):
        return k * (k + 1) // 2 + t

    def grads(at):
        d0 = score_grads(*at[0])
        d1 = score_grads(*at[1])
        g0 = split_grads(tile_of(*at[0]), *at[0], d0)
        add_grads(*at[0], *g0)
        d2 = score_grads(*at[2])
        g1 = split_grads(tile_of(*at[1]), *at[1], d1)
        add_grads(*at[1], *g1)
        g2 = split_grads(tile_of(*at[2]), *at[2], d2)
        add_grads(*at[2], *g2)

    def group_tiles(g):
        return GROUP * GROUP * g + GROUP * (GROUP + 1) // 2

    def over_tiles(step, g):
        def steps(at):
            for k, t in at:
                step(tile_of(k, t), k, t)

        walk(steps, group_tiles(g), GROUP * g, 0, nslot)

    def each(fn):
        lax.fori_loop(0, groups, lambda g, c: (fn(g), c)[1], 0)

    orders = (((0, 0), (1, 1), (1, 0), (3, 0), (3, 1), (3, 3), (2, 0), (2, 1), (2, 2), (3, 2)),
              ((1, 1), (0, 0), (1, 0), (3, 0), (3, 1), (3, 3), (2, 0), (2, 1), (2, 2), (3, 2)),
              ((2, 2), (3, 3), (3, 2), (0, 0), (2, 0), (3, 0), (1, 1), (1, 0), (2, 1), (3, 1)),
              ((3, 3), (2, 2), (3, 2), (0, 0), (2, 0), (3, 0), (1, 1), (1, 0), (2, 1), (3, 1)))

    def schedule(order):
        seen = ([], [], [])
        rows = []
        for gq, gk in order:
            row = [gq, gk]
            for t, g in ((0, gq - gk), (0, gq - gk - 1), (1, gk), (2, gq)):
                new = g >= 0 and g not in seen[t]
                row.append(g if new else -1)
                if new:
                    seen[t].append(g)
            rows.append(row)
        return rows

    schedules = [schedule(order) for order in orders]

    def look_up(x, column):
        value = jnp.int32(-1)
        for at in range(len(orders[0])):
            here = jnp.int32(schedules[-1][at][column])
            for z in range(groups - 1):
                here = jnp.where(chip == z, schedules[z][at][column], here)
            value = jnp.where(x == at, here, value)
        return value

    def forward_scores(x):
        gq, gk, *need, new_q = (look_up(x, column) for column in range(6))
        *ahead, ahead_q = (look_up(x + 1, column) for column in range(2, 6))

        def arrives_now(g, q):
            return (q >= 0) & ((g < groups // 2) != lower)

        for t, g in zip((0, 0, 1), need):
            pl.when((g >= 0) & ((x == 0) | arrives_now(g, new_q)))(functools.partial(pass_on, t, g))
        for t, g, g1 in zip((0, 0, 1), need, ahead):
            pl.when((g1 >= 0) & ~arrives_now(g1, ahead_q))(functools.partial(pass_on, t, g1))
            pl.when(g >= 0)(functools.partial(from_mate, t, g))

        @pl.when(new_q >= 0)
        def _():
            for i in range(GROUP):
                row_landed(0, GROUP * new_q + i)
            for i in range(GROUP):
                prepare(GROUP * new_q + i)

        pl.when(x == VALUES_AT)(send_values)
        for i in range(GROUP):
            prepare_skew(GROUP * gq + i, i, GROUP * gk)
        count = jnp.where(gq == gk, GROUP * (GROUP + 1) // 2, GROUP * GROUP)
        walk(score_tiles, count, GROUP * gq, GROUP * gk, GROUP * gk + GROUP - 1)

    def score_tiles(at):
        for k, t in at:
            scores(tile_of(k, t), k, t)

    lax.fori_loop(0, len(orders[0]), lambda x, c: (forward_scores(x), c)[1], 0)
    send_cotangent()
    each(lambda g: pass_on(2, g))

    def row_max(g):
        for i in range(GROUP):
            k = GROUP * g + i
            mx[k] = jnp.broadcast_to(jnp.max(mx[k], axis=1, keepdims=True), (BQ, 128))

    each(row_max)

    def weigh_group(g):
        from_mate(2, g)
        over_tiles(weigh, g)

    each(weigh_group)

    def out_rows(t, k, wait):
        rb = row_block(k)
        to, j = rb // per_blk, lax.rem(rb, per_blk)
        src = (oT, dqT)[t].at[:, slot_cols(k)]
        dst = (o_out, dq_out)[t].at[chip, :, pl.ds(aligned(j * BQ, BQ), BQ)]

        @pl.when(to != me)
        def _():
            c = remote_copy(src, dst, send_o.at[t, k], recv_o.at[t, chip, j], to)
            c.wait_send() if wait else c.start()

        @pl.when(to == me)
        def _():
            c = pltpu.make_async_copy(src, dst, loc_o.at[t, j])
            c.wait() if wait else c.start()

    def finish_group(g):
        for i in range(GROUP):
            row_landed(1, GROUP * g + i)
        for i in range(GROUP):
            finish_rows(GROUP * g + i)
        for i in range(GROUP):
            out_rows(0, GROUP * g + i, False)

    each(finish_group)

    parts, sinks = (drF, dkT, dvT), (dr_buf, dk_out, dv_out)

    hw = blk // 2
    slots = pair_buf.shape[1]

    def out_block(t, step):
        return n - 1 - step if t == 0 else jnp.where(lower, n - 1 - step, step)

    def half_of(t, step, c):
        b = out_block(t, step)
        b = n - 1 - b if t == 0 else b
        return pl.ds(aligned(b * blk + c * hw, 128), hw)

    def pair(t, step):
        s = lax.rem(step, slots)
        return remote_copy(parts[t].at[:, half_of(t, step, 1 - core)], pair_buf.at[t, s], send_p.at[t, s], recv_p.at[t, s], mate)

    def ready(t, step):
        return dr_send.at[step] if t == 0 else send_buf.at[t - 1, step]

    def sink_at(t, h, c):
        return sinks[t].at[h, :, pl.ds(aligned(c * hw, 128), hw)]

    def sink(t, step):
        return remote_copy(ready(t, step), sink_at(t, chip, core), send_s.at[t, step], recv_s.at[t, chip, core], out_block(t, step))

    def keep(t, step):
        return pltpu.make_async_copy(ready(t, step), sink_at(t, chip, core), loc_s.at[t])

    def combine(t, step):
        s = lax.rem(step, slots)
        mine = half_of(t, step, core)
        remote_copy(parts[t].at[:, mine], pair_buf.at[t, s], send_p.at[t, s], recv_p.at[t, s], mate).wait_recv()
        ready(t, step)[...] = (parts[t][:, mine] + pair_buf[t, s]).astype(BF16)

    def to_owner(t, step, wait):
        b = out_block(t, step)

        @pl.when(b != me)
        def _():
            sink(t, step).wait_send() if wait else sink(t, step).start()

        @pl.when(b == me)
        def _():
            keep(t, step).wait() if wait else keep(t, step).start()

    def arrived(t):
        for h in range(heads):
            for c in range(2):
                @pl.when(2 * h + c != me)
                def _():
                    remote_copy(ready(t, 0), sink_at(t, h, c), send_s.at[t, 0], recv_s.at[t, h, c], me).wait_recv()

    def final_slots(step, fn):
        first, end = (3 * step + 1) // 2, (3 * step + 4) // 2
        for i in range(2):
            at = first + i
            pl.when(at < end)(functools.partial(fn, jnp.where(lower, nslot - 1 - at, at)))

    def row_grads(k):
        dqT[:, slot_cols(k)] = flip_lanes((acc[k, :, :dim] + acc[k, :, dim:]).T.astype(BF16), eye)

    def exchange(step):
        for t in range(3):
            pl.when(step >= slots)(pair(t, step - slots).wait_send)
            pair(t, step).start()
        final_slots(step, row_grads)

    def release(step):
        combine(0, step)
        to_owner(0, step, False)
        for t in (1, 2):
            combine(t, step)
        for t in (1, 2):
            to_owner(t, step, False)
        final_slots(step, lambda k: out_rows(1, k, False))

    w_acc, w_in, w_half, w_part, w_mine = (9, 0), (10, 0), (10, 1), (11, 0), (11, 1)
    chunks, wide = range(4), BK // 2
    half = heads * dim // 2
    piece = half // heads

    def place(kt, c, row0, count):
        at = kt[0] * (kt[0] + 1) // 2 + kt[1]
        return s_all.at[at, pl.ds(row0, count), pl.ds(c % 2 * wide, wide)]

    def acc_at(c, row0, count):
        return place((w_acc[0], w_acc[1] + c // 2), c, row0, count)

    def swap(c):
        return remote_copy(acc_at(c, aligned((1 - core) * half, half), half), place(w_in, c, c // 2 * half, half),
                           send_w.at[0, c], recv_w.at[0, c], mate)

    def spread(i, c):
        z = lax.rem(chip + i, heads)
        return remote_copy(place(w_half, c, aligned(c // 2 * half + z * piece, piece), piece),
                           place(w_part, c, (2 * i + c // 2) * piece, piece), send_w.at[i, c], recv_w.at[i, c], 2 * z + core)

    def table_grad():
        arrived(0)
        keep(0, 0).wait()
        dr = jnp.concatenate([flip_lanes(dr_buf[h], eye) for h in range(heads)], 0)
        for c in chunks:
            acc_at(c, 0, 2 * half)[...] = dot_nn(dr, table[:, c * wide:(c + 1) * wide])
        for c in chunks:
            swap(c).start()
        for c in chunks:
            swap(c).wait()
            place(w_half, c, c // 2 * half, half)[...] = (
                acc_at(c, aligned(core * half, half), half)[...] + place(w_in, c, c // 2 * half, half)[...])
        for c in chunks:
            for i in (3, 2, 1):
                spread(i, c).start()

    bodies, done = [], 0
    for step in range(n):
        tiles_done = sum(nslot - i for i in range((3 * step + 4) // 2))
        bodies.append(-(-tiles_done // UNROLL) - done)
        done += bodies[-1]
    phases = [c for b in bodies[:-1] for c in (min(b, 1), max(b - 1, 0))]

    def next_tile(k, t):
        last = jnp.where(lower, t == k, k == nslot - 1)
        k1 = jnp.where(lower, k - 1, t + 1)
        return (jnp.where(last, k1, jnp.where(lower, k, k + 1)), jnp.where(last, jnp.where(lower, 0, t + 1), jnp.where(lower, t + 1, t)))

    def phase(x, kt):
        count = jnp.int32(0)
        for at, c in enumerate(phases):
            count = jnp.where(x == at, c, count)

        def some(i, kt):
            at = []
            for u in range(UNROLL):
                at.append(kt)
                kt = next_tile(*kt)
            grads(at)
            return kt

        kt = lax.fori_loop(0, count, some, kt)
        pl.when(lax.rem(x, 2) == 1)(lambda: exchange(x // 2))
        pl.when((lax.rem(x, 2) == 0) & (x > 0))(lambda: release(x // 2 - 1))
        return kt

    lax.fori_loop(0, len(phases), phase, (jnp.where(lower, nslot - 1, 0), jnp.int32(0)))
    exchange(n - 1)
    release(n - 2)
    release(n - 1)
    rows_sum = jnp.sum(jnp.sum(acc[...].reshape(nslot * BQ // 8, 8, 2 * dim), axis=0), axis=0, keepdims=True)
    for t in range(2):
        bias_buf[me, t] = rows_sum[:, t * dim:(t + 1) * dim] + jnp.zeros((8, dim), F32)

    def bias(o):
        return remote_copy(bias_buf.at[me], bias_buf.at[me], send_b.at[o], recv_b2.at[me], lax.rem(me + o, n))

    for o in range(1, n):
        bias(o).start()
    table_grad()

    def home(co, z, c):
        return dw_out.at[pl.ds(aligned(co * half + z * piece, piece), piece), pl.ds(c * wide, wide)]

    def my_piece(c):
        return place(w_mine, c, c // 2 * piece, piece)

    def collect(i, c):
        z = lax.rem(chip + i, heads)
        return remote_copy(my_piece(c), home(core, chip, c), send_w.at[4 + i, c], recv_w.at[4 + chip, c], 2 * z + core)

    def hand_over(i, c):
        z = lax.rem(chip + i, heads)
        return remote_copy(my_piece(c) if i == 0 else home(core, z, c), home(core, z, c), send_w.at[8 + i, c], recv_w.at[8 + z, c], mate)

    def stay(c):
        return pltpu.make_async_copy(my_piece(c), home(core, chip, c), loc_w.at[c])

    for c in chunks:
        for i in range(1, heads):
            spread(i, c).wait()
        got = place(w_half, c, aligned(c // 2 * half + chip * piece, piece), piece)[...]
        for i in range(1, heads):
            got = got + place(w_part, c, (2 * i + c // 2) * piece, piece)[...]
        my_piece(c)[...] = got
        for i in range(1, heads):
            collect(i, c).start()
        hand_over(0, c).start()
        stay(c).start()
    for c in chunks:
        for i in range(1, heads):
            z = lax.rem(chip + i, heads)
            remote_copy(my_piece(c), home(core, z, c), send_w.at[0, c], recv_w.at[4 + z, c], me).wait_recv()
            hand_over(i, c).start()
    for o in range(1, n):
        b = lax.rem(me + o, n)
        remote_copy(bias_buf.at[b], bias_buf.at[b], send_b.at[0], recv_b2.at[b], me).wait_recv()
    for t in range(2):
        bias_out[t] = jnp.concatenate([bias_buf[2 * h, t, :1] + bias_buf[2 * h + 1, t, :1] for h in range(heads)], 0)

    for c in chunks:
        stay(c).wait()
        for i in range(heads):
            remote_copy(my_piece(c), home(1 - core, i, c), send_w.at[0, c], recv_w.at[8 + i, c], me).wait_recv()
            hand_over(i, c).wait_send()
            if i:
                collect(i, c).wait_send()
    for o in range(1, n):
        bias(o).wait_send()
    for step in range(n):
        pl.when(out_block(0, step) != me)(sink(0, step).wait_send)
    for t in range(3):
        for step in range(n - slots, n):
            pair(t, step).wait_send()
        if t:
            for step in range(n):
                to_owner(t, step, True)
            arrived(t)
        if t:
            to_mate(t).wait_send()
        for i in range(1, heads):
            h = lax.rem(chip + i, heads)
            forward(t, h).wait_send()
            if t:
                direct(t, h).wait_send()
    for t in (0, 1):
        for i in range(heads):
            for j in range(per_blk):
                to = 2 * i + owner_core(me * per_blk + j)

                @pl.when(to != me)
                def _():
                    remote_copy((q_in, do_in)[t].at[0, :, pl.ds(0, BQ)], (qT, doT)[t].at[:, pl.ds(0, BQ)],
                                send_q.at[t, i, j], recv_q.at[t, 0], to).wait_send()
        for k in range(nslot):
            out_rows(t, k, True)
        for h in range(heads):
            for j in range(per_blk):
                @pl.when(2 * h + owner_core(me * per_blk + j) != me)
                def _():
                    remote_copy((oT, dqT)[t].at[:, pl.ds(0, BQ)], (o_out, dq_out)[t].at[h, :, pl.ds(j * BQ, BQ)],
                                send_o.at[t, 0], recv_o.at[t, h, j], me).wait_recv()


def solution(mesh):
    n = mesh.shape['cp']
    seq_spec, head_spec, weight_spec = P('cp', 'hp', None), P('hp', None), P(None, 'hp', None)
    vmem = pl.BlockSpec(memory_space=pltpu.VMEM)
    hbm = pl.BlockSpec(memory_space=pl.ANY)
    dma, sds, buf = pltpu.SemaphoreType.DMA, jax.ShapeDtypeStruct, pltpu.VMEM

    def local_fn(q, k, v, u_bias, v_bias, rel_table, w_rel, d_out):
        blk, heads, dim = q.shape
        seq = n * blk
        rows = seq // 2
        nslot = rows // BQ
        per_blk = blk // BQ
        tiles = nslot * (nslot + 1) // 2
        qT, kT, vT, doT = (x.transpose(1, 2, 0) for x in (q, k, v, d_out))
        wT = w_rel.transpose(1, 2, 0).reshape(heads * dim, -1)
        model = wT.shape[1]
        o, dq, dk, dvv, dw, bias = pl.pallas_call(
            functools.partial(attention_kernel, n),
            out_shape=[sds((heads, dim, blk), BF16)] * 4 + [sds((heads * dim, model), F32), sds((2, heads, dim), F32)],
            in_specs=[hbm] * 5 + [vmem] * 3, out_specs=[hbm] * 5 + [vmem],
            scratch_shapes=[
                buf((dim, rows), BF16), buf((dim, rows), BF16), buf((dim, seq), BF16), buf((dim, seq), BF16), buf((KX, seq + PAD), BF16),
                buf((dim, rows), BF16), buf((dim, rows), BF16), buf((dim, seq), F32), buf((dim, seq), F32), buf((dim, seq + PAD), F32),
                buf((tiles, BQ, BK), F32), buf((nslot, BQ, 128), BF16), buf((nslot, BQ, 128), BF16), buf((nslot, BQ, dim), BF16),
                buf((nslot, dim, BQ), BF16), buf((nslot, dim, BQ), BF16), buf((nslot, dim, BQ), BF16),
                buf((nslot, BQ, 128), F32), buf((nslot, BQ, 128), F32), buf((nslot, BQ, 2 * dim), F32),
                buf((GROUP + 1, BQ, 256), F32),
                buf((3, 4, dim, blk // 2), F32), buf((n, dim, blk // 2), BF16), buf((2, n, dim, blk // 2), BF16), buf((heads, dim, blk), BF16), buf((blk, model), BF16),
                buf((n, 2, 8, dim), F32),
                dma((3, heads)), dma((3, heads)), dma((2, heads, per_blk)), dma((3, n)), dma((2, nslot)), dma((3,)), dma((2, per_blk)),
                dma((2, nslot)), dma((2, heads, per_blk)), dma((2, per_blk)), dma((3, 4)), dma((3, 4)),
                dma((3, n)), dma((3, heads, 2)), dma((3,)),
                dma, dma((12, 4)), dma((12, 4)), dma((4,)), dma((n,)), dma((n,))],
            compiler_params=pltpu.CompilerParams(collective_id=0, has_side_effects=True, vmem_limit_bytes=67043328),
            name='attention',
        )(qT, kT, vT, doT, rel_table, wT, u_bias, v_bias)
        steps = 2
        part = pl.BlockSpec((heads // steps, dim, blk), lambda i: (i, 0, 0))
        wide = pl.BlockSpec((heads * dim // steps, model), lambda i: (i, 0))
        whole = lambda *shape: pl.BlockSpec(shape, lambda i: (0,) * len(shape))
        o, dq, dk, dvv, dw, du, dv = pl.pallas_call(
            hand_off_kernel, grid=(steps,),
            out_shape=[sds((heads, dim, blk), BF16)] * 4 + [sds((heads * dim, model), F32)] + [sds((heads, dim), F32)] * 2,
            in_specs=[part] * 4 + [wide, whole(2, heads, dim)],
            out_specs=[part] * 4 + [wide, whole(heads, dim), whole(heads, dim)],
            name='hand_off',
        )(o, dq, dk, dvv, dw, bias)
        back = lambda x: x.transpose(2, 0, 1)
        return back(o), back(dq), back(dk), back(dvv), du, dv, back(dw.reshape(heads, dim, model))

    return jax.shard_map(
        local_fn, mesh=mesh,
        in_specs=(seq_spec, seq_spec, seq_spec, head_spec, head_spec, P('cp', None), weight_spec, seq_spec),
        out_specs=(seq_spec, seq_spec, seq_spec, seq_spec, head_spec, head_spec, weight_spec),
        check_vma=False,
    )
```

```python
import functools
import math
import jax
import jax.numpy as jnp
from jax import lax
from jax.experimental import pallas as pl
from jax.experimental.pallas import tpu as pltpu
from jax.sharding import PartitionSpec as P

F32, BF16 = jnp.float32, jnp.bfloat16
LOG2E = math.log2(math.e)
BQ = 256
BK = 512
LANES = 128
NC = BK // LANES
PAD = 512
KX = 80
GROUP = 3
UNROLL_SUM = 13
UNROLL_GRAD = 6
VALUES_AT = 6
MESH_ID = pl.DeviceIdType.MESH


def dot_nn(a, b):
    return lax.dot_general(a, b, (((1,), (0,)), ((), ())), preferred_element_type=F32)


def dot_nt(a, b):
    return lax.dot_general(a, b, (((1,), (1,)), ((), ())), preferred_element_type=F32)


def lanes(m, count=1):
    return slice(m * LANES, (m + count) * LANES)


def aligned(x, m):
    return pl.multiple_of(x, m)


def anti_eye(n):
    rows = lax.broadcasted_iota(jnp.int32, (n, n), 0)
    cols = lax.broadcasted_iota(jnp.int32, (n, n), 1)
    return (rows + cols == n - 1).astype(F32).astype(BF16)


def flip_lanes(x, eye):
    n, w = x.shape[1], eye.shape[0]
    parts = [dot_nn(x[:, s:s + w], eye).astype(BF16) for s in range(0, n, w)]
    return jnp.concatenate(parts[::-1], axis=1)


def reverse_rows(x):
    ix = 7 - lax.broadcasted_iota(jnp.int32, (8, x.shape[1]), 0)
    n = x.shape[0] // 8
    return jnp.concatenate([jnp.take_along_axis(x[(n - 1 - g) * 8:(n - g) * 8], ix, axis=0) for g in range(n)], 0)


def owner_core(rb):
    return lax.rem(rb + rb // 2, 2)


def remote_copy(src, dst, send_sem, recv_sem, to):
    return pltpu.make_async_remote_copy(src, dst, send_sem, recv_sem, device_id=(lax.axis_index('hp'), to),
                                        device_id_type=MESH_ID)


def greet_all(n):
    me, hp = lax.axis_index('cp'), lax.axis_index('hp')
    bar = pltpu.get_barrier_semaphore()
    for o in range(1, n):
        pl.semaphore_signal(bar, 1, device_id=(hp, lax.rem(me + o, n)), device_id_type=MESH_ID)


def await_all(n):
    pl.semaphore_wait(pltpu.get_barrier_semaphore(), n - 1)


def hand_off_kernel(o, dq, dk, dv, dw, bias, o_out, dq_out, dk_out, dv_out, dw_out, u_out, v_out):
    for src, dst in ((o, o_out), (dq, dq_out), (dk, dk_out), (dv, dv_out), (dw, dw_out)):
        dst[...] = src[...]
    u_out[...], v_out[...] = bias[0], bias[1]


def attention_kernel(n, q_in, k_in, v_in, do_in, table_in, w_rel, ub, vb,
                     o_out, dq_out, dk_out, dv_out, dw_out, bias_out,
                     qT, doT, kT, vT, relX, oT, dqT, dkT, dvT, drF,
                     s_all, q_off, q_row, do_row, q_col, qo_col, do_col, mx, total, acc, r_scr,
                     pair_buf, dr_send, send_buf, dr_buf, table, bias_buf,
                     send_d, send_f, send_q, recv_b, recv_q, loc_b, loc_q,
                     send_o, recv_o, send_p, recv_p, send_s, recv_s,
                     loc_t, send_w, recv_w, loc_w, send_b, recv_b2,
                     recv_u, recv_d2, recv_c, recv_h, send_x):
    me = lax.axis_index('cp')
    chip, core = me // 2, lax.rem(me, 2)
    mate = 2 * chip + 1 - core
    heads, dim, blk = q_in.shape
    seq = n * blk
    per_blk = blk // BQ
    groups = n // 2
    nslot = qT.shape[1] // BQ
    tiles = s_all.shape[0]
    scale = dim ** -0.5
    model = table.shape[1]

    def weight_block(m):
        return pltpu.make_async_copy(w_rel.at[:, pl.ds(m * LANES, LANES)], q_off.at[m], loc_t.at[1 + m])

    greet_all(n)
    pltpu.make_async_copy(table_in, table, loc_t.at[0]).start()
    for m in range(model // LANES):
        weight_block(m).start()

    rel_buf = dr_buf
    srcs, fulls = (rel_buf, k_in, v_in), (relX, kT, vT)

    def col(t, b, flipped):
        b = (n - 1 - b) if t == flipped else b
        return pl.ds(aligned(b * blk, blk), blk)

    def full_at(t, b):
        return fulls[t].at[pl.ds(0, dim), col(t, b, 0)]

    def direct(t, h):
        return remote_copy(srcs[t].at[h], full_at(t, me), send_d.at[t, h], recv_b.at[t, me], 2 * h + core)

    def own(t):
        return pltpu.make_async_copy(srcs[t].at[chip], full_at(t, me), loc_b.at[t])

    def to_mate(t):
        return remote_copy(srcs[t].at[chip], full_at(t, me), send_f.at[t, chip], recv_b.at[t, me], mate)

    def forward(t, g):
        b = 2 * g + core
        return remote_copy(full_at(t, b), full_at(t, b), send_f.at[t, g], recv_b.at[t, b], mate)

    def landed(t, b):
        remote_copy(srcs[t].at[0], full_at(t, b), send_f.at[t, 0], recv_b.at[t, b], me).wait_recv()

    def pass_on(t, g):
        @pl.when(g != chip)
        def _():
            landed(t, 2 * g + core)
            forward(t, g).start()

        pl.when(g == chip)(own(t).wait)

    def from_mate(t, g):
        landed(t, 2 * g + 1 - core)

    def row_copy(t, h, j, wait):
        rb = me * per_blk + j
        src = (q_in, do_in)[t].at[h, :, pl.ds(j * BQ, BQ)]
        dst = (qT, doT)[t].at[:, pl.ds(aligned(rb // 2 * BQ, BQ), BQ)]
        to = 2 * h + owner_core(rb)

        @pl.when(to != me)
        def _():
            c = remote_copy(src, dst, send_q.at[t, h, j], recv_q.at[t, rb // 2], to)
            c.wait_send() if wait else c.start()

        @pl.when(to == me)
        def _():
            c = pltpu.make_async_copy(src, dst, loc_q.at[t, j])
            c.wait() if wait else c.start()

    def row_block(k):
        return 2 * k + lax.rem(k + core, 2)

    def row_landed(t, k):
        src = (q_in, do_in)[t].at[0, :, pl.ds(0, BQ)]
        dst = (qT, doT)[t].at[:, pl.ds(aligned(k * BQ, BQ), BQ)]
        rb = row_block(k)

        @pl.when(rb // per_blk != me)
        def _():
            remote_copy(src, dst, send_q.at[t, 0, 0], recv_q.at[t, k], me).wait_recv()

        @pl.when(rb // per_blk == me)
        def _():
            pltpu.make_async_copy(src, dst, loc_q.at[t, lax.rem(rb, per_blk)]).wait()

    lower = chip < groups // 2
    side = chip + 1 - 2 * lax.rem(chip, 2)
    near, far = jnp.where(lower, groups // 2, groups // 2 - 1), jnp.where(lower, groups - 1, 0)
    across = near, far

    def send_rows(t, h):
        for j in range(per_blk):
            row_copy(t, h, j, False)

    def send_scores_input(h):
        direct(1, h).start()
        send_rows(0, h)

    eye = anti_eye(BQ)
    pltpu.make_async_copy(table_in, table, loc_t.at[0]).wait()
    for m in range(model // LANES):
        weight_block(m).wait()
    weights_in = jnp.concatenate([q_off[m] for m in range(model // LANES)], 1)
    rel = flip_lanes(dot_nt(weights_in, table[...]).astype(BF16), eye)
    for h in range(heads):
        rel_buf[h] = rel[h * dim:(h + 1) * dim]
    await_all(n)
    to_mate(1).start()
    own(1).start()
    send_scores_input(side)
    send_rows(0, chip)
    to_mate(0).start()
    own(0).start()
    for h in (side, *across):
        direct(0, h).start()
    for h in across:
        send_scores_input(h)

    def send_values():
        to_mate(2).start()
        own(2).start()
        for h in (side, *across):
            direct(2, h).start()

    def send_cotangent():
        for h in (side, *across):
            direct(0, h).wait_send()
        to_mate(0).wait_send()
        for h in (side, *across, chip):
            send_rows(1, h)

    for ref in (dkT, dvT, drF, total, acc):
        ref[...] = jnp.zeros_like(ref)
    mx[...] = jnp.full(mx.shape, -jnp.inf, F32)
    relX[pl.ds(0, dim), pl.ds(seq, PAD)] = jnp.zeros((dim, PAD), BF16)
    first = lax.broadcasted_iota(jnp.int32, (KX - dim, PAD), 0) == 0
    relX[pl.ds(dim, KX - dim), pl.ds(0, seq)] = jnp.zeros((KX - dim, seq), BF16)
    relX[pl.ds(dim, KX - dim), pl.ds(seq, PAD)] = jnp.where(first, -jnp.inf, 0.0).astype(BF16)
    ones_col = (lax.broadcasted_iota(jnp.int32, (BQ, KX - dim), 1) == 0).astype(F32).astype(BF16)
    lane = lax.broadcasted_iota(jnp.int32, (128, LANES), 1)
    row = lax.broadcasted_iota(jnp.int32, (128, LANES), 0)
    past, before = lane > row, lane < row

    def bias_col(ref):
        pick = lax.broadcasted_iota(jnp.int32, ref.shape, 0) == chip
        r = jnp.sum(jnp.where(pick, ref[...], 0.0), axis=0, keepdims=True)
        return jnp.broadcast_to(r, (LANES, dim)).T[:, :1]

    u_col, v_col = bias_col(ub), bias_col(vb)

    def skew(t):
        return pltpu.roll(t, 1, 1, stride=1, stride_axis=0)

    def slot_cols(k):
        return pl.ds(aligned(k * BQ, BQ), BQ)

    def transposed(x):
        return x.astype(F32).T.astype(BF16)

    def prepare(k):
        q = qT[:, slot_cols(k)].astype(F32)
        quT, qvT = (q + u_col).astype(BF16), (q + v_col).astype(BF16)
        q_off[k, :, :KX] = jnp.concatenate([transposed(qvT), ones_col], 1)
        q_col[k] = flip_lanes(quT, eye)
        q_row[k, :, :dim] = transposed(q_col[k])
        qo_col[k] = flip_lanes(qvT, eye)

    def prepare_skew(k, i, t):
        start = seq - row_block(k) * BQ + t * BK - 256
        t0 = dot_nn(q_off[k, :, :KX], relX[:, pl.ds(aligned(start, LANES), 256)])
        for m in range(2):
            r_scr[i, :, lanes(m)] = skew(t0[:, lanes(m)])

    def score_products(k, t):
        j0 = aligned(t * BK, BK)
        base = seq - row_block(k) * BQ
        by_offset = dot_nn(q_off[k, :, :KX], relX[:, pl.ds(aligned(base + j0, LANES), BK)])
        return by_offset, dot_nn(q_row[k, :, :dim], kT[:, pl.ds(j0, BK)])

    def scores(k, t, by_offset, content):
        ri = jnp.where(lax.rem(t, GROUP) == 0, lax.rem(k, GROUP), GROUP)
        rolled = [r_scr[ri, :, lanes(m)] for m in range(2)]
        rolled += [skew(by_offset[:, lanes(m)]) for m in range(NC)]
        top_s = mx[k]
        for m in range(NC):
            top = jnp.where(past, rolled[m + 2][:LANES], rolled[m + 1][:LANES])
            bot = jnp.where(past, rolled[m + 1][LANES:], rolled[m][LANES:])
            s = content[:, lanes(m)] + reverse_rows(jnp.concatenate([top, bot], 0))
            s = s * (scale * LOG2E)
            s_all[tile_of(k, t), :, lanes(m)] = s
            top_s = jnp.maximum(top_s, s)
        mx[k] = top_s
        for m in range(2):
            r_scr[GROUP, :, lanes(m)] = rolled[NC + m]

    def weights(k, t):
        tile, top_s, tot = tile_of(k, t), mx[k], total[k]
        parts = []
        for m in range(NC):
            p = jnp.exp2(s_all[tile, :, lanes(m)] - top_s)
            s_all[tile, :, lanes(m)] = p
            tot = tot + p
            parts.append(p.astype(BF16))
        total[k] = tot
        return jnp.concatenate(parts, 1)

    def add_values(k, t, p_all):
        acc[k, :, :dim] += dot_nt(p_all, vT[:, pl.ds(aligned(t * BK, BK), BK)])

    def finish_rows(k):
        do_col[k] = flip_lanes(doT[:, slot_cols(k)], eye)
        do_row[k] = transposed(do_col[k])
        inv = 1.0 / jnp.sum(total[k], axis=1, keepdims=True)
        out = acc[k, :, :dim] * inv
        delta = jnp.sum(do_row[k].astype(F32) * out, axis=1, keepdims=True)
        total[k] = jnp.broadcast_to(inv, (BQ, LANES))
        mx[k] = jnp.broadcast_to(delta, (BQ, LANES))
        oT[:, slot_cols(k)] = flip_lanes(out.T.astype(BF16), eye)
        acc[k] = jnp.zeros((BQ, 2 * dim), F32)

    def score_grads(k, t):
        return dot_nn(do_row[k], vT[:, pl.ds(aligned(t * BK, BK), BK)])

    def split_grads(tile, k, t, dp):
        inv, delta = total[k], mx[k]
        carry = (q_off, q_row)
        ps, dss = [], []
        held = [jnp.where(t > 0, c[k], jnp.zeros((BQ, LANES), BF16)) for c in carry]
        for m in range(NC):
            p = s_all[tile, :, lanes(m)] * inv
            ds = (p * ((dp[:, lanes(m)] - delta) * scale)).astype(BF16)
            ps.append(p.astype(BF16))
            dss.append(ds)
            held.append(pltpu.roll(ds, 0, 1, stride=1, stride_axis=0))
        for m in range(2):
            carry[m][k] = held[NC + m]
        by_offset = []
        for m in range(NC):
            top = jnp.where(before, held[m + 1][:LANES], held[m + 2][:LANES])
            bot = jnp.where(before, held[m][LANES:], held[m + 1][LANES:])
            by_offset.append(jnp.concatenate([top, bot], 0))
        return tuple(jnp.concatenate(x, 1) for x in (ps, dss, by_offset))

    def add_grads(k, t, p_all, ds_all, by_offset):
        j0 = aligned(t * BK, BK)
        base = seq - row_block(k) * BQ
        js, us = pl.ds(j0, BK), pl.ds(aligned(base + j0 - 256, LANES), BK)
        dvT[:, js] += dot_nn(do_col[k], p_all)
        dkT[:, js] += dot_nn(q_col[k], ds_all)
        drF[:, us] += dot_nn(qo_col[k], by_offset)
        none = jnp.zeros((dim, BK), BF16)
        keys = jnp.concatenate([jnp.concatenate([kT[:, js], none], 0), jnp.concatenate([none, relX[:dim, us]], 0)], 1)
        acc[k] += dot_nt(jnp.concatenate([ds_all, by_offset], 1), keys)

    def walk(steps, count, k, t_low, t_cap, unroll):
        def some(i, kt):
            k, t = kt
            at = []
            for u in range(unroll):
                at.append((k, t))
                last = t == jnp.minimum(k, t_cap)
                k, t = jnp.where(last, k + 1, k), jnp.where(last, t_low, t + 1)
            steps(at)
            return k, t

        lax.fori_loop(0, count // unroll, some, (k, t_low))

    def tile_of(k, t):
        return k * (k + 1) // 2 + t

    def grads(at):
        count = len(at)
        dps = [score_grads(*at[0])]
        for u, here in enumerate(at):
            if u + 1 < count:
                dps.append(score_grads(*at[u + 1]))
            add_grads(*here, *split_grads(tile_of(*here), *here, dps[u]))

    def group_tiles(g):
        return GROUP * GROUP * g + GROUP * (GROUP + 1) // 2

    def score_tiles(at):
        products = score_products(*at[0])
        for u, here in enumerate(at):
            ahead = score_products(*at[u + 1]) if u + 1 < len(at) else None
            scores(*here, *products)
            products = ahead

    def weigh_tiles(at):
        p_all = weights(*at[0])
        for u, here in enumerate(at):
            ahead = weights(*at[u + 1]) if u + 1 < len(at) else None
            add_values(*here, p_all)
            p_all = ahead

    def each(fn):
        lax.fori_loop(0, groups, lambda g, c: (fn(g), c)[1], 0)

    orders = ('00111030313320212232', '11001030313320212232', '22333200203011102131', '33223200203011102131')
    orders = [[(int(word[at]), int(word[at + 1])) for at in range(0, len(word), 2)] for word in orders]

    def schedule(order):
        seen = ([], [], [])
        rows = []
        for gq, gk in order:
            row = [gq, gk]
            for t, g in ((0, gq - gk), (0, gq - gk - 1), (1, gk), (2, gq)):
                new = g >= 0 and g not in seen[t]
                row.append(g if new else -1)
                if new:
                    seen[t].append(g)
            rows.append(row)
        return rows

    schedules = [schedule(order) for order in orders]

    def look_up(x, column):
        value = jnp.int32(-1)
        for at in range(len(orders[0])):
            here = jnp.int32(schedules[-1][at][column])
            for z in range(groups - 1):
                here = jnp.where(chip == z, schedules[z][at][column], here)
            value = jnp.where(x == at, here, value)
        return value

    def forward_scores(x):
        gq, gk, *need, new_q = (look_up(x, column) for column in range(6))
        *ahead, ahead_q = (look_up(x + 1, column) for column in range(2, 6))

        def arrives_now(g, q):
            return (q >= 0) & ((g < groups // 2) != lower)

        for t, g in zip((0, 0, 1), need):
            pl.when((g >= 0) & ((x == 0) | arrives_now(g, new_q)))(functools.partial(pass_on, t, g))
        for t, g, g1 in zip((0, 0, 1), need, ahead):
            pl.when((g1 >= 0) & ~arrives_now(g1, ahead_q))(functools.partial(pass_on, t, g1))
            pl.when(g >= 0)(functools.partial(from_mate, t, g))

        @pl.when(new_q >= 0)
        def _():
            for i in range(GROUP):
                row_landed(0, GROUP * new_q + i)
            for i in range(GROUP):
                prepare(GROUP * new_q + i)

        pl.when(x == VALUES_AT)(send_values)
        for i in range(GROUP):
            prepare_skew(GROUP * gq + i, i, GROUP * gk)
        here = GROUP * gq, GROUP * gk, GROUP * gk + GROUP - 1
        pl.when(gq == gk)(lambda: walk(score_tiles, GROUP * (GROUP + 1) // 2, *here, GROUP * (GROUP + 1) // 2))
        pl.when(gq != gk)(lambda: walk(score_tiles, GROUP * GROUP, *here, GROUP * GROUP))

    lax.fori_loop(0, len(orders[0]), lambda x, c: (forward_scores(x), c)[1], 0)
    send_cotangent()
    each(lambda g: pass_on(2, g))

    def row_max(g):
        for i in range(GROUP):
            k = GROUP * g + i
            mx[k] = jnp.broadcast_to(jnp.max(mx[k], axis=1, keepdims=True), (BQ, LANES))

    each(row_max)

    each(lambda g: from_mate(2, g))
    walk(weigh_tiles, tiles, 0, 0, nslot, UNROLL_SUM)

    def out_rows(t, k):
        rb = row_block(k)
        to, j = rb // per_blk, lax.rem(rb, per_blk)
        src = (oT, dqT)[t].at[:, slot_cols(k)]
        dst = (o_out, dq_out)[t].at[chip, :, pl.ds(aligned(j * BQ, BQ), BQ)]
        pl.when(to != me)(lambda: remote_copy(src, dst, send_o.at[t], recv_o.at[t], to).start())
        pl.when(to == me)(lambda: pltpu.make_async_copy(src, dst, recv_o.at[t]).start())

    def rows_done(t):
        src, dst = (oT, dqT)[t], (o_out, dq_out)[t]
        remote_copy(dst, dst, send_o.at[t], recv_o.at[t], mate).wait_recv()
        kept = sum((owner_core(me * per_blk + j) == core).astype(jnp.int32) for j in range(per_blk))
        for count in (1, 2):
            left = src.at[:, pl.ds(0, (nslot - count) * BQ)]
            pl.when(kept == count)(remote_copy(left, left, send_o.at[t], recv_o.at[t], mate).wait_send)

    def finish_group(g):
        for i in range(GROUP):
            row_landed(1, GROUP * g + i)
        for i in range(GROUP):
            finish_rows(GROUP * g + i)
        for i in range(GROUP):
            out_rows(0, GROUP * g + i)

    each(finish_group)

    parts, sinks = (drF, dkT, dvT), (dr_buf, dk_out, dv_out)

    hw = blk // 2
    slots = pair_buf.shape[1]

    def out_block(t, step):
        return n - 1 - step if t == 0 else jnp.where(lower, n - 1 - step, step)

    def half_of(t, step, c):
        b = out_block(t, step)
        b = n - 1 - b if t == 0 else b
        return pl.ds(aligned(b * blk + c * hw, LANES), hw)

    def pair(t, step):
        s = lax.rem(step, slots)
        return remote_copy(parts[t].at[:, half_of(t, step, 1 - core)], pair_buf.at[t, s], send_p.at[t, s], recv_p.at[t, s], mate)

    def ready(t, step):
        return dr_send.at[step] if t == 0 else send_buf.at[t - 1, step]

    def sink_at(t, h, c):
        return sinks[t].at[h, :, pl.ds(aligned(c * hw, LANES), hw)]

    def sink(t, step):
        return remote_copy(ready(t, step), sink_at(t, chip, core), send_s.at[t], recv_s.at[t], out_block(t, step))

    def keep(t, step):
        return pltpu.make_async_copy(ready(t, step), sink_at(t, chip, core), recv_s.at[t])

    def combine(t, step):
        s = lax.rem(step, slots)
        mine = half_of(t, step, core)
        remote_copy(parts[t].at[:, mine], pair_buf.at[t, s], send_p.at[t, s], recv_p.at[t, s], mate).wait_recv()
        ready(t, step)[...] = (parts[t][:, mine] + pair_buf[t, s]).astype(BF16)
        pair(t, step).wait_send()

    def to_owner(t, step):
        b = out_block(t, step)
        pl.when(b != me)(lambda: sink(t, step).start())
        pl.when(b == me)(lambda: keep(t, step).start())

    def arrived(t):
        remote_copy(sinks[t], sinks[t], send_s.at[t], recv_s.at[t], mate).wait_recv()

    def departed(t):
        others = (dr_send if t == 0 else send_buf.at[t - 1]).at[pl.ds(0, n - 1)]
        remote_copy(others, others, send_s.at[t], recv_s.at[t], mate).wait_send()

    def final_slots(step, fn):
        first, end = (3 * step + 1) // 2, (3 * step + 4) // 2
        for i in range(2):
            at = first + i
            pl.when(at < end)(functools.partial(fn, jnp.where(lower, nslot - 1 - at, at)))

    def row_grads(k):
        dqT[:, slot_cols(k)] = flip_lanes((acc[k, :, :dim] + acc[k, :, dim:]).T.astype(BF16), eye)

    def exchange(step):
        for t in range(3):
            pair(t, step).start()
        final_slots(step, row_grads)

    def release(step):
        combine(0, step)
        to_owner(0, step)
        for t in (1, 2):
            combine(t, step)
        for t in (1, 2):
            to_owner(t, step)
        final_slots(step, lambda k: out_rows(1, k))

    w_acc, w_in, w_half, w_part, w_mine = (9, 0), (10, 0), (10, 1), (11, 0), (11, 1)
    chunks, wide = range(4), BK // 2
    half = heads * dim // 2
    piece = half // heads

    def place(kt, c, row0, count):
        at = kt[0] * (kt[0] + 1) // 2 + kt[1]
        return s_all.at[at, pl.ds(row0, count), pl.ds(c % 2 * wide, wide)]

    def acc_at(c, row0, count):
        return place((w_acc[0], w_acc[1] + c // 2), c, row0, count)

    def swap(c):
        return remote_copy(acc_at(c, aligned((1 - core) * half, half), half), place(w_in, c, c // 2 * half, half),
                           send_w.at[c], recv_w.at[c], mate)

    def share(c, z):
        return place(w_half, c, aligned(c // 2 * half + z * piece, piece), piece)

    def from_below(c, z):
        return place(w_part, c, aligned((2 * z + c // 2) * piece, piece), piece)

    def from_above(c, z):
        return place(w_mine, c, (2 + 2 * z + c // 2) * piece, piece)

    def up(z, c):
        return remote_copy(share(c, z), from_below(c, chip), send_x.at[0], recv_u.at[chip, c], 2 * z + core)

    def down(z, c):
        return remote_copy(share(c, z), from_above(c, z), send_x.at[0], recv_d2.at[z, c], me - 2)

    def table_grad():
        arrived(0)
        dr = jnp.concatenate([flip_lanes(dr_buf[h], eye) for h in range(heads)], 0)
        for c in chunks:
            acc_at(c, 0, 2 * half)[...] = dot_nn(dr, table[:, c * wide:(c + 1) * wide])
        for c in chunks:
            swap(c).start()
        for c in chunks:
            swap(c).wait()
            place(w_half, c, c // 2 * half, half)[...] = (
                acc_at(c, aligned(core * half, half), half)[...] + place(w_in, c, c // 2 * half, half)[...])
        for c in chunks:
            for z in range(heads - 1, 0, -1):
                pl.when(z > chip)(up(z, c).start)

    bodies, done = [], 0
    for step in range(n):
        tiles_done = sum(nslot - i for i in range((3 * step + 4) // 2))
        bodies.append(-(-tiles_done // UNROLL_GRAD) - done)
        done += bodies[-1]
    phases = [c for b in bodies[:-1] for c in (min(b, 1), max(b - 1, 0))]

    def next_tile(k, t):
        last = jnp.where(lower, t == k, k == nslot - 1)
        k1 = jnp.where(lower, k - 1, t + 1)
        return (jnp.where(last, k1, jnp.where(lower, k, k + 1)), jnp.where(last, jnp.where(lower, 0, t + 1), jnp.where(lower, t + 1, t)))

    def phase(x, kt):
        count = jnp.int32(0)
        for at, c in enumerate(phases):
            count = jnp.where(x == at, c, count)

        def some(i, kt):
            at = []
            for u in range(UNROLL_GRAD):
                at.append(kt)
                kt = next_tile(*kt)
            grads(at)
            return kt

        kt = lax.fori_loop(0, count, some, kt)
        pl.when(lax.rem(x, 2) == 1)(lambda: exchange(x // 2))
        pl.when((lax.rem(x, 2) == 0) & (x > 0))(lambda: release(x // 2 - 1))
        return kt

    lax.fori_loop(0, len(phases), phase, (jnp.where(lower, nslot - 1, 0), jnp.int32(0)))
    exchange(n - 1)
    release(n - 2)
    release(n - 1)
    rows_sum = jnp.sum(jnp.sum(acc[...].reshape(nslot * BQ // 8, 8, 2 * dim), axis=0), axis=0, keepdims=True)
    for t in range(2):
        bias_buf[me, t] = rows_sum[:, t * dim:(t + 1) * dim] + jnp.zeros((8, dim), F32)

    def bias(o):
        return remote_copy(bias_buf.at[me], bias_buf.at[me], send_b.at[0], recv_b2.at[0], lax.rem(me + o, n))

    for o in range(1, n):
        bias(o).start()
    for t in range(3):
        if t:
            to_mate(t).wait_send()
        for i in range(1, heads):
            h = lax.rem(chip + i, heads)
            forward(t, h).wait_send()
            if t:
                direct(t, h).wait_send()
    for t in (0, 1):
        for h in range(heads):
            for j in range(per_blk):
                to = 2 * h + owner_core(me * per_blk + j)

                @pl.when(to != me)
                def _():
                    remote_copy((q_in, do_in)[t].at[0, :, pl.ds(0, BQ)], (qT, doT)[t].at[:, pl.ds(0, BQ)],
                                send_q.at[t, h, j], recv_q.at[t, 0], to).wait_send()
    rows_done(0)
    table_grad()

    def up_landed(z, c):
        remote_copy(share(c, 0), from_below(c, z), send_x.at[0], recv_u.at[z, c], me).wait_recv()

    def take_above(z, c):
        @pl.when(chip < groups - 1)
        def _():
            remote_copy(share(c, z), from_above(c, z), send_x.at[0], recv_d2.at[z, c], me).wait_recv()
            share(c, z)[...] += from_above(c, z)[...]

        pl.when(z < chip)(down(z, c).start)

    def home(co, z, c):
        return dw_out.at[pl.ds(aligned(co * half + z * piece, piece), piece), pl.ds(c * wide, wide)]

    def my_piece(c):
        return place(w_mine, c, c // 2 * piece, piece)

    end = jnp.where(lower, heads - 1, 0)

    def collect(z, c):
        return remote_copy(my_piece(c), home(core, chip, c), send_x.at[0], recv_c.at[chip, c], 2 * z + core)

    def relay(z, c):
        return remote_copy(home(core, z, c), home(core, z, c), send_x.at[0], recv_c.at[z, c], jnp.where(lower, core, n - 2 + core))

    def relays(z):
        return ((chip == 1) & (z > 1)) | ((chip == groups - 2) & (z < groups - 2))

    def hand_over(z):
        whole = dw_out.at[pl.ds(aligned(core * half + z * piece, piece), piece)]
        return remote_copy(whole, whole, send_x.at[0], recv_h.at[0], mate)

    def hand_over_mine(c):
        return remote_copy(my_piece(c), home(core, chip, c), send_x.at[0], recv_h.at[0], mate)

    def stay(c):
        return pltpu.make_async_copy(my_piece(c), home(core, chip, c), loc_w.at[0])

    for c in chunks:
        for z in range(heads - 1):
            pl.when(z <= chip)(functools.partial(take_above, z, c))
    for c in chunks:
        for z in range(heads - 1):
            @pl.when(z < chip)
            def _():
                up_landed(z, c)
                share(c, chip)[...] += from_below(c, z)[...]

        my_piece(c)[...] = share(c, chip)[...]
        for z in range(heads):
            pl.when((z != chip) & (z != end))(collect(z, c).start)
        hand_over_mine(c).start()
        stay(c).start()
    for c in chunks:
        for at in range(heads):
            z = jnp.where(lower, at, heads - 1 - at)

            @pl.when(z != chip)
            def _():
                remote_copy(my_piece(c), home(core, z, c), send_x.at[0], recv_c.at[z, c], me).wait_recv()
                pl.when(relays(z))(relay(z, c).start)
                if c == chunks[-1]:
                    hand_over(z).start()

    others = bias_buf.at[pl.ds(0, n - 1)]
    remote_copy(others, others, send_b.at[0], recv_b2.at[0], mate).wait_recv()
    for t in range(2):
        bias_out[t] = jnp.concatenate([bias_buf[2 * h, t, :1] + bias_buf[2 * h + 1, t, :1] for h in range(heads)], 0)

    my_rows = dw_out.at[pl.ds(aligned(core * half + chip * piece, piece), piece)]
    pltpu.make_async_copy(my_rows, my_rows, loc_w.at[0]).wait()
    remote_copy(others, others, send_b.at[0], recv_b2.at[0], mate).wait_send()
    for t in range(3):
        departed(t)
        if t:
            arrived(t)
    rows_done(1)
    for count, here in ((9, (chip == 0) | (chip == groups - 1)), (11, (chip > 0) & (chip < groups - 1))):
        sent = s_all.at[pl.ds(0, count), pl.ds(0, 2 * piece)]
        pl.when(here)(remote_copy(sent, sent, send_x.at[0], recv_h.at[0], mate).wait_send)
    theirs = dw_out.at[pl.ds(aligned((1 - core) * half, half), half)]
    remote_copy(theirs, theirs, send_x.at[0], recv_h.at[0], mate).wait_recv()


def solution(mesh):
    n = mesh.shape['cp']
    seq_spec, head_spec, weight_spec = P('cp', 'hp', None), P('hp', None), P(None, 'hp', None)
    vmem = pl.BlockSpec(memory_space=pltpu.VMEM)
    hbm = pl.BlockSpec(memory_space=pl.ANY)
    dma, sds, buf = pltpu.SemaphoreType.DMA, jax.ShapeDtypeStruct, pltpu.VMEM

    def local_fn(q, k, v, u_bias, v_bias, rel_table, w_rel, d_out):
        blk, heads, dim = q.shape
        seq = n * blk
        rows = seq // 2
        nslot = rows // BQ
        per_blk = blk // BQ
        tiles = nslot * (nslot + 1) // 2
        qT, kT, vT, doT = (x.transpose(1, 2, 0) for x in (q, k, v, d_out))
        wT = w_rel.transpose(1, 2, 0).reshape(heads * dim, -1)
        model = wT.shape[1]
        o, dq, dk, dvv, dw, bias = pl.pallas_call(
            functools.partial(attention_kernel, n),
            out_shape=[sds((heads, dim, blk), BF16)] * 4 + [sds((heads * dim, model), F32), sds((2, heads, dim), F32)],
            in_specs=[hbm] * 6 + [vmem] * 2, out_specs=[hbm] * 5 + [vmem],
            scratch_shapes=[
                buf((dim, rows), BF16), buf((dim, rows), BF16), buf((dim, seq), BF16), buf((dim, seq), BF16), buf((KX, seq + PAD), BF16),
                buf((dim, rows), BF16), buf((dim, rows), BF16), buf((dim, seq), F32), buf((dim, seq), F32), buf((dim, seq + PAD), F32),
                buf((tiles, BQ, BK), F32), buf((nslot, BQ, LANES), BF16), buf((nslot, BQ, LANES), BF16), buf((nslot, BQ, dim), BF16),
                buf((nslot, dim, BQ), BF16), buf((nslot, dim, BQ), BF16), buf((nslot, dim, BQ), BF16),
                buf((nslot, BQ, LANES), F32), buf((nslot, BQ, LANES), F32), buf((nslot, BQ, 2 * dim), F32),
                buf((GROUP + 1, BQ, 256), F32),
                buf((3, 4, dim, blk // 2), F32), buf((n, dim, blk // 2), BF16), buf((2, n, dim, blk // 2), BF16), buf((heads, dim, blk), BF16), buf((blk, model), BF16),
                buf((n, 2, 8, dim), F32),
                dma((3, heads)), dma((3, heads)), dma((2, heads, per_blk)), dma((3, n)), dma((2, nslot)), dma((3,)), dma((2, per_blk)),
                dma((2,)), dma((2,)), dma((3, 4)), dma((3, 4)), dma((3,)), dma((3,)),
                dma((1 + model // LANES,)), dma((4,)), dma((4,)), dma((1,)), dma((1,)), dma((1,)),
                *[dma((heads, 4))] * 3, dma((1,)), dma((1,))],
            compiler_params=pltpu.CompilerParams(collective_id=0, has_side_effects=True, vmem_limit_bytes=67043328),
            name='attention',
        )(qT, kT, vT, doT, rel_table, wT, u_bias, v_bias)
        steps = 2
        part = pl.BlockSpec((heads // steps, dim, blk), lambda i: (i, 0, 0))
        wide = pl.BlockSpec((heads * dim // steps, model), lambda i: (i, 0))
        whole = lambda *shape: pl.BlockSpec(shape, lambda i: (0,) * len(shape))
        o, dq, dk, dvv, dw, du, dv = pl.pallas_call(
            hand_off_kernel, grid=(steps,),
            out_shape=[sds((heads, dim, blk), BF16)] * 4 + [sds((heads * dim, model), F32)] + [sds((heads, dim), F32)] * 2,
            in_specs=[part] * 4 + [wide, whole(2, heads, dim)],
            out_specs=[part] * 4 + [wide, whole(heads, dim), whole(heads, dim)],
            name='hand_off',
        )(o, dq, dk, dvv, dw, bias)
        back = lambda x: x.transpose(2, 0, 1)
        return back(o), back(dq), back(dk), back(dvv), du, dv, back(dw.reshape(heads, dim, model))

    return jax.shard_map(
        local_fn, mesh=mesh,
        in_specs=(seq_spec, seq_spec, seq_spec, head_spec, head_spec, P('cp', None), weight_spec, seq_spec),
        out_specs=(seq_spec, seq_spec, seq_spec, seq_spec, head_spec, head_spec, weight_spec),
        check_vma=False,
    )
```

```python
import functools
import math
import jax
import jax.numpy as jnp
from jax import lax
from jax.experimental import pallas as pl
from jax.experimental.pallas import tpu as pltpu
from jax.sharding import PartitionSpec as P

F32, BF16 = jnp.float32, jnp.bfloat16
LOG2E = math.log2(math.e)
BQ = 256
BK = 512
LANES = 128
NC = BK // LANES
PAD = 512
KX = 80
GROUP = 3
UNROLL_SUM = 26
UNROLL_GRAD = 6
VALUES_AT = 5
MESH_ID = pl.DeviceIdType.MESH


def dot_nn(a, b):
    return lax.dot_general(a, b, (((1,), (0,)), ((), ())), preferred_element_type=F32)


def dot_nt(a, b):
    return lax.dot_general(a, b, (((1,), (1,)), ((), ())), preferred_element_type=F32)


def lanes(m, count=1):
    return slice(m * LANES, (m + count) * LANES)


def aligned(x, m):
    return pl.multiple_of(x, m)


def anti_eye(n):
    rows = lax.broadcasted_iota(jnp.int32, (n, n), 0)
    cols = lax.broadcasted_iota(jnp.int32, (n, n), 1)
    return (rows + cols == n - 1).astype(F32).astype(BF16)


def flip_lanes(x, eye):
    n, w = x.shape[1], eye.shape[0]
    parts = [dot_nn(x[:, s:s + w], eye).astype(BF16) for s in range(0, n, w)]
    return jnp.concatenate(parts[::-1], axis=1)


def reverse_rows(x):
    ix = 7 - lax.broadcasted_iota(jnp.int32, (8, x.shape[1]), 0)
    n = x.shape[0] // 8
    return jnp.concatenate([jnp.take_along_axis(x[(n - 1 - g) * 8:(n - g) * 8], ix, axis=0) for g in range(n)], 0)


def owner_core(rb):
    return lax.rem(rb + rb // 2, 2)


def remote_copy(src, dst, send_sem, recv_sem, to):
    return pltpu.make_async_remote_copy(src, dst, send_sem, recv_sem, device_id=(lax.axis_index('hp'), to),
                                        device_id_type=MESH_ID)


def greet_all(n):
    me, hp = lax.axis_index('cp'), lax.axis_index('hp')
    bar = pltpu.get_barrier_semaphore()
    for o in range(1, n):
        pl.semaphore_signal(bar, 1, device_id=(hp, lax.rem(me + o, n)), device_id_type=MESH_ID)


def await_all(n):
    pl.semaphore_wait(pltpu.get_barrier_semaphore(), n - 1)


def hand_off_kernel(o, dq, dk, dv, dw, bias, o_out, dq_out, dk_out, dv_out, dw_out, u_out, v_out):
    for src, dst in ((o, o_out), (dq, dq_out), (dk, dk_out), (dv, dv_out), (dw, dw_out)):
        dst[...] = src[...]
    u_out[...], v_out[...] = bias[0], bias[1]


def attention_kernel(n, q_in, k_in, v_in, do_in, table_in, w_rel, ub, vb,
                     o_out, dq_out, dk_out, dv_out, dw_out, bias_out,
                     qT, doT, kT, vT, relX, oT, dqT, dkT, dvT, drF,
                     s_all, q_off, q_row, do_row, q_col, qo_col, do_col, mx, total, acc, r_scr,
                     pair_buf, dr_send, send_buf, dr_buf, table, bias_buf,
                     send_d, send_f, send_q, recv_b, recv_q, loc_b, loc_q,
                     send_o, recv_o, send_p, recv_p, send_s, recv_s,
                     loc_t, send_w, recv_w, loc_w, send_b, recv_b2,
                     recv_u, recv_d2, recv_c, recv_h, send_x):
    me = lax.axis_index('cp')
    chip, core = me // 2, lax.rem(me, 2)
    mate = 2 * chip + 1 - core
    heads, dim, blk = q_in.shape
    seq = n * blk
    per_blk = blk // BQ
    groups = n // 2
    nslot = qT.shape[1] // BQ
    tiles = s_all.shape[0]
    scale = dim ** -0.5
    model = table.shape[1]

    def weight_block(m):
        return pltpu.make_async_copy(w_rel.at[:, pl.ds(m * LANES, LANES)], q_off.at[m], loc_t.at[1 + m])

    greet_all(n)
    pltpu.make_async_copy(table_in, table, loc_t.at[0]).start()
    for m in range(model // LANES):
        weight_block(m).start()

    rel_buf = dr_buf
    srcs, fulls = (rel_buf, k_in, v_in), (relX, kT, vT)

    def col(t, b, flipped):
        b = (n - 1 - b) if t == flipped else b
        return pl.ds(aligned(b * blk, blk), blk)

    def full_at(t, b):
        return fulls[t].at[pl.ds(0, dim), col(t, b, 0)]

    def direct(t, h):
        return remote_copy(srcs[t].at[h], full_at(t, me), send_d.at[t, h], recv_b.at[t, me], 2 * h + core)

    def own(t):
        return pltpu.make_async_copy(srcs[t].at[chip], full_at(t, me), loc_b.at[t])

    def to_mate(t):
        return remote_copy(srcs[t].at[chip], full_at(t, me), send_f.at[t, chip], recv_b.at[t, me], mate)

    def forward(t, g):
        b = 2 * g + core
        return remote_copy(full_at(t, b), full_at(t, b), send_f.at[t, g], recv_b.at[t, b], mate)

    def landed(t, b):
        remote_copy(srcs[t].at[0], full_at(t, b), send_f.at[t, 0], recv_b.at[t, b], me).wait_recv()

    def pass_on(t, g):
        @pl.when(g != chip)
        def _():
            landed(t, 2 * g + core)
            forward(t, g).start()

        pl.when(g == chip)(own(t).wait)

    def from_mate(t, g):
        landed(t, 2 * g + 1 - core)

    def row_copy(t, h, j, wait):
        rb = me * per_blk + j
        src = (q_in, do_in)[t].at[h, :, pl.ds(j * BQ, BQ)]
        dst = (qT, doT)[t].at[:, pl.ds(aligned(rb // 2 * BQ, BQ), BQ)]
        to = 2 * h + owner_core(rb)

        @pl.when(to != me)
        def _():
            c = remote_copy(src, dst, send_q.at[t, h, j], recv_q.at[t, rb // 2], to)
            c.wait_send() if wait else c.start()

        @pl.when(to == me)
        def _():
            c = pltpu.make_async_copy(src, dst, loc_q.at[t, j])
            c.wait() if wait else c.start()

    def row_block(k):
        return 2 * k + lax.rem(k + core, 2)

    def row_landed(t, k):
        src = (q_in, do_in)[t].at[0, :, pl.ds(0, BQ)]
        dst = (qT, doT)[t].at[:, pl.ds(aligned(k * BQ, BQ), BQ)]
        rb = row_block(k)

        @pl.when(rb // per_blk != me)
        def _():
            remote_copy(src, dst, send_q.at[t, 0, 0], recv_q.at[t, k], me).wait_recv()

        @pl.when(rb // per_blk == me)
        def _():
            pltpu.make_async_copy(src, dst, loc_q.at[t, lax.rem(rb, per_blk)]).wait()

    lower = chip < groups // 2
    side = chip + 1 - 2 * lax.rem(chip, 2)
    near, far = jnp.where(lower, groups // 2, groups // 2 - 1), jnp.where(lower, groups - 1, 0)
    across = near, far

    def send_rows(t, h):
        for j in range(per_blk):
            row_copy(t, h, j, False)

    def send_scores_input(h):
        direct(1, h).start()
        send_rows(0, h)

    eye = anti_eye(BQ)
    pltpu.make_async_copy(table_in, table, loc_t.at[0]).wait()
    for m in range(model // LANES):
        weight_block(m).wait()
    weights_in = jnp.concatenate([q_off[m] for m in range(model // LANES)], 1)
    rel = flip_lanes(dot_nt(weights_in, table[...]).astype(BF16), eye)
    for h in range(heads):
        rel_buf[h] = rel[h * dim:(h + 1) * dim]
    await_all(n)
    to_mate(1).start()
    own(1).start()
    send_scores_input(side)
    send_rows(0, chip)
    to_mate(0).start()
    own(0).start()
    for h in (side, *across):
        direct(0, h).start()
    for h in across:
        send_scores_input(h)

    def send_values():
        to_mate(2).start()
        own(2).start()
        for h in (side, *across):
            direct(2, h).start()

    def send_cotangent():
        for h in (side, *across):
            direct(0, h).wait_send()
        to_mate(0).wait_send()
        for h in (side, *across, chip):
            send_rows(1, h)

    for ref in (dkT, dvT, drF, total, acc):
        ref[...] = jnp.zeros_like(ref)
    mx[...] = jnp.full(mx.shape, -jnp.inf, F32)
    relX[pl.ds(0, dim), pl.ds(seq, PAD)] = jnp.zeros((dim, PAD), BF16)
    first = lax.broadcasted_iota(jnp.int32, (KX - dim, PAD), 0) == 0
    relX[pl.ds(dim, KX - dim), pl.ds(0, seq)] = jnp.zeros((KX - dim, seq), BF16)
    relX[pl.ds(dim, KX - dim), pl.ds(seq, PAD)] = jnp.where(first, -jnp.inf, 0.0).astype(BF16)
    ones_col = (lax.broadcasted_iota(jnp.int32, (BQ, KX - dim), 1) == 0).astype(F32).astype(BF16)
    lane = lax.broadcasted_iota(jnp.int32, (128, LANES), 1)
    row = lax.broadcasted_iota(jnp.int32, (128, LANES), 0)
    past, before = lane > row, lane < row

    def bias_col(ref):
        pick = lax.broadcasted_iota(jnp.int32, ref.shape, 0) == chip
        r = jnp.sum(jnp.where(pick, ref[...], 0.0), axis=0, keepdims=True)
        return jnp.broadcast_to(r, (LANES, dim)).T[:, :1]

    u_col, v_col = bias_col(ub), bias_col(vb)

    def skew(t):
        return pltpu.roll(t, 1, 1, stride=1, stride_axis=0)

    def slot_cols(k):
        return pl.ds(aligned(k * BQ, BQ), BQ)

    def transposed(x):
        return x.astype(F32).T.astype(BF16)

    def prepare(k):
        q = qT[:, slot_cols(k)].astype(F32)
        quT, qvT = (q + u_col).astype(BF16), (q + v_col).astype(BF16)
        q_off[k, :, :KX] = jnp.concatenate([transposed(qvT), ones_col], 1)
        q_col[k] = flip_lanes(quT, eye)
        q_row[k, :, :dim] = transposed(q_col[k])
        qo_col[k] = flip_lanes(qvT, eye)

    def prepare_skew(k, i, t):
        start = seq - row_block(k) * BQ + t * BK - 256
        t0 = dot_nn(q_off[k, :, :KX], relX[:, pl.ds(aligned(start, LANES), 256)])
        for m in range(2):
            r_scr[i, :, lanes(m)] = skew(t0[:, lanes(m)])

    def score_products(k, t):
        j0 = aligned(t * BK, BK)
        base = seq - row_block(k) * BQ
        by_offset = dot_nn(q_off[k, :, :KX], relX[:, pl.ds(aligned(base + j0, LANES), BK)])
        return by_offset, dot_nn(q_row[k, :, :dim], kT[:, pl.ds(j0, BK)])

    def scores(k, t, by_offset, content):
        ri = jnp.where(lax.rem(t, GROUP) == 0, lax.rem(k, GROUP), GROUP)
        rolled = [r_scr[ri, :, lanes(m)] for m in range(2)]
        rolled += [skew(by_offset[:, lanes(m)]) for m in range(NC)]
        top_s = mx[k]
        for m in range(NC):
            top = jnp.where(past, rolled[m + 2][:LANES], rolled[m + 1][:LANES])
            bot = jnp.where(past, rolled[m + 1][LANES:], rolled[m][LANES:])
            s = content[:, lanes(m)] + reverse_rows(jnp.concatenate([top, bot], 0))
            s = s * (scale * LOG2E)
            s_all[tile_of(k, t), :, lanes(m)] = s
            top_s = jnp.maximum(top_s, s)
        mx[k] = top_s
        for m in range(2):
            r_scr[GROUP, :, lanes(m)] = rolled[NC + m]

    def weights(k, t):
        tile, top_s, tot = tile_of(k, t), mx[k], total[k]
        parts = []
        for m in range(NC):
            p = jnp.exp2(s_all[tile, :, lanes(m)] - top_s)
            s_all[tile, :, lanes(m)] = p
            tot = tot + p
            parts.append(p.astype(BF16))
        total[k] = tot
        return jnp.concatenate(parts, 1)

    def add_values(k, t, p_all):
        acc[k, :, :dim] += dot_nt(p_all, vT[:, pl.ds(aligned(t * BK, BK), BK)])

    def finish_rows(k):
        do_col[k] = flip_lanes(doT[:, slot_cols(k)], eye)
        do_row[k] = transposed(do_col[k])
        inv = 1.0 / jnp.sum(total[k], axis=1, keepdims=True)
        out = acc[k, :, :dim] * inv
        delta = jnp.sum(do_row[k].astype(F32) * out, axis=1, keepdims=True)
        total[k] = jnp.broadcast_to(inv, (BQ, LANES))
        mx[k] = jnp.broadcast_to(delta, (BQ, LANES))
        oT[:, slot_cols(k)] = flip_lanes(out.T.astype(BF16), eye)
        acc[k] = jnp.zeros((BQ, 2 * dim), F32)

    def score_grads(k, t):
        return dot_nn(do_row[k], vT[:, pl.ds(aligned(t * BK, BK), BK)])

    def split_grads(tile, k, t, dp):
        inv, delta = total[k], mx[k]
        carry = (q_off, q_row)
        ps, dss = [], []
        held = [jnp.where(t > 0, c[k], jnp.zeros((BQ, LANES), BF16)) for c in carry]
        for m in range(NC):
            p = s_all[tile, :, lanes(m)] * inv
            ds = (p * ((dp[:, lanes(m)] - delta) * scale)).astype(BF16)
            ps.append(p.astype(BF16))
            dss.append(ds)
            held.append(pltpu.roll(ds, 0, 1, stride=1, stride_axis=0))
        for m in range(2):
            carry[m][k] = held[NC + m]
        by_offset = []
        for m in range(NC):
            top = jnp.where(before, held[m + 1][:LANES], held[m + 2][:LANES])
            bot = jnp.where(before, held[m][LANES:], held[m + 1][LANES:])
            by_offset.append(jnp.concatenate([top, bot], 0))
        return tuple(jnp.concatenate(x, 1) for x in (ps, dss, by_offset))

    def add_grads(k, t, p_all, ds_all, by_offset):
        j0 = aligned(t * BK, BK)
        base = seq - row_block(k) * BQ
        js, us = pl.ds(j0, BK), pl.ds(aligned(base + j0 - 256, LANES), BK)
        dvT[:, js] += dot_nn(do_col[k], p_all)
        dkT[:, js] += dot_nn(q_col[k], ds_all)
        drF[:, us] += dot_nn(qo_col[k], by_offset)
        none = jnp.zeros((dim, BK), BF16)
        keys = jnp.concatenate([jnp.concatenate([kT[:, js], none], 0), jnp.concatenate([none, relX[:dim, us]], 0)], 1)
        acc[k] += dot_nt(jnp.concatenate([ds_all, by_offset], 1), keys)

    def walk(steps, count, k, t_low, t_cap, unroll):
        def some(i, kt):
            k, t = kt
            at = []
            for u in range(unroll):
                at.append((k, t))
                last = t == jnp.minimum(k, t_cap)
                k, t = jnp.where(last, k + 1, k), jnp.where(last, t_low, t + 1)
            steps(at)
            return k, t

        lax.fori_loop(0, count // unroll, some, (k, t_low))

    def tile_of(k, t):
        return k * (k + 1) // 2 + t

    def grads(at):
        count = len(at)
        dps = [score_grads(*at[0])]
        for u, here in enumerate(at):
            if u + 1 < count:
                dps.append(score_grads(*at[u + 1]))
            add_grads(*here, *split_grads(tile_of(*here), *here, dps[u]))

    def group_tiles(g):
        return GROUP * GROUP * g + GROUP * (GROUP + 1) // 2

    def score_tiles(at):
        products = score_products(*at[0])
        for u, here in enumerate(at):
            ahead = score_products(*at[u + 1]) if u + 1 < len(at) else None
            scores(*here, *products)
            products = ahead

    def weigh_tiles(at):
        p_all = weights(*at[0])
        for u, here in enumerate(at):
            ahead = weights(*at[u + 1]) if u + 1 < len(at) else None
            add_values(*here, p_all)
            p_all = ahead

    def each(fn):
        lax.fori_loop(0, groups, lambda g, c: (fn(g), c)[1], 0)

    orders = ('00111030313320212232', '11001030313320212232', '22333200203011102131', '33223200203011102131')
    orders = [[(int(word[at]), int(word[at + 1])) for at in range(0, len(word), 2)] for word in orders]

    def schedule(order):
        seen = ([], [], [])
        rows = []
        for gq, gk in order:
            row = [gq, gk]
            for t, g in ((0, gq - gk), (0, gq - gk - 1), (1, gk), (2, gq)):
                new = g >= 0 and g not in seen[t]
                row.append(g if new else -1)
                if new:
                    seen[t].append(g)
            rows.append(row)
        return rows

    schedules = [schedule(order) for order in orders]

    def look_up(x, column):
        value = jnp.int32(-1)
        for at in range(len(orders[0])):
            here = jnp.int32(schedules[-1][at][column])
            for z in range(groups - 1):
                here = jnp.where(chip == z, schedules[z][at][column], here)
            value = jnp.where(x == at, here, value)
        return value

    def forward_scores(x):
        gq, gk, *need, new_q = (look_up(x, column) for column in range(6))
        *ahead, ahead_q = (look_up(x + 1, column) for column in range(2, 6))

        def arrives_now(g, q):
            return (q >= 0) & ((g < groups // 2) != lower) & (chip == 0)

        for t, g in zip((0, 0, 1), need):
            pl.when((g >= 0) & ((x == 0) | arrives_now(g, new_q)))(functools.partial(pass_on, t, g))
        for t, g, g1 in zip((0, 0, 1), need, ahead):
            pl.when((g1 >= 0) & ~arrives_now(g1, ahead_q))(functools.partial(pass_on, t, g1))
            pl.when(g >= 0)(functools.partial(from_mate, t, g))

        @pl.when(new_q >= 0)
        def _():
            for i in range(GROUP):
                row_landed(0, GROUP * new_q + i)
            for i in range(GROUP):
                prepare(GROUP * new_q + i)

        pl.when(x == VALUES_AT)(send_values)
        for i in range(GROUP):
            prepare_skew(GROUP * gq + i, i, GROUP * gk)
        here = GROUP * gq, GROUP * gk, GROUP * gk + GROUP - 1
        pl.when(gq == gk)(lambda: walk(score_tiles, GROUP * (GROUP + 1) // 2, *here, GROUP * (GROUP + 1) // 2))
        pl.when(gq != gk)(lambda: walk(score_tiles, GROUP * GROUP, *here, GROUP * GROUP))

    lax.fori_loop(0, len(orders[0]), lambda x, c: (forward_scores(x), c)[1], 0)
    send_cotangent()
    each(lambda g: pass_on(2, g))

    def row_max(g):
        for i in range(GROUP):
            k = GROUP * g + i
            mx[k] = jnp.broadcast_to(jnp.max(mx[k], axis=1, keepdims=True), (BQ, LANES))

    each(row_max)

    each(lambda g: from_mate(2, g))
    walk(weigh_tiles, tiles, 0, 0, nslot, UNROLL_SUM)

    def out_rows(t, k):
        rb = row_block(k)
        to, j = rb // per_blk, lax.rem(rb, per_blk)
        src = (oT, dqT)[t].at[:, slot_cols(k)]
        dst = (o_out, dq_out)[t].at[chip, :, pl.ds(aligned(j * BQ, BQ), BQ)]
        pl.when(to != me)(lambda: remote_copy(src, dst, send_o.at[t], recv_o.at[t], to).start())
        pl.when(to == me)(lambda: pltpu.make_async_copy(src, dst, recv_o.at[t]).start())

    def rows_done(t):
        src, dst = (oT, dqT)[t], (o_out, dq_out)[t]
        remote_copy(dst, dst, send_o.at[t], recv_o.at[t], mate).wait_recv()
        kept = sum((owner_core(me * per_blk + j) == core).astype(jnp.int32) for j in range(per_blk))
        for count in (1, 2):
            left = src.at[:, pl.ds(0, (nslot - count) * BQ)]
            pl.when(kept == count)(remote_copy(left, left, send_o.at[t], recv_o.at[t], mate).wait_send)

    def finish_group(g):
        for i in range(GROUP):
            row_landed(1, GROUP * g + i)
        for i in range(GROUP):
            finish_rows(GROUP * g + i)
        for i in range(GROUP):
            out_rows(0, GROUP * g + i)

    each(finish_group)

    parts, sinks = (drF, dkT, dvT), (dr_buf, dk_out, dv_out)

    hw = blk // 2
    slots = pair_buf.shape[1]

    def out_block(t, step):
        return n - 1 - step if t == 0 else jnp.where(lower, n - 1 - step, step)

    def half_of(t, step, c):
        b = out_block(t, step)
        b = n - 1 - b if t == 0 else b
        return pl.ds(aligned(b * blk + c * hw, LANES), hw)

    def pair(t, step):
        s = lax.rem(step, slots)
        return remote_copy(parts[t].at[:, half_of(t, step, 1 - core)], pair_buf.at[t, s], send_p.at[t, s], recv_p.at[t, s], mate)

    def ready(t, step):
        return dr_send.at[step] if t == 0 else send_buf.at[t - 1, step]

    def sink_at(t, h, c):
        return sinks[t].at[h, :, pl.ds(aligned(c * hw, LANES), hw)]

    def sink(t, step):
        return remote_copy(ready(t, step), sink_at(t, chip, core), send_s.at[t], recv_s.at[t], out_block(t, step))

    def keep(t, step):
        return pltpu.make_async_copy(ready(t, step), sink_at(t, chip, core), recv_s.at[t])

    def combine(t, step):
        s = lax.rem(step, slots)
        mine = half_of(t, step, core)
        remote_copy(parts[t].at[:, mine], pair_buf.at[t, s], send_p.at[t, s], recv_p.at[t, s], mate).wait_recv()
        ready(t, step)[...] = (parts[t][:, mine] + pair_buf[t, s]).astype(BF16)
        pair(t, step).wait_send()

    def to_owner(t, step):
        b = out_block(t, step)
        pl.when(b != me)(lambda: sink(t, step).start())
        pl.when(b == me)(lambda: keep(t, step).start())

    def arrived(t):
        remote_copy(sinks[t], sinks[t], send_s.at[t], recv_s.at[t], mate).wait_recv()

    def departed(t):
        others = (dr_send if t == 0 else send_buf.at[t - 1]).at[pl.ds(0, n - 1)]
        remote_copy(others, others, send_s.at[t], recv_s.at[t], mate).wait_send()

    def final_slots(step, fn):
        first, end = (3 * step + 1) // 2, (3 * step + 4) // 2
        for i in range(2):
            at = first + i
            pl.when(at < end)(functools.partial(fn, jnp.where(lower, nslot - 1 - at, at)))

    def row_grads(k):
        dqT[:, slot_cols(k)] = flip_lanes((acc[k, :, :dim] + acc[k, :, dim:]).T.astype(BF16), eye)

    def exchange(step):
        for t in range(3):
            pair(t, step).start()
        final_slots(step, row_grads)

    def bulk(step):
        for t in (1, 2):
            to_owner(t, step)
        final_slots(step, lambda k: out_rows(1, k))

    def held(step):
        return ((chip == 3) & ((step == 3) | (step == 4) | (step == 5)))

    def release_offsets(step):
        combine(0, step)
        to_owner(0, step)

    def release_rest(step):
        for t in (1, 2):
            combine(t, step)
        pl.when(~held(step))(lambda: bulk(step))

    def release(step):
        release_offsets(step)
        release_rest(step)

    w_acc, w_in, w_half, w_part, w_mine = (9, 0), (10, 0), (10, 1), (11, 0), (11, 1)
    chunks, wide = range(4), BK // 2
    half = heads * dim // 2
    piece = half // heads

    def place(kt, c, row0, count):
        at = kt[0] * (kt[0] + 1) // 2 + kt[1]
        return s_all.at[at, pl.ds(row0, count), pl.ds(c % 2 * wide, wide)]

    def acc_at(c, row0, count):
        return place((w_acc[0], w_acc[1] + c // 2), c, row0, count)

    def swap(c):
        return remote_copy(acc_at(c, aligned((1 - core) * half, half), half), place(w_in, c, c // 2 * half, half),
                           send_w.at[c], recv_w.at[c], mate)

    def share(c, z):
        return place(w_half, c, aligned(c // 2 * half + z * piece, piece), piece)

    def from_below(c, z):
        return place(w_part, c, aligned((2 * z + c // 2) * piece, piece), piece)

    def from_above(c, z):
        return place(w_mine, c, (2 + 2 * z + c // 2) * piece, piece)

    def up(z, c):
        return remote_copy(share(c, z), from_below(c, chip), send_x.at[0], recv_u.at[chip, c], 2 * z + core)

    def down(z, c):
        return remote_copy(share(c, z), from_above(c, z), send_x.at[0], recv_d2.at[z, c], me - 2)

    def table_grad():
        arrived(0)
        dr = jnp.concatenate([flip_lanes(dr_buf[h], eye) for h in range(heads)], 0)
        for c in chunks:
            acc_at(c, 0, 2 * half)[...] = dot_nn(dr, table[:, c * wide:(c + 1) * wide])
        for c in chunks:
            swap(c).start()
        for c in chunks:
            swap(c).wait()
            place(w_half, c, c // 2 * half, half)[...] = (
                acc_at(c, aligned(core * half, half), half)[...] + place(w_in, c, c // 2 * half, half)[...])
        for c in chunks:
            for z in range(heads - 1, 0, -1):
                pl.when(z > chip)(up(z, c).start)

    bodies, done = [], 0
    for step in range(n):
        tiles_done = sum(nslot - i for i in range((3 * step + 4) // 2))
        bodies.append(-(-tiles_done // UNROLL_GRAD) - done)
        done += bodies[-1]
    phases = [c for b in bodies[:-1] for c in (min(b, 1), max(b - 1, 0))]

    def next_tile(k, t):
        last = jnp.where(lower, t == k, k == nslot - 1)
        k1 = jnp.where(lower, k - 1, t + 1)
        return (jnp.where(last, k1, jnp.where(lower, k, k + 1)), jnp.where(last, jnp.where(lower, 0, t + 1), jnp.where(lower, t + 1, t)))

    def phase(x, kt):
        count = jnp.int32(0)
        for at, c in enumerate(phases):
            count = jnp.where(x == at, c, count)

        def some(i, kt):
            at = []
            for u in range(UNROLL_GRAD):
                at.append(kt)
                kt = next_tile(*kt)
            grads(at)
            return kt

        kt = lax.fori_loop(0, count, some, kt)
        pl.when(lax.rem(x, 2) == 1)(lambda: exchange(x // 2))
        pl.when((lax.rem(x, 2) == 0) & (x > 0))(lambda: release(x // 2 - 1))
        return kt

    lax.fori_loop(0, len(phases), phase, (jnp.where(lower, nslot - 1, 0), jnp.int32(0)))
    exchange(n - 1)
    for part in (release_offsets, release_rest):
        part(n - 2)
        part(n - 1)
    rows_sum = jnp.sum(jnp.sum(acc[...].reshape(nslot * BQ // 8, 8, 2 * dim), axis=0), axis=0, keepdims=True)
    for t in range(2):
        bias_buf[me, t] = rows_sum[:, t * dim:(t + 1) * dim] + jnp.zeros((8, dim), F32)

    def bias(o):
        return remote_copy(bias_buf.at[me], bias_buf.at[me], send_b.at[0], recv_b2.at[0], lax.rem(me + o, n))

    for o in range(1, n):
        bias(o).start()
    for t in range(3):
        if t:
            to_mate(t).wait_send()
        for i in range(1, heads):
            h = lax.rem(chip + i, heads)
            forward(t, h).wait_send()
            if t:
                direct(t, h).wait_send()
    for t in (0, 1):
        for h in range(heads):
            for j in range(per_blk):
                to = 2 * h + owner_core(me * per_blk + j)

                @pl.when(to != me)
                def _():
                    remote_copy((q_in, do_in)[t].at[0, :, pl.ds(0, BQ)], (qT, doT)[t].at[:, pl.ds(0, BQ)],
                                send_q.at[t, h, j], recv_q.at[t, 0], to).wait_send()
    rows_done(0)
    table_grad()

    def up_landed(z, c):
        remote_copy(share(c, 0), from_below(c, z), send_x.at[0], recv_u.at[z, c], me).wait_recv()

    def take_above(z, c):
        @pl.when(chip < groups - 1)
        def _():
            remote_copy(share(c, z), from_above(c, z), send_x.at[0], recv_d2.at[z, c], me).wait_recv()
            share(c, z)[...] += from_above(c, z)[...]

        pl.when(z < chip)(down(z, c).start)

    def home(co, z, c):
        return dw_out.at[pl.ds(aligned(co * half + z * piece, piece), piece), pl.ds(c * wide, wide)]

    def my_piece(c):
        return place(w_mine, c, c // 2 * piece, piece)

    end = jnp.where(lower, heads - 1, 0)

    def collect(z, c):
        return remote_copy(my_piece(c), home(core, chip, c), send_x.at[0], recv_c.at[chip, c], 2 * z + core)

    def relay(z, c):
        return remote_copy(home(core, z, c), home(core, z, c), send_x.at[0], recv_c.at[z, c], jnp.where(lower, core, n - 2 + core))

    def relays(z):
        return ((chip == 1) & (z > 1)) | ((chip == groups - 2) & (z < groups - 2))

    def hand_over(z):
        whole = dw_out.at[pl.ds(aligned(core * half + z * piece, piece), piece)]
        return remote_copy(whole, whole, send_x.at[0], recv_h.at[0], mate)

    def hand_over_mine(c):
        return remote_copy(my_piece(c), home(core, chip, c), send_x.at[0], recv_h.at[0], mate)

    def stay(c):
        return pltpu.make_async_copy(my_piece(c), home(core, chip, c), loc_w.at[0])

    for c in chunks:
        for z in range(heads - 1):
            pl.when(z <= chip)(functools.partial(take_above, z, c))
    for step in (3, 4, 5):
        pl.when(held(step))(functools.partial(bulk, step))
    for c in chunks:
        for z in range(heads - 1):
            @pl.when(z < chip)
            def _():
                up_landed(z, c)
                share(c, chip)[...] += from_below(c, z)[...]

        my_piece(c)[...] = share(c, chip)[...]
        for z in range(heads):
            pl.when((z != chip) & (z != end))(collect(z, c).start)
        hand_over_mine(c).start()
        stay(c).start()
    for c in chunks:
        for at in range(heads):
            z = jnp.where(lower, at, heads - 1 - at)

            @pl.when(z != chip)
            def _():
                remote_copy(my_piece(c), home(core, z, c), send_x.at[0], recv_c.at[z, c], me).wait_recv()
                pl.when(relays(z))(relay(z, c).start)
                if c == chunks[-1]:
                    hand_over(z).start()

    others = bias_buf.at[pl.ds(0, n - 1)]
    remote_copy(others, others, send_b.at[0], recv_b2.at[0], mate).wait_recv()
    for t in range(2):
        bias_out[t] = jnp.concatenate([bias_buf[2 * h, t, :1] + bias_buf[2 * h + 1, t, :1] for h in range(heads)], 0)

    my_rows = dw_out.at[pl.ds(aligned(core * half + chip * piece, piece), piece)]
    pltpu.make_async_copy(my_rows, my_rows, loc_w.at[0]).wait()
    remote_copy(others, others, send_b.at[0], recv_b2.at[0], mate).wait_send()
    for t in range(3):
        departed(t)
        if t:
            arrived(t)
    rows_done(1)
    for count, here in ((9, (chip == 0) | (chip == groups - 1)), (11, (chip > 0) & (chip < groups - 1))):
        sent = s_all.at[pl.ds(0, count), pl.ds(0, 2 * piece)]
        pl.when(here)(remote_copy(sent, sent, send_x.at[0], recv_h.at[0], mate).wait_send)
    theirs = dw_out.at[pl.ds(aligned((1 - core) * half, half), half)]
    remote_copy(theirs, theirs, send_x.at[0], recv_h.at[0], mate).wait_recv()


def solution(mesh):
    n = mesh.shape['cp']
    seq_spec, head_spec, weight_spec = P('cp', 'hp', None), P('hp', None), P(None, 'hp', None)
    vmem = pl.BlockSpec(memory_space=pltpu.VMEM)
    hbm = pl.BlockSpec(memory_space=pl.ANY)
    dma, sds, buf = pltpu.SemaphoreType.DMA, jax.ShapeDtypeStruct, pltpu.VMEM

    def local_fn(q, k, v, u_bias, v_bias, rel_table, w_rel, d_out):
        blk, heads, dim = q.shape
        seq = n * blk
        rows = seq // 2
        nslot = rows // BQ
        per_blk = blk // BQ
        tiles = nslot * (nslot + 1) // 2
        qT, kT, vT, doT = (x.transpose(1, 2, 0) for x in (q, k, v, d_out))
        wT = w_rel.transpose(1, 2, 0).reshape(heads * dim, -1)
        model = wT.shape[1]
        o, dq, dk, dvv, dw, bias = pl.pallas_call(
            functools.partial(attention_kernel, n),
            out_shape=[sds((heads, dim, blk), BF16)] * 4 + [sds((heads * dim, model), F32), sds((2, heads, dim), F32)],
            in_specs=[hbm] * 6 + [vmem] * 2, out_specs=[hbm] * 5 + [vmem],
            scratch_shapes=[
                buf((dim, rows), BF16), buf((dim, rows), BF16), buf((dim, seq), BF16), buf((dim, seq), BF16), buf((KX, seq + PAD), BF16),
                buf((dim, rows), BF16), buf((dim, rows), BF16), buf((dim, seq), F32), buf((dim, seq), F32), buf((dim, seq + PAD), F32),
                buf((tiles, BQ, BK), F32), buf((nslot, BQ, LANES), BF16), buf((nslot, BQ, LANES), BF16), buf((nslot, BQ, dim), BF16),
                buf((nslot, dim, BQ), BF16), buf((nslot, dim, BQ), BF16), buf((nslot, dim, BQ), BF16),
                buf((nslot, BQ, LANES), F32), buf((nslot, BQ, LANES), F32), buf((nslot, BQ, 2 * dim), F32),
                buf((GROUP + 1, BQ, 256), F32),
                buf((3, 4, dim, blk // 2), F32), buf((n, dim, blk // 2), BF16), buf((2, n, dim, blk // 2), BF16), buf((heads, dim, blk), BF16), buf((blk, model), BF16),
                buf((n, 2, 8, dim), F32),
                dma((3, heads)), dma((3, heads)), dma((2, heads, per_blk)), dma((3, n)), dma((2, nslot)), dma((3,)), dma((2, per_blk)),
                dma((2,)), dma((2,)), dma((3, 4)), dma((3, 4)), dma((3,)), dma((3,)),
                dma((1 + model // LANES,)), dma((4,)), dma((4,)), dma((1,)), dma((1,)), dma((1,)),
                *[dma((heads, 4))] * 3, dma((1,)), dma((1,))],
            compiler_params=pltpu.CompilerParams(collective_id=0, has_side_effects=True, vmem_limit_bytes=67043328),
            name='attention',
        )(qT, kT, vT, doT, rel_table, wT, u_bias, v_bias)
        steps = 2
        part = pl.BlockSpec((heads // steps, dim, blk), lambda i: (i, 0, 0))
        wide = pl.BlockSpec((heads * dim // steps, model), lambda i: (i, 0))
        whole = lambda *shape: pl.BlockSpec(shape, lambda i: (0,) * len(shape))
        o, dq, dk, dvv, dw, du, dv = pl.pallas_call(
            hand_off_kernel, grid=(steps,),
            out_shape=[sds((heads, dim, blk), BF16)] * 4 + [sds((heads * dim, model), F32)] + [sds((heads, dim), F32)] * 2,
            in_specs=[part] * 4 + [wide, whole(2, heads, dim)],
            out_specs=[part] * 4 + [wide, whole(heads, dim), whole(heads, dim)],
            name='hand_off',
        )(o, dq, dk, dvv, dw, bias)
        back = lambda x: x.transpose(2, 0, 1)
        return back(o), back(dq), back(dk), back(dvv), du, dv, back(dw.reshape(heads, dim, model))

    return jax.shard_map(
        local_fn, mesh=mesh,
        in_specs=(seq_spec, seq_spec, seq_spec, head_spec, head_spec, P('cp', None), weight_spec, seq_spec),
        out_specs=(seq_spec, seq_spec, seq_spec, seq_spec, head_spec, head_spec, weight_spec),
        check_vma=False,
    )
```

```python
import functools
import math
import jax
import jax.numpy as jnp
from jax import lax
from jax.experimental import pallas as pl
from jax.experimental.pallas import tpu as pltpu
from jax.sharding import PartitionSpec as P

F32, BF16 = jnp.float32, jnp.bfloat16
LOG2E = math.log2(math.e)
BQ = 256
BK = 512
LANES = 128
NC = BK // LANES
PAD = 512
KX = 80
GROUP = 3
UNROLL_SUM = 26
UNROLL_GRAD = 6
VALUES_AT = 5
MESH_ID = pl.DeviceIdType.MESH


def dot_nn(a, b):
    return lax.dot_general(a, b, (((1,), (0,)), ((), ())), preferred_element_type=F32)


def dot_nt(a, b):
    return lax.dot_general(a, b, (((1,), (1,)), ((), ())), preferred_element_type=F32)


def lanes(m, count=1):
    return slice(m * LANES, (m + count) * LANES)


def aligned(x, m):
    return pl.multiple_of(x, m)


def anti_eye(n):
    rows = lax.broadcasted_iota(jnp.int32, (n, n), 0)
    cols = lax.broadcasted_iota(jnp.int32, (n, n), 1)
    return (rows + cols == n - 1).astype(F32).astype(BF16)


def flip_lanes(x, eye):
    n, w = x.shape[1], eye.shape[0]
    parts = [dot_nn(x[:, s:s + w], eye).astype(BF16) for s in range(0, n, w)]
    return jnp.concatenate(parts[::-1], axis=1)


def reverse_rows(x):
    ix = 7 - lax.broadcasted_iota(jnp.int32, (8, x.shape[1]), 0)
    n = x.shape[0] // 8
    return jnp.concatenate([jnp.take_along_axis(x[(n - 1 - g) * 8:(n - g) * 8], ix, axis=0) for g in range(n)], 0)


def owner_core(rb):
    return lax.rem(rb + rb // 2, 2)


def remote_copy(src, dst, send_sem, recv_sem, to):
    return pltpu.make_async_remote_copy(src, dst, send_sem, recv_sem, device_id=(lax.axis_index('hp'), to),
                                        device_id_type=MESH_ID)


def greet_all(n):
    me, hp = lax.axis_index('cp'), lax.axis_index('hp')
    bar = pltpu.get_barrier_semaphore()
    for o in range(1, n):
        pl.semaphore_signal(bar, 1, device_id=(hp, lax.rem(me + o, n)), device_id_type=MESH_ID)


def await_all(n):
    pl.semaphore_wait(pltpu.get_barrier_semaphore(), n - 1)


def hand_off_kernel(o, dq, dk, dv, dw, bias, o_out, dq_out, dk_out, dv_out, dw_out, u_out, v_out):
    for src, dst in ((o, o_out), (dq, dq_out), (dk, dk_out), (dv, dv_out), (dw, dw_out)):
        dst[...] = src[...]
    u_out[...], v_out[...] = bias[0], bias[1]


def attention_kernel(n, q_in, k_in, v_in, do_in, table_in, w_rel, ub, vb,
                     o_out, dq_out, dk_out, dv_out, dw_out, bias_out,
                     qT, doT, kT, vT, relX, oT, dqT, dkT, dvT, drF,
                     s_all, q_off, q_row, do_row, q_col, qo_col, do_col, mx, total, acc, r_scr,
                     pair_buf, dr_send, send_buf, dr_buf, table, bias_buf,
                     send_d, send_f, send_q, recv_b, recv_q, loc_b, loc_q,
                     send_o, recv_o, send_p, recv_p, send_s, recv_s,
                     loc_t, send_w, recv_w, loc_w, send_b, recv_b2,
                     recv_u, recv_d2, recv_c, recv_h, send_x):
    me = lax.axis_index('cp')
    chip, core = me // 2, lax.rem(me, 2)
    mate = 2 * chip + 1 - core
    heads, dim, blk = q_in.shape
    seq = n * blk
    per_blk = blk // BQ
    groups = n // 2
    nslot = qT.shape[1] // BQ
    tiles = s_all.shape[0]
    scale = dim ** -0.5
    model = table.shape[1]

    def weight_block(m):
        return pltpu.make_async_copy(w_rel.at[:, pl.ds(m * LANES, LANES)], q_off.at[m], loc_t.at[1 + m])

    greet_all(n)
    pltpu.make_async_copy(table_in, table, loc_t.at[0]).start()
    for m in range(model // LANES):
        weight_block(m).start()

    rel_buf = dr_buf
    srcs, fulls = (rel_buf, k_in, v_in), (relX, kT, vT)

    def col(t, b, flipped):
        b = (n - 1 - b) if t == flipped else b
        return pl.ds(aligned(b * blk, blk), blk)

    def full_at(t, b):
        return fulls[t].at[pl.ds(0, dim), col(t, b, 0)]

    def direct(t, h):
        return remote_copy(srcs[t].at[h], full_at(t, me), send_d.at[t, h], recv_b.at[t, me], 2 * h + core)

    def own(t):
        return pltpu.make_async_copy(srcs[t].at[chip], full_at(t, me), loc_b.at[t])

    def to_mate(t):
        return remote_copy(srcs[t].at[chip], full_at(t, me), send_f.at[t, chip], recv_b.at[t, me], mate)

    def forward(t, g):
        b = 2 * g + core
        return remote_copy(full_at(t, b), full_at(t, b), send_f.at[t, g], recv_b.at[t, b], mate)

    def landed(t, b):
        remote_copy(srcs[t].at[0], full_at(t, b), send_f.at[t, 0], recv_b.at[t, b], me).wait_recv()

    def pass_on(t, g):
        @pl.when(g != chip)
        def _():
            landed(t, 2 * g + core)
            forward(t, g).start()

        pl.when(g == chip)(own(t).wait)

    def from_mate(t, g):
        landed(t, 2 * g + 1 - core)

    def row_copy(t, h, j, wait):
        rb = me * per_blk + j
        src = (q_in, do_in)[t].at[h, :, pl.ds(j * BQ, BQ)]
        dst = (qT, doT)[t].at[:, pl.ds(aligned(rb // 2 * BQ, BQ), BQ)]
        to = 2 * h + owner_core(rb)

        @pl.when(to != me)
        def _():
            c = remote_copy(src, dst, send_q.at[t, h, j], recv_q.at[t, rb // 2], to)
            c.wait_send() if wait else c.start()

        @pl.when(to == me)
        def _():
            c = pltpu.make_async_copy(src, dst, loc_q.at[t, j])
            c.wait() if wait else c.start()

    def row_block(k):
        return 2 * k + lax.rem(k + core, 2)

    def row_landed(t, k):
        src = (q_in, do_in)[t].at[0, :, pl.ds(0, BQ)]
        dst = (qT, doT)[t].at[:, pl.ds(aligned(k * BQ, BQ), BQ)]
        rb = row_block(k)

        @pl.when(rb // per_blk != me)
        def _():
            remote_copy(src, dst, send_q.at[t, 0, 0], recv_q.at[t, k], me).wait_recv()

        @pl.when(rb // per_blk == me)
        def _():
            pltpu.make_async_copy(src, dst, loc_q.at[t, lax.rem(rb, per_blk)]).wait()

    lower = chip < groups // 2
    side = chip + 1 - 2 * lax.rem(chip, 2)
    near, far = jnp.where(lower, groups // 2, groups // 2 - 1), jnp.where(lower, groups - 1, 0)
    across = near, far

    def send_rows(t, h):
        for j in range(per_blk):
            row_copy(t, h, j, False)

    def send_scores_input(h):
        direct(1, h).start()
        send_rows(0, h)

    eye = anti_eye(BQ)
    pltpu.make_async_copy(table_in, table, loc_t.at[0]).wait()
    for m in range(model // LANES):
        weight_block(m).wait()
    weights_in = jnp.concatenate([q_off[m] for m in range(model // LANES)], 1)
    rel = flip_lanes(dot_nt(weights_in, table[...]).astype(BF16), eye)
    for h in range(heads):
        rel_buf[h] = rel[h * dim:(h + 1) * dim]
    await_all(n)
    to_mate(1).start()
    own(1).start()
    send_scores_input(side)
    send_rows(0, chip)
    to_mate(0).start()
    own(0).start()
    for h in (side, *across):
        direct(0, h).start()
    for h in across:
        send_scores_input(h)

    def send_values():
        to_mate(2).start()
        own(2).start()
        for h in (side, *across):
            direct(2, h).start()

    def send_cotangent():
        for h in (side, *across):
            direct(0, h).wait_send()
        to_mate(0).wait_send()
        for h in (side, *across, chip):
            send_rows(1, h)

    for ref in (dkT, dvT, drF, total, acc):
        ref[...] = jnp.zeros_like(ref)
    mx[...] = jnp.full(mx.shape, -jnp.inf, F32)
    relX[pl.ds(0, dim), pl.ds(seq, PAD)] = jnp.zeros((dim, PAD), BF16)
    first = lax.broadcasted_iota(jnp.int32, (KX - dim, PAD), 0) == 0
    relX[pl.ds(dim, KX - dim), pl.ds(0, seq)] = jnp.zeros((KX - dim, seq), BF16)
    relX[pl.ds(dim, KX - dim), pl.ds(seq, PAD)] = jnp.where(first, -jnp.inf, 0.0).astype(BF16)
    ones_col = (lax.broadcasted_iota(jnp.int32, (BQ, KX - dim), 1) == 0).astype(F32).astype(BF16)
    lane = lax.broadcasted_iota(jnp.int32, (128, LANES), 1)
    row = lax.broadcasted_iota(jnp.int32, (128, LANES), 0)
    past, before = lane > row, lane < row

    def bias_col(ref):
        pick = lax.broadcasted_iota(jnp.int32, ref.shape, 0) == chip
        r = jnp.sum(jnp.where(pick, ref[...], 0.0), axis=0, keepdims=True)
        return jnp.broadcast_to(r, (LANES, dim)).T[:, :1]

    u_col, v_col = bias_col(ub), bias_col(vb)

    def skew(t):
        return pltpu.roll(t, 1, 1, stride=1, stride_axis=0)

    def slot_cols(k):
        return pl.ds(aligned(k * BQ, BQ), BQ)

    def transposed(x):
        return x.astype(F32).T.astype(BF16)

    def prepare(k):
        q = qT[:, slot_cols(k)].astype(F32)
        quT, qvT = (q + u_col).astype(BF16), (q + v_col).astype(BF16)
        q_off[k, :, :KX] = jnp.concatenate([transposed(qvT), ones_col], 1)
        q_col[k] = flip_lanes(quT, eye)
        q_row[k, :, :dim] = transposed(q_col[k])
        qo_col[k] = flip_lanes(qvT, eye)

    def prepare_skew(k, i, t):
        start = seq - row_block(k) * BQ + t * BK - 256
        t0 = dot_nn(q_off[k, :, :KX], relX[:, pl.ds(aligned(start, LANES), 256)])
        for m in range(2):
            r_scr[i, :, lanes(m)] = skew(t0[:, lanes(m)])

    def score_products(k, t):
        j0 = aligned(t * BK, BK)
        base = seq - row_block(k) * BQ
        by_offset = dot_nn(q_off[k, :, :KX], relX[:, pl.ds(aligned(base + j0, LANES), BK)])
        return by_offset, dot_nn(q_row[k, :, :dim], kT[:, pl.ds(j0, BK)])

    def scores(k, t, by_offset, content):
        ri = jnp.where(lax.rem(t, GROUP) == 0, lax.rem(k, GROUP), GROUP)
        rolled = [r_scr[ri, :, lanes(m)] for m in range(2)]
        rolled += [skew(by_offset[:, lanes(m)]) for m in range(NC)]
        top_s = mx[k]
        for m in range(NC):
            top = jnp.where(past, rolled[m + 2][:LANES], rolled[m + 1][:LANES])
            bot = jnp.where(past, rolled[m + 1][LANES:], rolled[m][LANES:])
            s = content[:, lanes(m)] + reverse_rows(jnp.concatenate([top, bot], 0))
            s = s * (scale * LOG2E)
            s_all[tile_of(k, t), :, lanes(m)] = s
            top_s = jnp.maximum(top_s, s)
        mx[k] = top_s
        for m in range(2):
            r_scr[GROUP, :, lanes(m)] = rolled[NC + m]

    def weights(k, t):
        tile, top_s, tot = tile_of(k, t), mx[k], total[k]
        parts = []
        for m in range(NC):
            p = jnp.exp2(s_all[tile, :, lanes(m)] - top_s)
            s_all[tile, :, lanes(m)] = p
            tot = tot + p
            parts.append(p.astype(BF16))
        total[k] = tot
        return jnp.concatenate(parts, 1)

    def add_values(k, t, p_all):
        acc[k, :, :dim] += dot_nt(p_all, vT[:, pl.ds(aligned(t * BK, BK), BK)])

    def finish_rows(k):
        do_col[k] = flip_lanes(doT[:, slot_cols(k)], eye)
        do_row[k] = transposed(do_col[k])
        inv = 1.0 / jnp.sum(total[k], axis=1, keepdims=True)
        out = acc[k, :, :dim] * inv
        delta = jnp.sum(do_row[k].astype(F32) * out, axis=1, keepdims=True)
        total[k] = jnp.broadcast_to(inv, (BQ, LANES))
        mx[k] = jnp.broadcast_to(delta, (BQ, LANES))
        oT[:, slot_cols(k)] = flip_lanes(out.T.astype(BF16), eye)
        acc[k] = jnp.zeros((BQ, 2 * dim), F32)

    def score_grads(k, t):
        return dot_nn(do_row[k], vT[:, pl.ds(aligned(t * BK, BK), BK)])

    def split_grads(tile, k, t, dp):
        inv, delta = total[k], mx[k]
        carry = (q_off, q_row)
        ps, dss = [], []
        held = [jnp.where(t > 0, c[k], jnp.zeros((BQ, LANES), BF16)) for c in carry]
        for m in range(NC):
            p = s_all[tile, :, lanes(m)] * inv
            ds = (p * ((dp[:, lanes(m)] - delta) * scale)).astype(BF16)
            ps.append(p.astype(BF16))
            dss.append(ds)
            held.append(pltpu.roll(ds, 0, 1, stride=1, stride_axis=0))
        for m in range(2):
            carry[m][k] = held[NC + m]
        by_offset = []
        for m in range(NC):
            top = jnp.where(before, held[m + 1][:LANES], held[m + 2][:LANES])
            bot = jnp.where(before, held[m][LANES:], held[m + 1][LANES:])
            by_offset.append(jnp.concatenate([top, bot], 0))
        return tuple(jnp.concatenate(x, 1) for x in (ps, dss, by_offset))

    def add_grads(k, t, p_all, ds_all, by_offset):
        j0 = aligned(t * BK, BK)
        base = seq - row_block(k) * BQ
        js, us = pl.ds(j0, BK), pl.ds(aligned(base + j0 - 256, LANES), BK)
        dvT[:, js] += dot_nn(do_col[k], p_all)
        dkT[:, js] += dot_nn(q_col[k], ds_all)
        drF[:, us] += dot_nn(qo_col[k], by_offset)
        none = jnp.zeros((dim, BK), BF16)
        keys = jnp.concatenate([jnp.concatenate([kT[:, js], none], 0), jnp.concatenate([none, relX[:dim, us]], 0)], 1)
        acc[k] += dot_nt(jnp.concatenate([ds_all, by_offset], 1), keys)

    def walk(steps, count, k, t_low, t_cap, unroll):
        def some(i, kt):
            k, t = kt
            at = []
            for u in range(unroll):
                at.append((k, t))
                last = t == jnp.minimum(k, t_cap)
                k, t = jnp.where(last, k + 1, k), jnp.where(last, t_low, t + 1)
            steps(at)
            return k, t

        lax.fori_loop(0, count // unroll, some, (k, t_low))

    def tile_of(k, t):
        return k * (k + 1) // 2 + t

    def grads(at):
        count = len(at)
        dps = [score_grads(*at[0])]
        for u, here in enumerate(at):
            if u + 1 < count:
                dps.append(score_grads(*at[u + 1]))
            add_grads(*here, *split_grads(tile_of(*here), *here, dps[u]))

    def group_tiles(g):
        return GROUP * GROUP * g + GROUP * (GROUP + 1) // 2

    def score_tiles(at):
        products = score_products(*at[0])
        for u, here in enumerate(at):
            ahead = score_products(*at[u + 1]) if u + 1 < len(at) else None
            scores(*here, *products)
            products = ahead

    def weigh_tiles(at):
        p_all = weights(*at[0])
        for u, here in enumerate(at):
            ahead = weights(*at[u + 1]) if u + 1 < len(at) else None
            add_values(*here, p_all)
            p_all = ahead

    def each(fn):
        lax.fori_loop(0, groups, lambda g, c: (fn(g), c)[1], 0)

    orders = ('00111030313320212232', '11001030313320212232', '22333200203011102131', '33223200203011102131')
    orders = [[(int(word[at]), int(word[at + 1])) for at in range(0, len(word), 2)] for word in orders]

    def schedule(order):
        seen = ([], [], [])
        rows = []
        for gq, gk in order:
            row = [gq, gk]
            for t, g in ((0, gq - gk), (0, gq - gk - 1), (1, gk), (2, gq)):
                new = g >= 0 and g not in seen[t]
                row.append(g if new else -1)
                if new:
                    seen[t].append(g)
            rows.append(row)
        return rows

    schedules = [schedule(order) for order in orders]

    def look_up(x, column):
        value = jnp.int32(-1)
        for at in range(len(orders[0])):
            here = jnp.int32(schedules[-1][at][column])
            for z in range(groups - 1):
                here = jnp.where(chip == z, schedules[z][at][column], here)
            value = jnp.where(x == at, here, value)
        return value

    def forward_scores(x):
        gq, gk, *need, new_q = (look_up(x, column) for column in range(6))
        *ahead, ahead_q = (look_up(x + 1, column) for column in range(2, 6))

        def arrives_now(g, q):
            return (q >= 0) & ((g < groups // 2) != lower) & (chip == 0)

        for t, g in zip((0, 0, 1), need):
            pl.when((g >= 0) & ((x == 0) | arrives_now(g, new_q)))(functools.partial(pass_on, t, g))
        for t, g, g1 in zip((0, 0, 1), need, ahead):
            pl.when((g1 >= 0) & ~arrives_now(g1, ahead_q))(functools.partial(pass_on, t, g1))
            pl.when(g >= 0)(functools.partial(from_mate, t, g))

        @pl.when(new_q >= 0)
        def _():
            for i in range(GROUP):
                row_landed(0, GROUP * new_q + i)
            for i in range(GROUP):
                prepare(GROUP * new_q + i)

        pl.when(x == VALUES_AT)(send_values)
        here = GROUP * gq, GROUP * gk, GROUP * gk + GROUP - 1

        def score_pair(count):
            for i in range(GROUP):
                prepare_skew(GROUP * gq + i, i, GROUP * gk)
            walk(score_tiles, count, *here, count)

        pl.when(gq == gk)(lambda: score_pair(GROUP * (GROUP + 1) // 2))
        pl.when(gq != gk)(lambda: score_pair(GROUP * GROUP))

    lax.fori_loop(0, len(orders[0]), lambda x, c: (forward_scores(x), c)[1], 0)
    send_cotangent()
    each(lambda g: pass_on(2, g))

    def row_max(g):
        for i in range(GROUP):
            k = GROUP * g + i
            mx[k] = jnp.broadcast_to(jnp.max(mx[k], axis=1, keepdims=True), (BQ, LANES))

    each(row_max)

    each(lambda g: from_mate(2, g))
    walk(weigh_tiles, tiles, 0, 0, nslot, UNROLL_SUM)

    def out_rows(t, k):
        rb = row_block(k)
        to, j = rb // per_blk, lax.rem(rb, per_blk)
        src = (oT, dqT)[t].at[:, slot_cols(k)]
        dst = (o_out, dq_out)[t].at[chip, :, pl.ds(aligned(j * BQ, BQ), BQ)]
        pl.when(to != me)(lambda: remote_copy(src, dst, send_o.at[t], recv_o.at[t], to).start())
        pl.when(to == me)(lambda: pltpu.make_async_copy(src, dst, recv_o.at[t]).start())

    def rows_done(t):
        src, dst = (oT, dqT)[t], (o_out, dq_out)[t]
        remote_copy(dst, dst, send_o.at[t], recv_o.at[t], mate).wait_recv()
        kept = sum((owner_core(me * per_blk + j) == core).astype(jnp.int32) for j in range(per_blk))
        for count in (1, 2):
            left = src.at[:, pl.ds(0, (nslot - count) * BQ)]
            pl.when(kept == count)(remote_copy(left, left, send_o.at[t], recv_o.at[t], mate).wait_send)

    def finish_group(g):
        for i in range(GROUP):
            row_landed(1, GROUP * g + i)
        for i in range(GROUP):
            finish_rows(GROUP * g + i)
        for i in range(GROUP):
            out_rows(0, GROUP * g + i)

    each(finish_group)

    parts, sinks = (drF, dkT, dvT), (dr_buf, dk_out, dv_out)

    hw = blk // 2
    slots = pair_buf.shape[1]

    def out_block(t, step):
        return n - 1 - step if t == 0 else jnp.where(lower, n - 1 - step, step)

    def half_of(t, step, c):
        b = out_block(t, step)
        b = n - 1 - b if t == 0 else b
        return pl.ds(aligned(b * blk + c * hw, LANES), hw)

    def pair(t, step):
        s = lax.rem(step, slots)
        return remote_copy(parts[t].at[:, half_of(t, step, 1 - core)], pair_buf.at[t, s], send_p.at[t, s], recv_p.at[t, s], mate)

    def ready(t, step):
        return dr_send.at[step] if t == 0 else send_buf.at[t - 1, step]

    def sink_at(t, h, c):
        return sinks[t].at[h, :, pl.ds(aligned(c * hw, LANES), hw)]

    def sink(t, step):
        return remote_copy(ready(t, step), sink_at(t, chip, core), send_s.at[t], recv_s.at[t], out_block(t, step))

    def keep(t, step):
        return pltpu.make_async_copy(ready(t, step), sink_at(t, chip, core), recv_s.at[t])

    def combine(t, step):
        s = lax.rem(step, slots)
        mine = half_of(t, step, core)
        remote_copy(parts[t].at[:, mine], pair_buf.at[t, s], send_p.at[t, s], recv_p.at[t, s], mate).wait_recv()
        ready(t, step)[...] = (parts[t][:, mine] + pair_buf[t, s]).astype(BF16)
        pair(t, step).wait_send()

    def to_owner(t, step):
        b = out_block(t, step)
        pl.when(b != me)(lambda: sink(t, step).start())
        pl.when(b == me)(lambda: keep(t, step).start())

    def arrived(t):
        remote_copy(sinks[t], sinks[t], send_s.at[t], recv_s.at[t], mate).wait_recv()

    def departed(t):
        others = (dr_send if t == 0 else send_buf.at[t - 1]).at[pl.ds(0, n - 1)]
        remote_copy(others, others, send_s.at[t], recv_s.at[t], mate).wait_send()

    def final_slots(step, fn):
        first, end = (3 * step + 1) // 2, (3 * step + 4) // 2
        for i in range(2):
            at = first + i
            pl.when(at < end)(functools.partial(fn, jnp.where(lower, nslot - 1 - at, at)))

    def row_grads(k):
        dqT[:, slot_cols(k)] = flip_lanes((acc[k, :, :dim] + acc[k, :, dim:]).T.astype(BF16), eye)

    def exchange(step):
        for t in range(3):
            pair(t, step).start()
        final_slots(step, row_grads)

    def bulk(step):
        for t in (1, 2):
            to_owner(t, step)
        final_slots(step, lambda k: out_rows(1, k))

    def held(step):
        return ((chip == 3) & ((step == 3) | (step == 4) | (step == 5)))

    def release_offsets(step):
        combine(0, step)
        to_owner(0, step)

    def release_rest(step):
        for t in (1, 2):
            combine(t, step)
        pl.when(~held(step))(lambda: bulk(step))

    def release(step):
        release_offsets(step)
        release_rest(step)

    w_acc, w_in, w_half, w_part, w_mine = (9, 0), (10, 0), (10, 1), (11, 0), (11, 1)
    chunks, wide = range(4), BK // 2
    half = heads * dim // 2
    piece = half // heads

    def place(kt, c, row0, count):
        at = kt[0] * (kt[0] + 1) // 2 + kt[1]
        return s_all.at[at, pl.ds(row0, count), pl.ds(c % 2 * wide, wide)]

    def acc_at(c, row0, count):
        return place((w_acc[0], w_acc[1] + c // 2), c, row0, count)

    def swap(c):
        return remote_copy(acc_at(c, aligned((1 - core) * half, half), half), place(w_in, c, c // 2 * half, half),
                           send_w.at[c], recv_w.at[c], mate)

    def share(c, z):
        return place(w_half, c, aligned(c // 2 * half + z * piece, piece), piece)

    def from_below(c, z):
        return place(w_part, c, aligned((2 * z + c // 2) * piece, piece), piece)

    def from_above(c, z):
        return place(w_mine, c, (2 + 2 * z + c // 2) * piece, piece)

    def up(z, c):
        return remote_copy(share(c, z), from_below(c, chip), send_x.at[0], recv_u.at[chip, c], 2 * z + core)

    def down(z, c):
        return remote_copy(share(c, z), from_above(c, z), send_x.at[0], recv_d2.at[z, c], me - 2)

    def table_grad():
        arrived(0)
        dr = jnp.concatenate([flip_lanes(dr_buf[h], eye) for h in range(heads)], 0)
        for c in chunks:
            acc_at(c, 0, 2 * half)[...] = dot_nn(dr, table[:, c * wide:(c + 1) * wide])
        for c in chunks:
            swap(c).start()
        for c in chunks:
            swap(c).wait()
            place(w_half, c, c // 2 * half, half)[...] = (
                acc_at(c, aligned(core * half, half), half)[...] + place(w_in, c, c // 2 * half, half)[...])
        for c in chunks:
            for z in range(heads - 1, 0, -1):
                pl.when(z > chip)(up(z, c).start)

    bodies, done = [], 0
    for step in range(n):
        tiles_done = sum(nslot - i for i in range((3 * step + 4) // 2))
        bodies.append(-(-tiles_done // UNROLL_GRAD) - done)
        done += bodies[-1]
    phases = [c for b in bodies[:-1] for c in (min(b, 1), max(b - 1, 0))]

    def next_tile(k, t):
        last = jnp.where(lower, t == k, k == nslot - 1)
        k1 = jnp.where(lower, k - 1, t + 1)
        return (jnp.where(last, k1, jnp.where(lower, k, k + 1)), jnp.where(last, jnp.where(lower, 0, t + 1), jnp.where(lower, t + 1, t)))

    def phase(x, kt):
        count = jnp.int32(0)
        for at, c in enumerate(phases):
            count = jnp.where(x == at, c, count)

        def some(i, kt):
            at = []
            for u in range(UNROLL_GRAD):
                at.append(kt)
                kt = next_tile(*kt)
            grads(at)
            return kt

        kt = lax.fori_loop(0, count, some, kt)
        pl.when(lax.rem(x, 2) == 1)(lambda: exchange(x // 2))
        pl.when((lax.rem(x, 2) == 0) & (x > 0))(lambda: release(x // 2 - 1))
        return kt

    lax.fori_loop(0, len(phases), phase, (jnp.where(lower, nslot - 1, 0), jnp.int32(0)))
    exchange(n - 1)
    for part in (release_offsets, release_rest):
        part(n - 2)
        part(n - 1)
    rows_sum = jnp.sum(jnp.sum(acc[...].reshape(nslot * BQ // 8, 8, 2 * dim), axis=0), axis=0, keepdims=True)
    for t in range(2):
        bias_buf[me, t] = rows_sum[:, t * dim:(t + 1) * dim] + jnp.zeros((8, dim), F32)

    def bias(o):
        return remote_copy(bias_buf.at[me], bias_buf.at[me], send_b.at[0], recv_b2.at[0], lax.rem(me + o, n))

    for o in range(1, n):
        bias(o).start()
    for t in range(3):
        if t:
            to_mate(t).wait_send()
        for i in range(1, heads):
            h = lax.rem(chip + i, heads)
            forward(t, h).wait_send()
            if t:
                direct(t, h).wait_send()
    for t in (0, 1):
        for h in range(heads):
            for j in range(per_blk):
                to = 2 * h + owner_core(me * per_blk + j)

                @pl.when(to != me)
                def _():
                    remote_copy((q_in, do_in)[t].at[0, :, pl.ds(0, BQ)], (qT, doT)[t].at[:, pl.ds(0, BQ)],
                                send_q.at[t, h, j], recv_q.at[t, 0], to).wait_send()
    rows_done(0)
    table_grad()

    def up_landed(z, c):
        remote_copy(share(c, 0), from_below(c, z), send_x.at[0], recv_u.at[z, c], me).wait_recv()

    def take_above(z, c):
        @pl.when(chip < groups - 1)
        def _():
            remote_copy(share(c, z), from_above(c, z), send_x.at[0], recv_d2.at[z, c], me).wait_recv()
            share(c, z)[...] += from_above(c, z)[...]

        pl.when(z < chip)(down(z, c).start)

    def home(co, z, c):
        return dw_out.at[pl.ds(aligned(co * half + z * piece, piece), piece), pl.ds(c * wide, wide)]

    def my_piece(c):
        return place(w_mine, c, c // 2 * piece, piece)

    end = jnp.where(lower, heads - 1, 0)

    def collect(z, c):
        return remote_copy(my_piece(c), home(core, chip, c), send_x.at[0], recv_c.at[chip, c], 2 * z + core)

    def relay(z, c):
        return remote_copy(home(core, z, c), home(core, z, c), send_x.at[0], recv_c.at[z, c], jnp.where(lower, core, n - 2 + core))

    def relays(z):
        return ((chip == 1) & (z > 1)) | ((chip == groups - 2) & (z < groups - 2))

    def hand_over(z):
        whole = dw_out.at[pl.ds(aligned(core * half + z * piece, piece), piece)]
        return remote_copy(whole, whole, send_x.at[0], recv_h.at[0], mate)

    def hand_over_mine(c):
        return remote_copy(my_piece(c), home(core, chip, c), send_x.at[0], recv_h.at[0], mate)

    def stay(c):
        return pltpu.make_async_copy(my_piece(c), home(core, chip, c), loc_w.at[0])

    for c in chunks:
        for z in range(heads - 1):
            pl.when(z <= chip)(functools.partial(take_above, z, c))
    for step in (3, 4, 5):
        pl.when(held(step))(functools.partial(bulk, step))
    for c in chunks:
        for z in range(heads - 1):
            @pl.when(z < chip)
            def _():
                up_landed(z, c)
                share(c, chip)[...] += from_below(c, z)[...]

        my_piece(c)[...] = share(c, chip)[...]
        for z in range(heads):
            pl.when((z != chip) & (z != end))(collect(z, c).start)
        hand_over_mine(c).start()
        stay(c).start()
    for c in chunks:
        for at in range(heads):
            z = jnp.where(lower, at, heads - 1 - at)

            @pl.when(z != chip)
            def _():
                remote_copy(my_piece(c), home(core, z, c), send_x.at[0], recv_c.at[z, c], me).wait_recv()
                pl.when(relays(z))(relay(z, c).start)
                if c == chunks[-1]:
                    hand_over(z).start()

    others = bias_buf.at[pl.ds(0, n - 1)]
    remote_copy(others, others, send_b.at[0], recv_b2.at[0], mate).wait_recv()
    for t in range(2):
        bias_out[t] = jnp.concatenate([bias_buf[2 * h, t, :1] + bias_buf[2 * h + 1, t, :1] for h in range(heads)], 0)

    my_rows = dw_out.at[pl.ds(aligned(core * half + chip * piece, piece), piece)]
    pltpu.make_async_copy(my_rows, my_rows, loc_w.at[0]).wait()
    remote_copy(others, others, send_b.at[0], recv_b2.at[0], mate).wait_send()
    for t in range(3):
        departed(t)
        if t:
            arrived(t)
    rows_done(1)
    for count, here in ((9, (chip == 0) | (chip == groups - 1)), (11, (chip > 0) & (chip < groups - 1))):
        sent = s_all.at[pl.ds(0, count), pl.ds(0, 2 * piece)]
        pl.when(here)(remote_copy(sent, sent, send_x.at[0], recv_h.at[0], mate).wait_send)
    theirs = dw_out.at[pl.ds(aligned((1 - core) * half, half), half)]
    remote_copy(theirs, theirs, send_x.at[0], recv_h.at[0], mate).wait_recv()


def solution(mesh):
    n = mesh.shape['cp']
    seq_spec, head_spec, weight_spec = P('cp', 'hp', None), P('hp', None), P(None, 'hp', None)
    vmem = pl.BlockSpec(memory_space=pltpu.VMEM)
    hbm = pl.BlockSpec(memory_space=pl.ANY)
    dma, sds, buf = pltpu.SemaphoreType.DMA, jax.ShapeDtypeStruct, pltpu.VMEM

    def local_fn(q, k, v, u_bias, v_bias, rel_table, w_rel, d_out):
        blk, heads, dim = q.shape
        seq = n * blk
        rows = seq // 2
        nslot = rows // BQ
        per_blk = blk // BQ
        tiles = nslot * (nslot + 1) // 2
        qT, kT, vT, doT = (x.transpose(1, 2, 0) for x in (q, k, v, d_out))
        wT = w_rel.transpose(1, 2, 0).reshape(heads * dim, -1)
        model = wT.shape[1]
        o, dq, dk, dvv, dw, bias = pl.pallas_call(
            functools.partial(attention_kernel, n),
            out_shape=[sds((heads, dim, blk), BF16)] * 4 + [sds((heads * dim, model), F32), sds((2, heads, dim), F32)],
            in_specs=[hbm] * 6 + [vmem] * 2, out_specs=[hbm] * 5 + [vmem],
            scratch_shapes=[
                buf((dim, rows), BF16), buf((dim, rows), BF16), buf((dim, seq), BF16), buf((dim, seq), BF16), buf((KX, seq + PAD), BF16),
                buf((dim, rows), BF16), buf((dim, rows), BF16), buf((dim, seq), F32), buf((dim, seq), F32), buf((dim, seq + PAD), F32),
                buf((tiles, BQ, BK), F32), buf((nslot, BQ, LANES), BF16), buf((nslot, BQ, LANES), BF16), buf((nslot, BQ, dim), BF16),
                buf((nslot, dim, BQ), BF16), buf((nslot, dim, BQ), BF16), buf((nslot, dim, BQ), BF16),
                buf((nslot, BQ, LANES), F32), buf((nslot, BQ, LANES), F32), buf((nslot, BQ, 2 * dim), F32),
                buf((GROUP + 1, BQ, 256), F32),
                buf((3, 4, dim, blk // 2), F32), buf((n, dim, blk // 2), BF16), buf((2, n, dim, blk // 2), BF16), buf((heads, dim, blk), BF16), buf((blk, model), BF16),
                buf((n, 2, 8, dim), F32),
                dma((3, heads)), dma((3, heads)), dma((2, heads, per_blk)), dma((3, n)), dma((2, nslot)), dma((3,)), dma((2, per_blk)),
                dma((2,)), dma((2,)), dma((3, 4)), dma((3, 4)), dma((3,)), dma((3,)),
                dma((1 + model // LANES,)), dma((4,)), dma((4,)), dma((1,)), dma((1,)), dma((1,)),
                *[dma((heads, 4))] * 3, dma((1,)), dma((1,))],
            compiler_params=pltpu.CompilerParams(collective_id=0, has_side_effects=True, vmem_limit_bytes=67043328),
            name='attention',
        )(qT, kT, vT, doT, rel_table, wT, u_bias, v_bias)
        steps = 2
        part = pl.BlockSpec((heads // steps, dim, blk), lambda i: (i, 0, 0))
        wide = pl.BlockSpec((heads * dim // steps, model), lambda i: (i, 0))
        whole = lambda *shape: pl.BlockSpec(shape, lambda i: (0,) * len(shape))
        o, dq, dk, dvv, dw, du, dv = pl.pallas_call(
            hand_off_kernel, grid=(steps,),
            out_shape=[sds((heads, dim, blk), BF16)] * 4 + [sds((heads * dim, model), F32)] + [sds((heads, dim), F32)] * 2,
            in_specs=[part] * 4 + [wide, whole(2, heads, dim)],
            out_specs=[part] * 4 + [wide, whole(heads, dim), whole(heads, dim)],
            name='hand_off',
        )(o, dq, dk, dvv, dw, bias)
        back = lambda x: x.transpose(2, 0, 1)
        return back(o), back(dq), back(dk), back(dvv), du, dv, back(dw.reshape(heads, dim, model))

    return jax.shard_map(
        local_fn, mesh=mesh,
        in_specs=(seq_spec, seq_spec, seq_spec, head_spec, head_spec, P('cp', None), weight_spec, seq_spec),
        out_specs=(seq_spec, seq_spec, seq_spec, seq_spec, head_spec, head_spec, weight_spec),
        check_vma=False,
    )
```
